256 devices in a mesh: seq: 32 (over z, y_lo, core), head: 8 (over y_hi, x).
Axes of the slice: x: 4, y: 4 (y_hi: 2, y_lo: 2; y = y_hi * 2 + y_lo), z: 8, core: 2. Of those that a mesh axis runs over, the one named last changes fastest.
Arguments:
- tokens: bfloat16 [16384, 1024], P('seq'), may hold values from -24 to 24
- norm_attn: float32 [1024], replicated, may hold values from 0.5 to 1.5
- self_qkv: bfloat16 [3, 1024, 1024], P(None, None, 'head'), may hold values from -4 to 4
- self_out: bfloat16 [1024, 1024], P('head'), may hold values from -0.1875 to 0.1875
- norm_ffn: float32 [1024], replicated, may hold values from 0.5 to 1.5
- ffn_in: bfloat16 [2, 1024, 2816], P(None, None, 'head'), may hold values from -0.1875 to 0.1875
- ffn_out: bfloat16 [2816, 1024], P('head'), may hold values from -0.109375 to 0.109375
- norm_final: float32 [1024], replicated, may hold values from 0.5 to 1.5
- pad_lengths: int32 [32], replicated, may hold values from 64 to 512
- targets: bfloat16 [512, 1024], replicated, may hold values from -8 to 8
- target_lengths: int32 [4], replicated, may hold values from 32 to 128
- norm_cross: float32 [1024], replicated, may hold values from 0.1 to 1.9
- cross_query: bfloat16 [1024, 1024], P(None, 'head'), may hold values from -4 to 4
- cross_kv: bfloat16 [2, 1024, 1024], P(None, None, 'head'), may hold values from -4 to 4
- cross_out: bfloat16 [1024, 1024], P('head'), may hold values from -4 to 4
Outputs:
- encoded: bfloat16 [16384, 1024], P('seq')
- decoded: bfloat16 [512, 1024], replicated
The draws below stay inside these ranges and needn't reach their ends.
All inputs are finite; a program needn't handle non-finite values.
Results may differ from the reference program's by a relative error of at most 0.033.
Values may be sent and summed in bfloat16 or wider, within the bound.
A program may use at most 128 MiB of HBM per device.

```python
import math
import jax
import jax.numpy as jnp
from jax import lax

D = 1024
HEADS = 16
HD = 64
FF = 2816
TOK_DEV = 512
TGT_SEQS = 4
TGT_LEN = 128
TOKENS = 16384
TGT = 512
BLOCKS = 32


def plant_strength():
    return math.sqrt(300.0 * math.sqrt(HD) / D)


def plant_vectors(seed_key):
    base_key = jax.random.fold_in(seed_key, 9001)
    direction = jax.random.normal(jax.random.fold_in(base_key, 1), (D,), jnp.float32)
    direction = direction / jnp.sqrt(jnp.sum(direction * direction))
    target_dir = jax.random.normal(jax.random.fold_in(base_key, 2), (HEADS, HD), jnp.float32)
    target_dir = target_dir / jnp.sqrt(jnp.sum(target_dir * target_dir, axis=1, keepdims=True))
    return (direction, target_dir.reshape(HEADS * HD))


def projection(seed_key, salt, planted):
    matrix = jax.random.normal(jax.random.fold_in(seed_key, salt), (planted.shape[0], D, HEADS * HD), jnp.float32) * D ** (-0.5)
    matrix = jnp.clip(matrix, -3.5, 3.5)
    direction, target_dir = plant_vectors(seed_key)
    bump = plant_strength() * jnp.outer(direction, target_dir)
    matrix = matrix + planted[:, None, None] * bump[None, :, :]
    return matrix


def draw_self_qkv(seed_key, part_index):
    return projection(seed_key, 11, jnp.array([1.0, 1.0, 0.0], jnp.float32)).astype(jnp.bfloat16)


def draw_cross_query(seed_key, part_index):
    return projection(seed_key, 12, jnp.array([1.0], jnp.float32))[0].astype(jnp.bfloat16)


def draw_cross_kv(seed_key, part_index):
    return projection(seed_key, 13, jnp.array([1.0, 0.0], jnp.float32)).astype(jnp.bfloat16)


def draw_tokens(seed_key, part_index):
    rows_drawn = jnp.clip(jax.random.normal(jax.random.fold_in(seed_key, 21), (TOKENS, D), jnp.float32), -6.0, 6.0)
    direction, target_dir = plant_vectors(seed_key)
    row_ids = jnp.arange(TOKENS, dtype=jnp.int32)[:, None]
    picked = (jax.random.randint(jax.random.fold_in(seed_key, 22), (TOKENS, 1), 0, 32) == 0) | (row_ids % (4 * TOK_DEV) == 0)
    planted_rows = 128.0 * direction[None, :] + 96.0 / math.sqrt(D) * rows_drawn
    rows_drawn = jnp.where(picked, planted_rows, rows_drawn)
    return jnp.clip(rows_drawn, -24.0, 24.0).astype(jnp.bfloat16)


def draw_targets(seed_key, part_index):
    rows_drawn = jnp.clip(jax.random.normal(jax.random.fold_in(seed_key, 31), (TGT, D), jnp.float32), -6.0, 6.0)
    direction, target_dir = plant_vectors(seed_key)
    row_ids = jnp.arange(TGT, dtype=jnp.int32)[:, None]
    picked = (jax.random.randint(jax.random.fold_in(seed_key, 32), (TGT, 1), 0, 16) == 0) | (row_ids == 0)
    rows_drawn = jnp.where(picked, 32.0 * direction[None, :], rows_drawn)
    return jnp.clip(rows_drawn, -8.0, 8.0).astype(jnp.bfloat16)


def set_ends(drawn, own_key, smallest, top_value):
    longest = drawn.shape.index(max(drawn.shape))
    spots = []
    for shift in (0, 1):
        where = [jax.random.randint(jax.random.fold_in(own_key, axis), (), 0, length) for axis, length in enumerate(drawn.shape)]
        where[longest] = (where[longest] + shift) % drawn.shape[longest]
        spots.append(tuple(where))
    return drawn.at[spots[0]].set(smallest).at[spots[1]].set(top_value)


def levels(own_key, shape, shards, least, largest):
    def one(axis_at, shards_of):
        steps = jax.random.uniform(jax.random.fold_in(jax.random.fold_in(own_key, 6), axis_at), (shards_of,), jnp.float32, least / len(shards), largest / len(shards))
        return jnp.repeat(jnp.exp(steps), shape[axis_at] // shards_of).reshape((-1,) + (1,) * (len(shape) - axis_at - 1))

    factor_of = one(*shards[0])
    for cut in shards[1:]:
        factor_of = factor_of * one(*cut)
    return factor_of


def scatter_about(stream_key, extent, scale, reach, cuts=(), held_as=jnp.bfloat16):
    loudness = levels(stream_key, extent, cuts, -0.22, 0.18) if cuts else 1.0
    values = jax.random.normal(stream_key, extent, jnp.float32) * scale * loudness
    return jnp.minimum(jnp.maximum(values, -reach), reach).astype(held_as)


def setup_inputs(seed: int = 0) -> dict:
    key_of = jax.random.split(jax.random.key(seed), 16)
    tokens = draw_tokens(jax.random.fold_in(key_of[15], 71), 0)
    norm_attn = jnp.clip(1.0 + 0.1 * jax.random.normal(key_of[1], (D,), jnp.float32), 0.5, 1.5)
    self_qkv = draw_self_qkv(jax.random.fold_in(key_of[15], 71), 0)
    self_out = scatter_about(key_of[3], (HEADS * HD, D), (HEADS * HD) ** -0.5, 0.1875, ((0, 8),))
    norm_ffn = jnp.clip(1.0 + 0.1 * jax.random.normal(key_of[4], (D,), jnp.float32), 0.5, 1.5)
    ffn_in = scatter_about(key_of[5], (2, D, FF), D ** -0.5, 0.1875, ((2, 8),))
    ffn_out = scatter_about(key_of[6], (FF, D), FF ** -0.5, 0.109375, ((0, 8),))
    norm_final = jnp.clip(1.0 + 0.1 * jax.random.normal(key_of[7], (D,), jnp.float32), 0.5, 1.5)
    pad_lengths = set_ends(jax.random.randint(key_of[8], (BLOCKS,), TOK_DEV // 8, TOK_DEV + 1), jax.random.fold_in(key_of[8], 1), TOK_DEV // 8, TOK_DEV).astype(jnp.int32)
    targets = draw_targets(jax.random.fold_in(key_of[15], 71), 0)
    target_lengths = set_ends(jax.random.randint(key_of[10], (TGT_SEQS,), TGT_LEN // 4, TGT_LEN + 1), jax.random.fold_in(key_of[10], 1), TGT_LEN // 4, TGT_LEN).astype(jnp.int32)
    norm_cross = jnp.clip(1.0 + 0.18 * jax.random.normal(key_of[11], (D,), jnp.float32), 0.1, 1.9)
    cross_query = draw_cross_query(jax.random.fold_in(key_of[15], 71), 0)
    cross_kv = draw_cross_kv(jax.random.fold_in(key_of[15], 71), 0)
    cross_out = scatter_about(key_of[14], (HEADS * HD, D), (8.0 / (HEADS * HD) ** 0.5), 4.0, ((0, 8),))
    return {"tokens": tokens, "norm_attn": norm_attn, "self_qkv": self_qkv, "self_out": self_out, "norm_ffn": norm_ffn, "ffn_in": ffn_in, "ffn_out": ffn_out, "norm_final": norm_final, "pad_lengths": pad_lengths, "targets": targets, "target_lengths": target_lengths, "norm_cross": norm_cross, "cross_query": cross_query, "cross_kv": cross_kv, "cross_out": cross_out}


epsilon = 1e-06
masked_score = -1e+30

def rms_norm(values, gain_vector):
    widened = values.astype(jnp.float32)
    return widened * lax.rsqrt(lax.optimization_barrier(jnp.mean(widened * widened, axis=-1, keepdims=True)) + epsilon) * gain_vector.astype(jnp.float32)

def attend(queries, keys, values, live_keys):
    query_count = queries.shape[0]
    key_count = keys.shape[0]
    query_heads = queries.reshape(query_count, HEADS, HD).transpose(1, 0, 2)
    key_heads = keys.reshape(key_count, HEADS, HD).transpose(1, 0, 2)
    value_heads = values.reshape(key_count, HEADS, HD).transpose(1, 0, 2)
    block_rows = math.gcd(query_count, 1024)
    scaling = HD ** (-0.5)

    def one_head(head_parts):
        head_queries, head_keys, head_values = head_parts
        blocked = head_queries.reshape(query_count // block_rows, block_rows, HD)

        def one_block(block_queries):
            scores = jnp.dot(block_queries, head_keys.T, preferred_element_type=jnp.float32) * scaling
            scores = jnp.where(live_keys[None, :], scores, masked_score)
            row_max = lax.optimization_barrier(jnp.max(scores, axis=1, keepdims=True))
            weights = jnp.where(live_keys[None, :], jnp.exp(scores - row_max), 0.0)
            weight_sum = lax.optimization_barrier(jnp.sum(weights, axis=1, keepdims=True))
            mixed_rows = jnp.dot(weights.astype(jnp.bfloat16), head_values, preferred_element_type=jnp.float32)
            return mixed_rows / weight_sum
        return lax.map(one_block, blocked).reshape(query_count, HD)
    per_head = lax.map(one_head, (query_heads, key_heads, value_heads))
    return per_head.transpose(1, 0, 2).reshape(query_count, HEADS * HD).astype(jnp.bfloat16)

def reference(tokens, norm_attn, self_qkv, self_out, norm_ffn, ffn_in, ffn_out, norm_final, pad_lengths, targets, target_lengths, norm_cross, cross_query, cross_kv, cross_out):
    normed = rms_norm(tokens, norm_attn).astype(jnp.bfloat16)
    queries = jnp.dot(normed, self_qkv[0], preferred_element_type=jnp.float32).astype(jnp.bfloat16)
    keys = jnp.dot(normed, self_qkv[1], preferred_element_type=jnp.float32).astype(jnp.bfloat16)
    values = jnp.dot(normed, self_qkv[2], preferred_element_type=jnp.float32).astype(jnp.bfloat16)
    positions = jnp.arange(TOKENS, dtype=jnp.int32)
    live = positions % TOK_DEV < jnp.repeat(pad_lengths, TOK_DEV, total_repeat_length=TOKENS)
    context = attend(queries, keys, values, live)
    hidden_in = tokens.astype(jnp.float32) + jnp.dot(context, self_out, preferred_element_type=jnp.float32)
    ffn_normed = rms_norm(hidden_in, norm_ffn).astype(jnp.bfloat16)
    gate_proj = jnp.dot(ffn_normed, ffn_in[0], preferred_element_type=jnp.float32)
    up_proj = jnp.dot(ffn_normed, ffn_in[1], preferred_element_type=jnp.float32)
    activated = (jax.nn.gelu(gate_proj, approximate=True) * up_proj).astype(jnp.bfloat16)
    final_in = hidden_in + jnp.dot(activated, ffn_out, preferred_element_type=jnp.float32)
    encoded = rms_norm(final_in, norm_final).astype(jnp.bfloat16)
    cross_normed = rms_norm(targets, norm_cross).astype(jnp.bfloat16)
    cross_queries = jnp.dot(cross_normed, cross_query, preferred_element_type=jnp.float32).astype(jnp.bfloat16)
    cross_keys = jnp.dot(encoded, cross_kv[0], preferred_element_type=jnp.float32).astype(jnp.bfloat16)
    cross_values = jnp.dot(encoded, cross_kv[1], preferred_element_type=jnp.float32).astype(jnp.bfloat16)
    cross_context = attend(cross_queries, cross_keys, cross_values, live)
    slots = jnp.arange(TGT, dtype=jnp.int32)
    target_live = slots % TGT_LEN < jnp.repeat(target_lengths, TGT_LEN, total_repeat_length=TGT)
    cross_total = jnp.dot(cross_context, cross_out, preferred_element_type=jnp.float32)
    decoded = (targets.astype(jnp.float32) + jnp.where(target_live[:, None], cross_total, 0.0)).astype(jnp.bfloat16)
    return (encoded, decoded)
```

```python
import functools
import math

import jax
import jax.numpy as jnp
from jax import lax
from jax.experimental import pallas as pl
from jax.experimental.pallas import tpu as pltpu
from jax.sharding import Mesh
from jax.sharding import PartitionSpec as P

D = 1024
HD = 64
TOK_DEV = 512
TGT_LEN = 128


epsilon = 1e-06
masked_score = -1e30


NZ = 8
SLOTS = 32
UP = (("O", 0, 0), ("O", 0, 1), ("O", 1, 0), ("O", 1, 1), ("O", 2, 0), ("O", 2, 1), ("P", 2, 0), ("O", 3, 0), ("P", 2, 1), ("P", 3, 0))
DOWN = (("O", 0, 1), ("O", 0, 0), ("O", -1, 1), ("O", -1, 0), ("O", -2, 1), ("O", -2, 0), ("P", -2, 1), ("O", -3, 1), ("P", -3, 1), ("P", -2, 0))
SIDE = (("O", 0, 0), ("O", 0, 1), ("O", 1, 0), ("O", -1, 1), ("O", 2, 0), ("O", -2, 1), ("O", 2, 1), ("O", -2, 0), ("O", 1, 1), ("O", -1, 0))
CHIPS = (("O", 0), ("O", 1), ("O", -1), ("P", 0), ("O", 2), ("O", -2), ("O", 3), ("O", -3), ("P", 2), ("P", -2), ("O", 4), ("P", 1), ("P", 3), ("P", -1), ("P", -3), ("P", 4))
STEPS_BEFORE = {1: (0, 1), 3: (2,), 4: (3,), 6: (4, 5), 8: (6,), 9: (7,), 11: (8,), 13: (9,)}
STEPS = 10


def link_plan():
    arrive = {("O", 0, 0): -1, ("O", 0, 1): -1}
    arrivals = []
    for s in range(STEPS):
        new = [(UP[s][0], UP[s][1] + 1, UP[s][2]), (DOWN[s][0], DOWN[s][1] - 1, DOWN[s][2])]
        new.append(("P", SIDE[s][1], SIDE[s][2]))
        arrive.update({item: s for item in new})
        arrivals.append(new)
    waiting = {"up": list(UP), "down": list(DOWN), "side": list(SIDE)}
    sent = {name: 0 for name in waiting}
    sends = []
    for s in range(-1, STEPS):
        now = []
        for name, queue in waiting.items():
            while queue and sent[name] <= s + 2 and arrive[queue[0]] <= s:
                now.append((name, queue.pop(0)))
                sent[name] += 1
        sends.append(now)
    return arrivals, sends


def key_bias(length, rows):
    row = lax.broadcasted_iota(jnp.int32, (rows, 128), 0)
    lane = lax.broadcasted_iota(jnp.int32, (rows, 128), 1)
    return jnp.where((lane == 0) & (row >= length), masked_score, 0.0).astype(jnp.bfloat16)


def spread_queries(q_t):
    rows = lax.broadcasted_iota(jnp.int32, (256, 2 * q_t.shape[1]), 0)
    cols = lax.broadcasted_iota(jnp.int32, (256, 2 * q_t.shape[1]), 1)
    half = q_t.shape[1]
    two = jnp.concatenate([q_t, q_t], axis=1)
    full = jnp.concatenate([two, jnp.zeros_like(two)], axis=0)
    keep = ((rows < HD) & (cols < half)) | ((rows >= HD) & (rows < 2 * HD) & (cols >= half))
    return jnp.where(keep, full, jnp.where(rows == 2 * HD, 1.0, 0.0)).astype(jnp.bfloat16)


def self_attention_kernel(
    lens, tokens, gain, wqkv, context, keys, values, spread, acc, scores_0, scores_1, send, recv
):
    me = lax.axis_index("seq")
    core = lax.rem(me, 2)
    y = lax.rem(me // 2, 2)
    z = me // 4

    def index(dz, dy, dc):
        z_at = lax.rem(z + dz + NZ, NZ)
        y_at = y if dy == 0 else 1 - y
        c_at = core if dc == 0 else 1 - core
        return z_at * 4 + y_at * 2 + c_at

    places = {"up": index(1, 0, 0), "down": index(-1, 0, 0), "side": index(0, 1, 0), "mate": index(0, 0, 1)}
    barrier = pltpu.get_barrier_semaphore()
    for place in places.values():
        pl.semaphore_signal(barrier, inc=1, device_id={"seq": place}, device_id_type=pl.DeviceIdType.MESH)

    x = tokens[...].astype(jnp.float32)
    normed = (
        x * lax.rsqrt(jnp.mean(x * x, axis=1, keepdims=True) + epsilon) * gain[...]
    ).astype(jnp.bfloat16)
    keys[me] = jnp.dot(normed, wqkv[1], preferred_element_type=jnp.float32).astype(jnp.bfloat16)
    values[me] = jnp.dot(normed, wqkv[2], preferred_element_type=jnp.float32).T.astype(jnp.bfloat16)
    q_t = jnp.dot(normed, wqkv[0], preferred_element_type=jnp.float32).T
    pl.semaphore_wait(barrier, 4)

    numbers = iter(range(128))
    started = []

    def copy(kv, slot, place, number):
        buffer = (keys, values)[kv]
        return pltpu.make_async_remote_copy(
            src_ref=buffer.at[slot],
            dst_ref=buffer.at[slot],
            send_sem=send.at[number],
            recv_sem=recv.at[kv, slot],
            device_id={"seq": places[place]},
            device_id_type=pl.DeviceIdType.MESH,
        )

    def slot_of(line, d):
        return index(-d, 0 if line == "O" else 1, 0)

    def push(kv, slot, place):
        number = next(numbers)
        copy(kv, slot, place, number).start()
        started.append((kv, place, number))

    arrivals, sends = link_plan()
    for name, (line, d, kv) in sends[0]:
        push(kv, me, name)
    for kv in range(2):
        push(kv, me, "mate")

    spread[...] = spread_queries(q_t * (HD ** (-0.5) * math.log2(math.e)))
    acc[...] = jnp.zeros_like(acc)

    def step(s):
        for line, d, kv in arrivals[s]:
            slot = slot_of(line, d)
            copy(kv, slot, "mate", 0).wait_recv()
            push(kv, slot, "mate")
        for name, (line, d, kv) in sends[s + 1]:
            push(kv, slot_of(line, d), name)

    def chip_slot(j, dc):
        dz, dy = jnp.int32(0), jnp.int32(0)
        for k, (line, d) in enumerate(CHIPS):
            dz = jnp.where(j == k, -d, dz)
            dy = jnp.where(j == k, 0 if line == "O" else 1, dy)
        z_at = lax.rem(z + dz + NZ, NZ)
        y_at = lax.rem(y + dy, 2)
        c_at = core if dc == 0 else 1 - core
        return z_at * 4 + y_at * 2 + c_at

    def score(slot, into):
        rows = jnp.concatenate([keys[slot], key_bias(lens[slot], TOK_DEV)], axis=1)
        s = jnp.dot(rows, spread[...], preferred_element_type=jnp.float32)
        into[...] = s
        return jnp.max(s, axis=0, keepdims=True)

    def rest(slot, held, old, top):
        p = jnp.exp2(held[...] - top).astype(jnp.bfloat16)
        shrink = jnp.exp2(old - top)
        ones = jnp.ones((16, TOK_DEV), jnp.bfloat16)
        for h in range(2):
            cols = slice(h * TOK_DEV, (h + 1) * TOK_DEV)
            lhs = jnp.concatenate([values[slot, pl.ds(h * HD, HD), :], ones], axis=0)
            acc[h] = acc[h] * shrink[:, cols] + jnp.dot(lhs, p[:, cols], preferred_element_type=jnp.float32)

    def arrived(slot):
        for kv in range(2):
            copy(kv, slot, "mate", 0).wait_recv()

    start = jnp.full((1, 2 * TOK_DEV), masked_score, jnp.float32)
    mate = index(0, 0, 1)
    top = score(me, scores_0)
    arrived(mate)
    following = jnp.maximum(top, score(mate, scores_1))
    rest(me, scores_0, start, top)

    def body(j, carry):
        old, top = carry
        for at, steps in STEPS_BEFORE.items():

            @pl.when(j == at)
            def _():
                for s in steps:
                    step(s)

        here, there = chip_slot(j, 0), chip_slot(j, 1)
        later = jnp.maximum(top, score(here, scores_0))
        rest(chip_slot(j - 1, 1), scores_1, old, top)
        old, top = top, later
        arrived(there)
        later = jnp.maximum(top, score(there, scores_1))
        rest(here, scores_0, old, top)
        return top, later

    old, top = lax.fori_loop(1, len(CHIPS), body, (top, following))
    rest(chip_slot(jnp.int32(len(CHIPS) - 1), 1), scores_1, old, top)
    both = jnp.concatenate([acc[h, 0:HD, :] / acc[h, HD : HD + 1, :] for h in range(2)], axis=0)
    context[...] = both.T.astype(jnp.bfloat16)
    for kv, place, number in started:
        copy(kv, me, place, number).wait_send()


def self_attention(lens, tokens, gain, wqkv):
    vmem = pl.BlockSpec(memory_space=pltpu.VMEM)
    return pl.pallas_call(
        self_attention_kernel,
        out_shape=jax.ShapeDtypeStruct((TOK_DEV, 2 * HD), jnp.bfloat16),
        in_specs=[pl.BlockSpec(memory_space=pltpu.SMEM), vmem, vmem, vmem],
        out_specs=vmem,
        scratch_shapes=[
            pltpu.VMEM((SLOTS, TOK_DEV, 2 * HD), jnp.bfloat16),
            pltpu.VMEM((SLOTS, 2 * HD, TOK_DEV), jnp.bfloat16),
            pltpu.VMEM((256, 2 * TOK_DEV), jnp.bfloat16),
            pltpu.VMEM((2, HD + 16, TOK_DEV), jnp.float32),
            pltpu.VMEM((TOK_DEV, 2 * TOK_DEV), jnp.float32),
            pltpu.VMEM((TOK_DEV, 2 * TOK_DEV), jnp.float32),
            pltpu.SemaphoreType.DMA((72,)),
            pltpu.SemaphoreType.DMA((2, SLOTS)),
        ],
        compiler_params=pltpu.CompilerParams(
            collective_id=0, has_side_effects=True, vmem_limit_bytes=56 << 20
        ),
        name="self_attention",
    )(lens, tokens, gain, wqkv)


def cut_along(x, dim, count):
    before, after = (x.shape[:dim], x.shape[dim + 1 :])
    return jnp.moveaxis(x.reshape(*before, count, -1, *after), dim, 0)


def sent_and_summed(x, axis, dim):
    blocks = cut_along(x, dim, lax.axis_size(axis))
    arrived = lax.all_to_all(blocks, axis, split_axis=0, concat_axis=0, tiled=True)
    return arrived.astype(jnp.float32).sum(axis=0)


def sent_to_all(x, axis):
    copies = jnp.broadcast_to(x, (lax.axis_size(axis), *x.shape))
    return lax.all_to_all(copies, axis, split_axis=0, concat_axis=0, tiled=True)


def laid_out(blocks, dim):
    shape = list(blocks.shape[1:])
    shape[dim] *= blocks.shape[0]
    return jnp.moveaxis(blocks, 0, dim).reshape(shape)


def gather_directly(x, axis, dim):
    blocks = sent_to_all(x, axis)
    return laid_out(blocks, dim)


def over_copies_2(x, axis):
    everything = sent_to_all(x, axis)
    return jnp.sum(everything.astype(jnp.float32), axis=0)


def rms_norm(values, gain_vector):
    widened = values.astype(jnp.float32)
    return (
        widened
        * lax.rsqrt(jnp.mean(widened * widened, axis=-1, keepdims=True) + epsilon)
        * gain_vector
    )


def spread_heads(per_head):
    return jnp.repeat(per_head.T, HD, axis=1)


def live_within(positions, lengths, span):
    block_ids = jnp.arange(lengths.shape[0], dtype=jnp.int32)
    owners = positions // span
    lengths_here = jnp.sum(
        jnp.where(owners[:, None] == block_ids[None, :], lengths[None, :], 0), axis=1
    )
    return positions % span < lengths_here


def live_keys(positions, pad_lengths):
    return live_within(positions, pad_lengths, TOK_DEV)


def feed_forward(normed_in, ffn_in, ffn_out):
    gate_proj = jnp.dot(normed_in, ffn_in[0], preferred_element_type=jnp.float32)
    up_proj = jnp.dot(normed_in, ffn_in[1], preferred_element_type=jnp.float32)
    activated = (jax.nn.gelu(gate_proj, approximate=True) * up_proj).astype(jnp.bfloat16)
    return jnp.dot(activated, ffn_out, preferred_element_type=jnp.float32)


def local(
    tokens,
    norm_attn,
    self_qkv,
    self_out,
    norm_ffn,
    ffn_in,
    ffn_out,
    norm_final,
    pad_lengths,
    targets,
    target_lengths,
    norm_cross,
    cross_query,
    cross_kv,
    cross_out,
):
    row_count = tokens.shape[0]
    heads_here = self_qkv.shape[2] // HD
    scaling = HD ** (-0.5)
    context = self_attention(pad_lengths, tokens, norm_attn.reshape(1, D), self_qkv)
    attn_part = jnp.dot(context, self_out, preferred_element_type=jnp.float32)
    share = row_count // lax.axis_size("head")
    first = lax.axis_index("head") * share
    token_share = lax.dynamic_slice_in_dim(tokens, first, share, 0).astype(jnp.float32)
    hidden_share = token_share + sent_and_summed(attn_part.astype(jnp.bfloat16), "head", 0)
    ffn_normed = gather_directly(rms_norm(hidden_share, norm_ffn).astype(jnp.bfloat16), "head", 0)
    ffn_part = feed_forward(ffn_normed, ffn_in, ffn_out)
    final_share = hidden_share + sent_and_summed(ffn_part.astype(jnp.bfloat16), "head", 0)
    encoded = gather_directly(rms_norm(final_share, norm_final).astype(jnp.bfloat16), "head", 0)
    target_rows = targets.shape[0]
    cross_normed = rms_norm(targets, norm_cross).astype(jnp.bfloat16)
    cross_queries = jnp.dot(cross_normed, cross_query, preferred_element_type=jnp.float32).astype(
        jnp.bfloat16
    )
    cross_keys = jnp.dot(encoded, cross_kv[0], preferred_element_type=jnp.float32).astype(
        jnp.bfloat16
    )
    cross_values = jnp.dot(encoded, cross_kv[1], preferred_element_type=jnp.float32).astype(
        jnp.bfloat16
    )
    cross_heads = cross_queries.reshape(target_rows, heads_here, HD)
    keys_split = cross_keys.reshape(row_count, heads_here, HD)
    values_split = cross_values.reshape(row_count, heads_here, HD)
    positions = lax.axis_index("seq") * row_count + jnp.arange(row_count, dtype=jnp.int32)
    live_here = live_keys(positions, pad_lengths)
    cross_scores = (
        jnp.einsum("qhd,khd->hqk", cross_heads, keys_split, preferred_element_type=jnp.float32)
        * scaling
    )
    cross_scores = jnp.where(live_here[None, None, :], cross_scores, masked_score)
    local_max = jnp.max(cross_scores, axis=-1)
    weights = jnp.where(
        live_here[None, None, :], jnp.exp(cross_scores - local_max[:, :, None]), 0.0
    )
    local_sum = jnp.sum(weights, axis=-1)
    local_mixed = jnp.einsum(
        "hqk,khd->qhd",
        weights.astype(jnp.bfloat16),
        values_split,
        preferred_element_type=jnp.float32,
    )
    shares = lax.axis_size("seq")
    share_rows = target_rows // shares
    tops_sums = jnp.concatenate([local_max, local_sum], axis=0)
    tops_sums = tops_sums.reshape(2 * heads_here, shares, share_rows).transpose(1, 0, 2)
    tops_sums = jnp.pad(tops_sums.reshape(shares, 1, -1), ((0, 0), (0, 0), (0, 128 - 2 * heads_here * share_rows)))
    parts = jnp.concatenate([local_mixed.reshape(shares, share_rows, heads_here * HD), tops_sums], axis=1)
    parts = lax.all_to_all(parts, "seq", split_axis=0, concat_axis=0, tiled=True)
    stats = parts[:, share_rows, : 2 * heads_here * share_rows].reshape(shares, 2, heads_here, share_rows)
    tops, sums = stats[:, 0], stats[:, 1]
    factors = jnp.exp(tops - jnp.max(tops, axis=0, keepdims=True))
    total = jnp.sum(sums * factors, axis=0)
    spread = jnp.repeat(factors.transpose(0, 2, 1), HD, axis=2)
    mixed_rows = jnp.sum(parts[:, :share_rows] * spread, axis=0)
    first_row = lax.axis_index("seq") * share_rows
    cross_context = (mixed_rows / spread_heads(total)).astype(jnp.bfloat16)
    cross_part = jnp.dot(cross_context, cross_out, preferred_element_type=jnp.float32)
    cross_total = over_copies_2(cross_part.astype(jnp.bfloat16), "head").astype(jnp.float32)
    slots = first_row + jnp.arange(share_rows, dtype=jnp.int32)
    target_live = live_within(slots, target_lengths, TGT_LEN)
    target_share = lax.dynamic_slice_in_dim(targets, first_row, share_rows, 0).astype(jnp.float32)
    decoded_share = (target_share + jnp.where(target_live[:, None], cross_total, 0.0)).astype(
        jnp.bfloat16
    )
    decoded = gather_directly(decoded_share, "seq", 0)
    return (encoded, decoded)


def solution(mesh):
    in_specs = (
        P("seq", None),
        P(),
        P(None, None, "head"),
        P("head", None),
        P(),
        P(None, None, "head"),
        P("head", None),
        P(),
        P(),
        P(),
        P(),
        P(),
        P(None, "head"),
        P(None, None, "head"),
        P("head", None),
    )
    out_specs = (P("seq", None), P())
    return jax.shard_map(local, mesh=mesh, in_specs=in_specs, out_specs=out_specs, check_vma=False)
```

```python
import functools
import math

import jax
import jax.numpy as jnp
from jax import lax
from jax.experimental import pallas as pl
from jax.experimental.pallas import tpu as pltpu
from jax.sharding import Mesh
from jax.sharding import PartitionSpec as P

D = 1024
HD = 64
TOK_DEV = 512
TGT_LEN = 128


epsilon = 1e-06
masked_score = -1e30


NZ = 8
SLOTS = 32
UP = (("O", 0, 0), ("O", 0, 1), ("O", 1, 0), ("O", 1, 1), ("O", 2, 0), ("O", 2, 1), ("P", 2, 0), ("O", 3, 0), ("P", 2, 1), ("P", 3, 0))
DOWN = (("O", 0, 1), ("O", 0, 0), ("O", -1, 1), ("O", -1, 0), ("O", -2, 1), ("O", -2, 0), ("P", -2, 1), ("O", -3, 1), ("P", -3, 1), ("P", -2, 0))
SIDE = (("O", 0, 0), ("O", 0, 1), ("O", 1, 0), ("O", -1, 1), ("O", 2, 0), ("O", -2, 1), ("O", 2, 1), ("O", -2, 0), ("O", 1, 1), ("O", -1, 0))
CHIPS = (("O", 0), ("O", 1), ("O", -1), ("P", 0), ("O", 2), ("O", -2), ("O", 3), ("O", -3), ("P", 2), ("P", -2), ("O", 4), ("P", 1), ("P", 3), ("P", -1), ("P", -3), ("P", 4))
STEPS_BEFORE = {1: (0, 1), 3: (2,), 4: (3,), 6: (4, 5), 8: (6,), 9: (7,), 11: (8,), 13: (9,)}
STEPS = 10
WEIGHT_STEPS_BEFORE = {3: (("pass", 0),), 9: (("pass", 1), ("end", 0)), 13: (("pass", 2),)}
FF_DEV = 352
ROWS = 128


def link_plan():
    arrive = {("O", 0, 0): -1, ("O", 0, 1): -1}
    arrivals = []
    for s in range(STEPS):
        new = [(UP[s][0], UP[s][1] + 1, UP[s][2]), (DOWN[s][0], DOWN[s][1] - 1, DOWN[s][2])]
        new.append(("P", SIDE[s][1], SIDE[s][2]))
        arrive.update({item: s for item in new})
        arrivals.append(new)
    waiting = {"up": list(UP), "down": list(DOWN), "side": list(SIDE)}
    sent = {name: 0 for name in waiting}
    sends = []
    for s in range(-1, STEPS):
        now = []
        for name, queue in waiting.items():
            while queue and sent[name] <= s + 2 and arrive[queue[0]] <= s:
                now.append((name, queue.pop(0)))
                sent[name] += 1
        sends.append(now)
    return arrivals, sends


def key_bias(length, rows):
    row = lax.broadcasted_iota(jnp.int32, (rows, 128), 0)
    lane = lax.broadcasted_iota(jnp.int32, (rows, 128), 1)
    return jnp.where((lane == 0) & (row >= length), masked_score, 0.0).astype(jnp.bfloat16)


def spread_queries(q_t):
    rows = lax.broadcasted_iota(jnp.int32, (256, 2 * q_t.shape[1]), 0)
    cols = lax.broadcasted_iota(jnp.int32, (256, 2 * q_t.shape[1]), 1)
    half = q_t.shape[1]
    two = jnp.concatenate([q_t, q_t], axis=1)
    full = jnp.concatenate([two, jnp.zeros_like(two)], axis=0)
    keep = ((rows < HD) & (cols < half)) | ((rows >= HD) & (rows < 2 * HD) & (cols >= half))
    return jnp.where(keep, full, jnp.where(rows == 2 * HD, 1.0, 0.0)).astype(jnp.bfloat16)


def normalised(x, gain):
    return x * lax.rsqrt(jnp.mean(x * x, axis=1, keepdims=True) + epsilon) * gain


def dot32(a, b):
    return jnp.dot(a, b, preferred_element_type=jnp.float32)


def layer_kernel(
    lens,
    tokens,
    gain_attn,
    wqkv,
    gain_ffn,
    gain_final,
    gain_cross,
    wo_hbm,
    wi_hbm,
    wf_hbm,
    targets_hbm,
    wcq_hbm,
    wckv_hbm,
    encoded,
    mixed,
    stats,
    keys,
    values,
    spread,
    acc,
    scores_0,
    scores_1,
    wo,
    wi,
    wf,
    targets,
    wcq,
    wckv,
    wo_all,
    wi_all,
    wf_all,
    ctx,
    ctx_in,
    hidden,
    part,
    out_1,
    in_1,
    out_2,
    in_2,
    enc,
    cross_spread,
    cross_values,
    local_sem,
    send,
    recv,
    recv_w,
    recv_c,
    recv_y,
    recv_e,
):
    me = lax.axis_index("seq")
    core = lax.rem(me, 2)
    y = lax.rem(me // 2, 2)
    z = me // 4
    head = lax.axis_index("head")
    x = lax.rem(head, 4)
    yh = head // 4

    def index(dz, dy, dc):
        z_at = lax.rem(z + dz + NZ, NZ)
        y_at = y if dy == 0 else 1 - y
        c_at = core if dc == 0 else 1 - core
        return z_at * 4 + y_at * 2 + c_at

    places = {
        "up": {"seq": index(1, 0, 0)},
        "down": {"seq": index(-1, 0, 0)},
        "side": {"seq": index(0, 1, 0)},
        "mate": {"seq": index(0, 0, 1)},
        "right": {"head": yh * 4 + lax.rem(x + 1, 4)},
        "left": {"head": yh * 4 + lax.rem(x + 3, 4)},
        "across": {"head": yh * 4 + lax.rem(x + 2, 4)},
        "partner": {"head": (1 - yh) * 4 + x},
    }
    barrier = pltpu.get_barrier_semaphore()
    for place in places.values():
        pl.semaphore_signal(barrier, inc=1, device_id=place, device_id_type=pl.DeviceIdType.MESH)

    loads = {
        "wo": pltpu.make_async_copy(wo_hbm, wo, local_sem.at[0]),
        "wi": pltpu.make_async_copy(wi_hbm, wi, local_sem.at[1]),
        "wf": pltpu.make_async_copy(wf_hbm, wf, local_sem.at[2]),
        "targets": pltpu.make_async_copy(targets_hbm, targets, local_sem.at[3]),
        "wcq": pltpu.make_async_copy(wcq_hbm, wcq, local_sem.at[4]),
        "wckv": pltpu.make_async_copy(wckv_hbm, wckv, local_sem.at[5]),
    }
    for load in loads.values():
        load.start()

    normed = normalised(tokens[...].astype(jnp.float32), gain_attn[...]).astype(jnp.bfloat16)
    keys[me] = dot32(normed, wqkv[1]).astype(jnp.bfloat16)
    values[me] = dot32(normed, wqkv[2]).T.astype(jnp.bfloat16)
    q_t = dot32(normed, wqkv[0]).T
    pl.semaphore_wait(barrier, len(places))

    numbers = iter(range(256))
    started = []

    def remote(source, target, number, arrival, place):
        return pltpu.make_async_remote_copy(
            src_ref=source,
            dst_ref=target,
            send_sem=send.at[number],
            recv_sem=arrival,
            device_id=places[place],
            device_id_type=pl.DeviceIdType.MESH,
        )

    def go(source, target, arrival, place, alike=None):
        number = next(numbers)
        remote(source, target, number, arrival, place).start()
        started.append((number, alike or (lambda: source)))

    def block_copy(kv, slot):
        buffer = (keys, values)[kv]
        return buffer.at[slot], buffer.at[slot], recv.at[kv, slot]

    def wait_block(kv, slot):
        source, target, arrival = block_copy(kv, slot)
        remote(source, target, 0, arrival, "mate").wait_recv()

    def push(kv, slot, place):
        go(*block_copy(kv, slot), place, lambda: (keys, values)[kv].at[0])

    def slot_of(line, d):
        return index(-d, 0 if line == "O" else 1, 0)

    arrivals, sends = link_plan()
    for name, (line, d, kv) in sends[0]:
        push(kv, me, name)
    for kv in range(2):
        push(kv, me, "mate")

    def piece(item, slot, which, c):
        own, gathered = ((wo, wo_all), (wi, wi_all), (wf, wf_all))[item]
        ref = own if slot is None else gathered.at[slot]
        if item == 0:
            first, size = ((0, 64), (0, 32), (32, 32))[which]
            return ref.at[pl.ds(pl.multiple_of(c * 64 + first, 32), size), :]
        if item == 1:
            first, size = ((0, D), (0, D // 2), (D // 2, D // 2))[which]
            return ref.at[c, pl.ds(first, size), :]
        first, size = ((0, 176), (0, 96), (96, 80))[which]
        return ref.at[pl.ds(pl.multiple_of(c * 176 + first, 16), size), :]

    def wait_piece(item, slot, which, k, c):
        ref = piece(item, slot, which, c)
        remote(ref, ref, 0, recv_w.at[item, k], "mate").wait_recv()

    def send_piece(item, slot, slot_there, which, k, to):
        source, target = piece(item, slot, which, core), piece(item, slot_there, which, core)
        go(source, target, recv_w.at[item, k], to, lambda: piece(item, 0, which, 0))

    def weights_start(item):
        loads[("wo", "wi", "wf")[item]].wait()
        for slot, to in ((0, "right"), (1, "left")):
            send_piece(item, None, slot, 0, slot, to)

    def weights_pass(item):
        for slot, half, onward in ((0, 1, "right"), (1, 2, "left")):
            wait_piece(item, slot, 0, slot, core)
            send_piece(item, slot, 2, half, 1 + half, onward)
            send_piece(item, slot, slot, 0, 4 + slot, "mate")

    def weights_end(item):
        for half in (1, 2):
            wait_piece(item, 2, half, 1 + half, core)
            send_piece(item, 2, 2, half, 5 + half, "mate")

    def weights_here(item):
        for slot in (0, 1):
            wait_piece(item, slot, 0, 4 + slot, 1 - core)
        for half in (1, 2):
            wait_piece(item, 2, half, 5 + half, 1 - core)

    for item in range(3):
        weights_start(item)

    spread[...] = spread_queries(q_t * (HD ** (-0.5) * math.log2(math.e)))
    acc[...] = jnp.zeros_like(acc)
    for name in ("targets", "wcq", "wckv"):
        loads[name].wait()
    cross_normed = normalised(targets[...].astype(jnp.float32), gain_cross[...]).astype(jnp.bfloat16)
    cross_spread[...] = spread_queries(
        dot32(cross_normed, wcq[...]).T * (HD ** (-0.5) * math.log2(math.e))
    )

    def step(s):
        for line, d, kv in arrivals[s]:
            slot = slot_of(line, d)
            wait_block(kv, slot)
            push(kv, slot, "mate")
        for name, (line, d, kv) in sends[s + 1]:
            push(kv, slot_of(line, d), name)

    def chip_slot(j, dc):
        dz, dy = jnp.int32(0), jnp.int32(0)
        for k, (line, d) in enumerate(CHIPS):
            dz = jnp.where(j == k, -d, dz)
            dy = jnp.where(j == k, 0 if line == "O" else 1, dy)
        z_at = lax.rem(z + dz + NZ, NZ)
        y_at = lax.rem(y + dy, 2)
        c_at = core if dc == 0 else 1 - core
        return z_at * 4 + y_at * 2 + c_at

    def score(block, length, queries, into):
        rows = jnp.concatenate([block, key_bias(length, TOK_DEV)], axis=1)
        s = dot32(rows, queries[...])
        into[...] = s
        return jnp.max(s, axis=0, keepdims=True)

    def own_score(slot, into):
        return score(keys[slot], lens[slot], spread, into)

    def rest(block, held, old, top):
        p = jnp.exp2(held[...] - top).astype(jnp.bfloat16)
        shrink = jnp.exp2(old - top)
        ones = jnp.ones((16, TOK_DEV), jnp.bfloat16)
        for h in range(2):
            cols = slice(h * TOK_DEV, (h + 1) * TOK_DEV)
            lhs = jnp.concatenate([block[pl.ds(h * HD, HD), :], ones], axis=0)
            acc[h] = acc[h] * shrink[:, cols] + dot32(lhs, p[:, cols])

    def arrived(slot):
        for kv in range(2):
            wait_block(kv, slot)

    start = jnp.full((1, 2 * TOK_DEV), masked_score, jnp.float32)
    mate = index(0, 0, 1)
    top = own_score(me, scores_0)
    arrived(mate)
    following = jnp.maximum(top, own_score(mate, scores_1))
    rest(values.at[me], scores_0, start, top)

    def body(j, carry):
        old, top = carry
        for at in sorted({*STEPS_BEFORE, *WEIGHT_STEPS_BEFORE}):

            @pl.when(j == at)
            def _():
                for s in STEPS_BEFORE.get(at, ()):
                    step(s)
                for what, item in WEIGHT_STEPS_BEFORE.get(at, ()):
                    (weights_pass if what == "pass" else weights_end)(item)

        here, there = chip_slot(j, 0), chip_slot(j, 1)
        later = jnp.maximum(top, own_score(here, scores_0))
        rest(values.at[chip_slot(j - 1, 1)], scores_1, old, top)
        old, top = top, later
        arrived(there)
        later = jnp.maximum(top, own_score(there, scores_1))
        rest(values.at[here], scores_0, old, top)
        return top, later

    old, top = lax.fori_loop(1, len(CHIPS), body, (top, following))
    rest(values.at[chip_slot(jnp.int32(len(CHIPS) - 1), 1)], scores_1, old, top)
    both = jnp.concatenate([acc[h, 0:HD, :] / acc[h, HD : HD + 1, :] for h in range(2)], axis=0)
    ctx[...] = both.T.astype(jnp.bfloat16)

    def ctx_rows(at):
        return ctx.at[pl.ds(pl.multiple_of(lax.rem(at, 4) * ROWS, ROWS), ROWS), :]

    for g, (to, at) in enumerate((("right", x + 1), ("left", x + 3), ("across", x + 2))):
        go(ctx_rows(at), ctx_in.at[g], recv_c.at[g], to)
    weights_here(0)
    weights_end(1)
    total = dot32(ctx_rows(x)[...], wo[...])
    for g in range(3):
        remote(ctx_in.at[g], ctx_in.at[g], 0, recv_c.at[g], "mate").wait_recv()
        total += dot32(ctx_in[g], wo_all[g])
    out_1[...] = total.astype(jnp.bfloat16)
    go(out_1, in_1, recv_y.at[0], "partner")
    total += tokens[pl.ds(pl.multiple_of(x * ROWS, ROWS), ROWS), :].astype(jnp.float32)
    weights_end(2)
    weights_here(1)
    weights_here(2)
    remote(out_1, in_1, 0, recv_y.at[0], "partner").wait_recv()
    total += in_1[...].astype(jnp.float32)
    hidden[...] = total
    ffn_normed = normalised(total, gain_ffn[...]).astype(jnp.bfloat16)
    ffn = jnp.zeros((ROWS, D), jnp.float32)
    for g in range(4):
        gate_w, up_w, down_w = (
            (wi[0], wi[1], wf[...]) if g == 3 else (wi_all[g, 0], wi_all[g, 1], wf_all[g])
        )
        gate = dot32(ffn_normed, gate_w)
        up = dot32(ffn_normed, up_w)
        activated = (jax.nn.gelu(gate, approximate=True) * up).astype(jnp.bfloat16)
        ffn += dot32(activated, down_w)
    part[...] = ffn
    share_rows = ROWS // 2
    mine = pl.ds(pl.multiple_of(yh * share_rows, share_rows), share_rows)
    other = pl.ds(pl.multiple_of((1 - yh) * share_rows, share_rows), share_rows)
    out_2[...] = part[other, :].astype(jnp.bfloat16)
    go(out_2, in_2, recv_y.at[1], "partner")
    final = hidden[mine, :] + part[mine, :]
    remote(out_2, in_2, 0, recv_y.at[1], "partner").wait_recv()
    final += in_2[...].astype(jnp.float32)

    def share(dx, dy):
        return lax.rem(x + dx + 4, 4) * 2 + (yh if dy == 0 else 1 - yh)

    enc[share(0, 0)] = normalised(final, gain_final[...]).astype(jnp.bfloat16)

    def rows_of(at, half):
        if half is None:
            return enc.at[at]
        return enc.at[at, pl.ds(half * 32, 32), :]

    def send_share(at, half, to):
        go(rows_of(at, half), rows_of(at, half), recv_e.at[at, half or 0], to)

    def wait_share(at, half):
        ref = rows_of(at, half)
        remote(ref, ref, 0, recv_e.at[at, half or 0], "mate").wait_recv()

    for to in ("partner", "right", "left"):
        send_share(share(0, 0), None, to)
    for dy in (0, 1):
        if dy:
            wait_share(share(0, 1), None)
            for to in ("right", "left"):
                send_share(share(0, 1), None, to)
        for dx, half, to in ((-1, 0, "right"), (1, 1, "left")):
            wait_share(share(dx, dy), None)
            send_share(share(dx, dy), half, to)
    for dy in (0, 1):
        for half in (0, 1):
            wait_share(share(2, dy), half)

    whole = enc[...].reshape(TOK_DEV, D)
    encoded[...] = whole
    cross_keys = dot32(whole, wckv[0]).astype(jnp.bfloat16)
    cross_values[...] = dot32(whole, wckv[1]).T.astype(jnp.bfloat16)
    acc[...] = jnp.zeros_like(acc)
    cross_top = score(cross_keys, lens[me], cross_spread, scores_0)
    rest(cross_values, scores_0, start, cross_top)
    mixed[...] = jnp.concatenate([acc[h, 0:HD, :] for h in range(2)], axis=0).T
    stats[...] = jnp.concatenate(
        [cross_top[:, :TOK_DEV], cross_top[:, TOK_DEV:], acc[0, HD : HD + 1, :], acc[1, HD : HD + 1, :]]
        + [jnp.zeros((4, TOK_DEV), jnp.float32)],
        axis=0,
    )
    for number, alike in started:
        remote(alike(), alike(), number, recv_y.at[0], "mate").wait_send()


def layer(lens, tokens, gains, wqkv, wo, wi, wf, targets, wcq, wckv):
    vmem = pl.BlockSpec(memory_space=pltpu.VMEM)
    hbm = pl.BlockSpec(memory_space=pl.ANY)
    b16, f32 = jnp.bfloat16, jnp.float32
    gain_attn, gain_ffn, gain_final, gain_cross = (g.reshape(1, D) for g in gains)
    scratch = [
        ((SLOTS, TOK_DEV, 2 * HD), b16),
        ((SLOTS, 2 * HD, TOK_DEV), b16),
        ((256, 2 * TOK_DEV), b16),
        ((2, HD + 16, TOK_DEV), f32),
        ((TOK_DEV, 2 * TOK_DEV), f32),
        ((TOK_DEV, 2 * TOK_DEV), f32),
        (wo.shape, b16),
        (wi.shape, b16),
        (wf.shape, b16),
        (targets.shape, b16),
        (wcq.shape, b16),
        (wckv.shape, b16),
        ((3, *wo.shape), b16),
        ((3, *wi.shape), b16),
        ((3, *wf.shape), b16),
        ((TOK_DEV, 2 * HD), b16),
        ((3, ROWS, 2 * HD), b16),
        ((ROWS, D), f32),
        ((ROWS, D), f32),
        ((ROWS, D), b16),
        ((ROWS, D), b16),
        ((ROWS // 2, D), b16),
        ((ROWS // 2, D), b16),
        ((8, ROWS // 2, D), b16),
        ((256, 2 * TOK_DEV), b16),
        ((2 * HD, TOK_DEV), b16),
    ]
    sems = [(8,), (160,), (2, SLOTS), (3, 8), (4,), (2,), (8, 2)]
    return pl.pallas_call(
        layer_kernel,
        out_shape=(
            jax.ShapeDtypeStruct((TOK_DEV, D), b16),
            jax.ShapeDtypeStruct((TOK_DEV, 2 * HD), f32),
            jax.ShapeDtypeStruct((8, TOK_DEV), f32),
        ),
        in_specs=[pl.BlockSpec(memory_space=pltpu.SMEM)] + [vmem] * 6 + [hbm] * 6,
        out_specs=(vmem, vmem, vmem),
        scratch_shapes=[pltpu.VMEM(*s) for s in scratch] + [pltpu.SemaphoreType.DMA(s) for s in sems],
        compiler_params=pltpu.CompilerParams(
            collective_id=0, has_side_effects=True, vmem_limit_bytes=60 << 20
        ),
        name="layer",
    )(lens, tokens, gain_attn, wqkv, gain_ffn, gain_final, gain_cross, wo, wi, wf, targets, wcq, wckv)


def sent_to_all(x, axis):
    copies = jnp.broadcast_to(x, (lax.axis_size(axis), *x.shape))
    return lax.all_to_all(copies, axis, split_axis=0, concat_axis=0, tiled=True)


def laid_out(blocks, dim):
    shape = list(blocks.shape[1:])
    shape[dim] *= blocks.shape[0]
    return jnp.moveaxis(blocks, 0, dim).reshape(shape)


def gather_directly(x, axis, dim):
    blocks = sent_to_all(x, axis)
    return laid_out(blocks, dim)


def over_copies_2(x, axis):
    everything = sent_to_all(x, axis)
    return jnp.sum(everything.astype(jnp.float32), axis=0)


def spread_heads(per_head):
    return jnp.repeat(per_head.T, HD, axis=1)


def live_within(positions, lengths, span):
    block_ids = jnp.arange(lengths.shape[0], dtype=jnp.int32)
    owners = positions // span
    lengths_here = jnp.sum(
        jnp.where(owners[:, None] == block_ids[None, :], lengths[None, :], 0), axis=1
    )
    return positions % span < lengths_here


def local(
    tokens,
    norm_attn,
    self_qkv,
    self_out,
    norm_ffn,
    ffn_in,
    ffn_out,
    norm_final,
    pad_lengths,
    targets,
    target_lengths,
    norm_cross,
    cross_query,
    cross_kv,
    cross_out,
):
    heads_here = self_qkv.shape[2] // HD
    target_rows = targets.shape[0]
    encoded, mixed, stats = layer(
        pad_lengths,
        tokens,
        (norm_attn, norm_ffn, norm_final, norm_cross),
        self_qkv,
        self_out,
        ffn_in,
        ffn_out,
        targets,
        cross_query,
        cross_kv,
    )
    shares = lax.axis_size("seq")
    share_rows = target_rows // shares
    tops_sums = stats[: 2 * heads_here].reshape(2 * heads_here, shares, share_rows).transpose(1, 0, 2)
    tops_sums = jnp.pad(tops_sums.reshape(shares, 1, -1), ((0, 0), (0, 0), (0, 128 - 2 * heads_here * share_rows)))
    parts = jnp.concatenate([mixed.reshape(shares, share_rows, heads_here * HD), tops_sums], axis=1)
    parts = lax.all_to_all(parts, "seq", split_axis=0, concat_axis=0, tiled=True)
    arrived = parts[:, share_rows, : 2 * heads_here * share_rows].reshape(shares, 2, heads_here, share_rows)
    tops, sums = arrived[:, 0], arrived[:, 1]
    factors = jnp.exp2(tops - jnp.max(tops, axis=0, keepdims=True))
    total = jnp.sum(sums * factors, axis=0)
    spread = jnp.repeat(factors.transpose(0, 2, 1), HD, axis=2)
    mixed_rows = jnp.sum(parts[:, :share_rows] * spread, axis=0)
    first_row = lax.axis_index("seq") * share_rows
    cross_context = (mixed_rows / spread_heads(total)).astype(jnp.bfloat16)
    cross_part = jnp.dot(cross_context, cross_out, preferred_element_type=jnp.float32)
    cross_total = over_copies_2(cross_part.astype(jnp.bfloat16), "head").astype(jnp.float32)
    slots = first_row + jnp.arange(share_rows, dtype=jnp.int32)
    target_live = live_within(slots, target_lengths, TGT_LEN)
    target_share = lax.dynamic_slice_in_dim(targets, first_row, share_rows, 0).astype(jnp.float32)
    decoded_share = (target_share + jnp.where(target_live[:, None], cross_total, 0.0)).astype(
        jnp.bfloat16
    )
    decoded = gather_directly(decoded_share, "seq", 0)
    return (encoded, decoded)


def solution(mesh):
    in_specs = (
        P("seq", None),
        P(),
        P(None, None, "head"),
        P("head", None),
        P(),
        P(None, None, "head"),
        P("head", None),
        P(),
        P(),
        P(),
        P(),
        P(),
        P(None, "head"),
        P(None, None, "head"),
        P("head", None),
    )
    out_specs = (P("seq", None), P())
    return jax.shard_map(local, mesh=mesh, in_specs=in_specs, out_specs=out_specs, check_vma=False)
```

```python
import functools
import math

import jax
import jax.numpy as jnp
from jax import lax
from jax.experimental import pallas as pl
from jax.experimental.pallas import tpu as pltpu
from jax.sharding import Mesh
from jax.sharding import PartitionSpec as P

D = 1024
HD = 64
TOK_DEV = 512


epsilon = 1e-06
masked_score = -1e30


NZ = 8
SLOTS = 32
UP = (("O", 0, 0), ("O", 0, 1), ("O", 1, 0), ("O", 1, 1), ("O", 2, 0), ("O", 2, 1), ("P", 2, 0), ("O", 3, 0), ("P", 2, 1), ("P", 3, 0))
DOWN = (("O", 0, 1), ("O", 0, 0), ("O", -1, 1), ("O", -1, 0), ("O", -2, 1), ("O", -2, 0), ("P", -2, 1), ("O", -3, 1), ("P", -3, 1), ("P", -2, 0))
SIDE = (("O", 0, 0), ("O", 0, 1), ("O", 1, 0), ("O", -1, 1), ("O", 2, 0), ("O", -2, 1), ("O", 2, 1), ("O", -2, 0), ("O", 1, 1), ("O", -1, 0))
CHIPS = (("O", 0), ("O", 1), ("O", -1), ("P", 0), ("O", 2), ("O", -2), ("O", 3), ("O", -3), ("P", 2), ("P", -2), ("O", 4), ("P", 1), ("P", 3), ("P", -1), ("P", -3), ("P", 4))
STEPS_BEFORE = {1: (0, 1), 3: (2,), 4: (3,), 6: (4, 5), 8: (6,), 9: (7,), 11: (8,), 13: (9,)}
STEPS = 10
WEIGHT_STEPS_BEFORE = {3: (("pass", 0),), 9: (("pass", 1), ("end", 0)), 13: (("pass", 2),), 15: (("pass", 3),)}
FF_DEV = 352
ROWS = 128


def link_plan():
    arrive = {("O", 0, 0): -1, ("O", 0, 1): -1}
    arrivals = []
    for s in range(STEPS):
        new = [(UP[s][0], UP[s][1] + 1, UP[s][2]), (DOWN[s][0], DOWN[s][1] - 1, DOWN[s][2])]
        new.append(("P", SIDE[s][1], SIDE[s][2]))
        arrive.update({item: s for item in new})
        arrivals.append(new)
    waiting = {"up": list(UP), "down": list(DOWN), "side": list(SIDE)}
    sent = {name: 0 for name in waiting}
    sends = []
    for s in range(-1, STEPS):
        now = []
        for name, queue in waiting.items():
            while queue and sent[name] <= s + 2 and arrive[queue[0]] <= s:
                now.append((name, queue.pop(0)))
                sent[name] += 1
        sends.append(now)
    return arrivals, sends


def key_bias(length, rows):
    row = lax.broadcasted_iota(jnp.int32, (rows, 128), 0)
    lane = lax.broadcasted_iota(jnp.int32, (rows, 128), 1)
    return jnp.where((lane == 0) & (row >= length), masked_score, 0.0).astype(jnp.bfloat16)


def spread_queries(q_t):
    rows = lax.broadcasted_iota(jnp.int32, (256, 2 * q_t.shape[1]), 0)
    cols = lax.broadcasted_iota(jnp.int32, (256, 2 * q_t.shape[1]), 1)
    half = q_t.shape[1]
    two = jnp.concatenate([q_t, q_t], axis=1)
    full = jnp.concatenate([two, jnp.zeros_like(two)], axis=0)
    keep = ((rows < HD) & (cols < half)) | ((rows >= HD) & (rows < 2 * HD) & (cols >= half))
    return jnp.where(keep, full, jnp.where(rows == 2 * HD, 1.0, 0.0)).astype(jnp.bfloat16)


def normalised(x, gain):
    return x * lax.rsqrt(jnp.mean(x * x, axis=1, keepdims=True) + epsilon) * gain


def dot32(a, b):
    return jnp.dot(a, b, preferred_element_type=jnp.float32)


def layer_kernel(
    lens,
    tokens,
    gain_attn,
    wqkv,
    gain_ffn,
    gain_final,
    gain_cross,
    wo_hbm,
    wi_hbm,
    wf_hbm,
    targets_hbm,
    wcq_hbm,
    wckv_hbm,
    wco_hbm,
    target_lens,
    encoded,
    decoded,
    keys,
    values,
    spread,
    acc,
    scores_0,
    scores_1,
    wo,
    wi,
    wf,
    targets,
    wcq,
    wckv,
    wo_all,
    wi_all,
    wf_all,
    ctx,
    ctx_in,
    hidden,
    part,
    out_1,
    in_1,
    out_2,
    in_2,
    enc,
    cross_spread,
    cross_values,
    wco_all,
    o_all,
    s_all,
    o_mate,
    s_mate,
    o_half,
    s_half,
    o_side,
    s_side,
    o_rows,
    s_rows,
    o_line,
    s_line,
    c_all,
    sum_out,
    sum_in,
    dec,
    local_sem,
    send,
    recv,
    recv_w,
    recv_c,
    recv_y,
    recv_e,
    recv_m,
    recv_l,
    recv_h,
    recv_d,
):
    me = lax.axis_index("seq")
    core = lax.rem(me, 2)
    y = lax.rem(me // 2, 2)
    z = me // 4
    head = lax.axis_index("head")
    x = lax.rem(head, 4)
    yh = head // 4

    def index(dz, dy, dc):
        z_at = lax.rem(z + dz + NZ, NZ)
        y_at = y if dy == 0 else 1 - y
        c_at = core if dc == 0 else 1 - core
        return z_at * 4 + y_at * 2 + c_at

    places = {
        "up": {"seq": index(1, 0, 0)},
        "down": {"seq": index(-1, 0, 0)},
        "side": {"seq": index(0, 1, 0)},
        "mate": {"seq": index(0, 0, 1)},
        "right": {"head": yh * 4 + lax.rem(x + 1, 4)},
        "left": {"head": yh * 4 + lax.rem(x + 3, 4)},
        "across": {"head": yh * 4 + lax.rem(x + 2, 4)},
        "partner": {"head": (1 - yh) * 4 + x},
    }
    for dz in range(2, NZ - 1):
        places[dz] = {"seq": index(dz, 0, 0)}
    line_place = {1: "up", NZ - 1: "down", **{dz: dz for dz in range(2, NZ - 1)}}
    barrier = pltpu.get_barrier_semaphore()
    for place in places.values():
        pl.semaphore_signal(barrier, inc=1, device_id=place, device_id_type=pl.DeviceIdType.MESH)

    loads = {
        "wo": pltpu.make_async_copy(wo_hbm, wo, local_sem.at[0]),
        "wi": pltpu.make_async_copy(wi_hbm, wi, local_sem.at[1]),
        "wf": pltpu.make_async_copy(wf_hbm, wf, local_sem.at[2]),
        "targets": pltpu.make_async_copy(targets_hbm, targets, local_sem.at[3]),
        "wcq": pltpu.make_async_copy(wcq_hbm, wcq, local_sem.at[4]),
        "wckv": pltpu.make_async_copy(wckv_hbm, wckv, local_sem.at[5]),
        "wco": pltpu.make_async_copy(wco_hbm, wco_all.at[3], local_sem.at[6]),
    }
    for load in loads.values():
        load.start()

    normed = normalised(tokens[...].astype(jnp.float32), gain_attn[...]).astype(jnp.bfloat16)
    keys[me] = dot32(normed, wqkv[1]).astype(jnp.bfloat16)
    values[me] = dot32(normed, wqkv[2]).T.astype(jnp.bfloat16)
    q_t = dot32(normed, wqkv[0]).T
    pl.semaphore_wait(barrier, len(places))

    numbers = iter(range(256))
    started = []

    def remote(source, target, number, arrival, place):
        return pltpu.make_async_remote_copy(
            src_ref=source,
            dst_ref=target,
            send_sem=send.at[number],
            recv_sem=arrival,
            device_id=places[place],
            device_id_type=pl.DeviceIdType.MESH,
        )

    def go(source, target, arrival, place, alike=None):
        number = next(numbers)
        remote(source, target, number, arrival, place).start()
        started.append((number, alike or (lambda: source)))

    def block_copy(kv, slot):
        buffer = (keys, values)[kv]
        return buffer.at[slot], buffer.at[slot], recv.at[kv, slot]

    def wait_block(kv, slot):
        source, target, arrival = block_copy(kv, slot)
        remote(source, target, 0, arrival, "mate").wait_recv()

    def push(kv, slot, place):
        go(*block_copy(kv, slot), place, lambda: (keys, values)[kv].at[0])

    def slot_of(line, d):
        return index(-d, 0 if line == "O" else 1, 0)

    arrivals, sends = link_plan()
    for name, (line, d, kv) in sends[0]:
        push(kv, me, name)
    for kv in range(2):
        push(kv, me, "mate")

    def piece(item, slot, which, c):
        own, gathered = ((wo, wo_all), (wi, wi_all), (wf, wf_all), (wco_all.at[3], wco_all))[item]
        ref = own if slot is None else gathered.at[slot]
        if item in (0, 3):
            first, size = ((0, 64), (0, 32), (32, 32))[which]
            return ref.at[pl.ds(pl.multiple_of(c * 64 + first, 32), size), :]
        if item == 1:
            first, size = ((0, 352), (0, 176), (176, 176))[which]
            return ref.at[c, pl.ds(first, size), :]
        first, size = ((0, 176), (0, 96), (96, 80))[which]
        return ref.at[pl.ds(pl.multiple_of(c * 176 + first, 16), size), :]

    def wait_piece(item, slot, which, k, c):
        ref = piece(item, slot, which, c)
        remote(ref, ref, 0, recv_w.at[item, k], "mate").wait_recv()

    def send_piece(item, slot, slot_there, which, k, to):
        source, target = piece(item, slot, which, core), piece(item, slot_there, which, core)
        go(source, target, recv_w.at[item, k], to, lambda: piece(item, 0, which, 0))

    def weights_start(item):
        loads[("wo", "wi", "wf", "wco")[item]].wait()
        for slot, to in ((0, "right"), (1, "left")):
            send_piece(item, None, slot, 0, slot, to)

    def weights_pass(item):
        for slot, half, onward in ((0, 1, "right"), (1, 2, "left")):
            wait_piece(item, slot, 0, slot, core)
            send_piece(item, slot, 2, half, 1 + half, onward)
            send_piece(item, slot, slot, 0, 4 + slot, "mate")

    def weights_end(item):
        for half in (1, 2):
            wait_piece(item, 2, half, 1 + half, core)
            send_piece(item, 2, 2, half, 5 + half, "mate")

    def weights_here(item):
        for slot in (0, 1):
            wait_piece(item, slot, 0, 4 + slot, 1 - core)
        for half in (1, 2):
            wait_piece(item, 2, half, 5 + half, 1 - core)

    for item in range(4):
        weights_start(item)

    spread[...] = spread_queries(q_t * (HD ** (-0.5) * math.log2(math.e)))
    acc[...] = jnp.zeros_like(acc)
    for name in ("targets", "wcq", "wckv"):
        loads[name].wait()
    cross_normed = normalised(targets[...].astype(jnp.float32), gain_cross[...]).astype(jnp.bfloat16)
    cross_spread[...] = spread_queries(
        dot32(cross_normed, wcq[...]).T * (HD ** (-0.5) * math.log2(math.e))
    )

    def step(s):
        for line, d, kv in arrivals[s]:
            slot = slot_of(line, d)
            wait_block(kv, slot)
            push(kv, slot, "mate")
        for name, (line, d, kv) in sends[s + 1]:
            push(kv, slot_of(line, d), name)

    def chip_slot(j, dc):
        dz, dy = jnp.int32(0), jnp.int32(0)
        for k, (line, d) in enumerate(CHIPS):
            dz = jnp.where(j == k, -d, dz)
            dy = jnp.where(j == k, 0 if line == "O" else 1, dy)
        z_at = lax.rem(z + dz + NZ, NZ)
        y_at = lax.rem(y + dy, 2)
        c_at = core if dc == 0 else 1 - core
        return z_at * 4 + y_at * 2 + c_at

    def score(block, length, queries, into):
        rows = jnp.concatenate([block, key_bias(length, TOK_DEV)], axis=1)
        s = dot32(rows, queries[...])
        into[...] = s
        return jnp.max(s, axis=0, keepdims=True)

    def own_score(slot, into):
        return score(keys[slot], lens[slot], spread, into)

    def rest(block, held, old, top):
        p = jnp.exp2(held[...] - top).astype(jnp.bfloat16)
        shrink = jnp.exp2(old - top)
        ones = jnp.ones((16, TOK_DEV), jnp.bfloat16)
        for h in range(2):
            cols = slice(h * TOK_DEV, (h + 1) * TOK_DEV)
            lhs = jnp.concatenate([block[pl.ds(h * HD, HD), :], ones], axis=0)
            acc[h] = acc[h] * shrink[:, cols] + dot32(lhs, p[:, cols])

    def arrived(slot):
        for kv in range(2):
            wait_block(kv, slot)

    start = jnp.full((1, 2 * TOK_DEV), masked_score, jnp.float32)
    mate = index(0, 0, 1)
    top = own_score(me, scores_0)
    arrived(mate)
    following = jnp.maximum(top, own_score(mate, scores_1))
    rest(values.at[me], scores_0, start, top)

    def body(j, carry):
        old, top = carry
        for at in sorted({*STEPS_BEFORE, *WEIGHT_STEPS_BEFORE}):

            @pl.when(j == at)
            def _():
                for s in STEPS_BEFORE.get(at, ()):
                    step(s)
                for what, item in WEIGHT_STEPS_BEFORE.get(at, ()):
                    (weights_pass if what == "pass" else weights_end)(item)

        here, there = chip_slot(j, 0), chip_slot(j, 1)
        later = jnp.maximum(top, own_score(here, scores_0))
        rest(values.at[chip_slot(j - 1, 1)], scores_1, old, top)
        old, top = top, later
        arrived(there)
        later = jnp.maximum(top, own_score(there, scores_1))
        rest(values.at[here], scores_0, old, top)
        return top, later

    old, top = lax.fori_loop(1, len(CHIPS), body, (top, following))
    rest(values.at[chip_slot(jnp.int32(len(CHIPS) - 1), 1)], scores_1, old, top)
    both = jnp.concatenate([acc[h, 0:HD, :] / acc[h, HD : HD + 1, :] for h in range(2)], axis=0)
    ctx[...] = both.T.astype(jnp.bfloat16)

    def ctx_rows(at):
        return ctx.at[pl.ds(pl.multiple_of(lax.rem(at, 4) * ROWS, ROWS), ROWS), :]

    for g, (to, at) in enumerate((("right", x + 1), ("left", x + 3), ("across", x + 2))):
        go(ctx_rows(at), ctx_in.at[g], recv_c.at[g], to)
    weights_here(0)
    weights_end(1)
    total = dot32(ctx_rows(x)[...], wo[...])
    for g in range(3):
        remote(ctx_in.at[g], ctx_in.at[g], 0, recv_c.at[g], "mate").wait_recv()
        total += dot32(ctx_in[g], wo_all[g])
    out_1[...] = total.astype(jnp.bfloat16)
    go(out_1, in_1, recv_y.at[0], "partner")
    total += tokens[pl.ds(pl.multiple_of(x * ROWS, ROWS), ROWS), :].astype(jnp.float32)
    weights_end(2)
    weights_here(1)
    weights_here(2)
    remote(out_1, in_1, 0, recv_y.at[0], "partner").wait_recv()
    total += in_1[...].astype(jnp.float32)
    hidden[...] = total
    ffn_normed = normalised(total, gain_ffn[...]).T.astype(jnp.bfloat16)
    ffn = jnp.zeros((ROWS, D), jnp.float32)
    for g in range(4):
        gate_w, up_w, down_w = (
            (wi[0], wi[1], wf[...]) if g == 3 else (wi_all[g, 0], wi_all[g, 1], wf_all[g])
        )
        gate = dot32(gate_w, ffn_normed)
        up = dot32(up_w, ffn_normed)
        activated = (jax.nn.gelu(gate, approximate=True) * up).T.astype(jnp.bfloat16)
        ffn += dot32(activated, down_w)
    part[...] = ffn
    share_rows = ROWS // 2
    mine = pl.ds(pl.multiple_of(yh * share_rows, share_rows), share_rows)
    other = pl.ds(pl.multiple_of((1 - yh) * share_rows, share_rows), share_rows)
    out_2[...] = part[other, :].astype(jnp.bfloat16)
    go(out_2, in_2, recv_y.at[1], "partner")
    weights_end(3)
    final = hidden[mine, :] + part[mine, :]
    remote(out_2, in_2, 0, recv_y.at[1], "partner").wait_recv()
    final += in_2[...].astype(jnp.float32)

    def share(dx, dy):
        return lax.rem(x + dx + 4, 4) * 2 + (yh if dy == 0 else 1 - yh)

    enc[share(0, 0)] = normalised(final, gain_final[...]).astype(jnp.bfloat16)

    def rows_of(at, half):
        if half is None:
            return enc.at[at]
        return enc.at[at, pl.ds(half * 32, 32), :]

    def send_share(at, half, to):
        go(rows_of(at, half), rows_of(at, half), recv_e.at[at, half or 0], to)

    def wait_share(at, half):
        ref = rows_of(at, half)
        remote(ref, ref, 0, recv_e.at[at, half or 0], "mate").wait_recv()

    for to in ("partner", "right", "left"):
        send_share(share(0, 0), None, to)
    for dy in (0, 1):
        if dy:
            wait_share(share(0, 1), None)
            for to in ("right", "left"):
                send_share(share(0, 1), None, to)
        for dx, half, to in ((-1, 0, "right"), (1, 1, "left")):
            wait_share(share(dx, dy), None)
            send_share(share(dx, dy), half, to)
    for dy in (0, 1):
        for half in (0, 1):
            wait_share(share(2, dy), half)

    whole = enc[...].reshape(TOK_DEV, D)
    encoded[...] = whole
    cross_keys = dot32(whole, wckv[0]).astype(jnp.bfloat16)
    cross_values[...] = dot32(whole, wckv[1]).T.astype(jnp.bfloat16)
    acc[...] = jnp.zeros_like(acc)
    cross_top = score(cross_keys, lens[me], cross_spread, scores_0)
    rest(cross_values, scores_0, start, cross_top)
    o_all[...] = jnp.concatenate([acc[h, 0:HD, :] / acc[h, HD : HD + 1, :] for h in range(2)], axis=0)
    s_all[...] = jnp.concatenate(
        [
            cross_top[:, h * TOK_DEV : (h + 1) * TOK_DEV] + jnp.log2(acc[h, HD : HD + 1, :])
            for h in range(2)
        ]
        + [jnp.zeros((6, TOK_DEV), jnp.float32)],
        axis=0,
    )

    def joined(first, first_lse, second, second_lse):
        outs, lses = [], []
        for h in range(2):
            one, two = first_lse[h : h + 1], second_lse[h : h + 1]
            top = jnp.maximum(one, two)
            one, two = jnp.exp2(one - top), jnp.exp2(two - top)
            both = one + two
            dims = slice(h * HD, (h + 1) * HD)
            outs.append(first[dims] * (one / both) + second[dims] * (two / both))
            lses.append(top + jnp.log2(both))
        return jnp.concatenate(outs, axis=0), lses

    def lanes(at, size):
        return pl.ds(pl.multiple_of(at * size, size), size)

    def wait_for(ref, arrival):
        remote(ref, ref, 0, arrival, "mate").wait_recv()

    half, quarter = TOK_DEV // 2, TOK_DEV // 4
    go(o_all.at[:, lanes(1 - core, half)], o_mate, recv_m.at[0], "mate", lambda: o_mate)
    go(s_all.at[:, lanes(1 - core, half)], s_mate, recv_m.at[1], "mate", lambda: s_mate)
    wait_for(o_mate, recv_m.at[0])
    wait_for(s_mate, recv_m.at[1])
    o, lse = joined(
        o_all[:, lanes(core, half)], s_all[:, lanes(core, half)], o_mate[...], s_mate[...]
    )
    o_half[...] = o.astype(jnp.bfloat16)
    s_half[...] = jnp.concatenate(lse + [jnp.zeros((6, half), jnp.float32)], axis=0)
    go(o_half.at[:, lanes(1 - y, quarter)], o_side, recv_m.at[2], "side", lambda: o_side)
    go(s_half.at[:, lanes(1 - y, quarter)], s_side, recv_m.at[3], "side", lambda: s_side)
    wait_for(o_side, recv_m.at[2])
    wait_for(s_side, recv_m.at[3])
    o, lse = joined(
        o_half[:, lanes(y, quarter)].astype(jnp.float32),
        s_half[:, lanes(y, quarter)],
        o_side[...].astype(jnp.float32),
        s_side[...],
    )
    o_rows[...] = o.T.astype(jnp.bfloat16)
    s_rows[...] = jnp.concatenate([jnp.broadcast_to(part, (HD, quarter)) for part in lse], axis=0).T
    few = quarter // NZ

    def few_rows(ref, at):
        return ref.at[pl.ds(pl.multiple_of(at * few, few), few), :]

    for dz in (4, 3, 5, 2, 6, 1, 7):
        at = lax.rem(z + dz, NZ)
        go(few_rows(o_rows, at), o_line.at[z], recv_l.at[0, z], line_place[dz], lambda: o_line.at[0])
        go(few_rows(s_rows, at), s_line.at[z], recv_l.at[1, z], line_place[dz], lambda: s_line.at[0])
    o_line[z] = few_rows(o_rows, z)[...]
    s_line[z] = few_rows(s_rows, z)[...]
    for dz in range(1, NZ):
        at = lax.rem(z + dz, NZ)
        wait_for(o_line.at[at], recv_l.at[0, at])
        wait_for(s_line.at[at], recv_l.at[1, at])
    lines = s_line[...]
    factors = jnp.exp2(lines - jnp.max(lines, axis=0, keepdims=True))
    c_all[3] = (
        jnp.sum(o_line[...].astype(jnp.float32) * factors, axis=0) / jnp.sum(factors, axis=0)
    ).astype(jnp.bfloat16)
    for g, to in enumerate(("right", "left", "across")):
        go(c_all.at[3], c_all.at[g], recv_h.at[g], to)
    weights_here(3)
    for g in range(3):
        wait_for(c_all.at[g], recv_h.at[g])
    total = jnp.zeros((few, D), jnp.float32)
    for k in range(4):
        away = lax.rem(k - x + 4, 4)
        g = jnp.where(away == 0, 3, jnp.where(away == 3, 0, away))
        total += dot32(c_all[g], wco_all[g])
    sum_out[...] = total.astype(jnp.bfloat16)
    go(sum_out, sum_in, recv_h.at[3], "partner")

    def place_of(z_at, dy, dc):
        y_at = y if dy == 0 else 1 - y
        c_at = core if dc == 0 else 1 - core
        return c_at * 16 + y_at * NZ + z_at

    mine = place_of(z, 0, 0)
    target_rows = targets[pl.ds(pl.multiple_of(mine * few, few), few), :].astype(jnp.float32)
    slots = z * few + lax.broadcasted_iota(jnp.int32, (few, D), 0)
    wait_for(sum_in, recv_h.at[3])
    total = sum_out[...].astype(jnp.float32) + sum_in[...].astype(jnp.float32)
    live = slots < target_lens[core * 2 + y]
    dec[mine] = (target_rows + jnp.where(live, total, 0.0)).astype(jnp.bfloat16)

    def hand(at, to):
        go(dec.at[at], dec.at[at], recv_d.at[at], to, lambda: dec.at[0])

    for dz in (4, 3, 5, 2, 6, 1, 7):
        hand(mine, line_place[dz])
    hand(mine, "side")
    hand(mine, "mate")
    for dz in (1, 7, 2, 6, 3, 5, 4):
        at = place_of(lax.rem(z + dz, NZ), 0, 0)
        wait_for(dec.at[at], recv_d.at[at])
        hand(at, "side")
        hand(at, "mate")
    for dz in (0, 1, 7, 2, 6, 3, 5, 4):
        at = place_of(lax.rem(z + dz, NZ), 1, 0)
        wait_for(dec.at[at], recv_d.at[at])
        hand(at, "mate")
    for dz in range(NZ):
        for dy in (0, 1):
            at = place_of(lax.rem(z + dz, NZ), dy, 1)
            wait_for(dec.at[at], recv_d.at[at])
    decoded[...] = dec[...].reshape(TOK_DEV, D)
    for number, alike in started:
        remote(alike(), alike(), number, recv_y.at[0], "mate").wait_send()


def layer(lens, tokens, gains, wqkv, wo, wi, wf, targets, wcq, wckv, wco, target_lens):
    vmem = pl.BlockSpec(memory_space=pltpu.VMEM)
    hbm = pl.BlockSpec(memory_space=pl.ANY)
    smem = pl.BlockSpec(memory_space=pltpu.SMEM)
    b16, f32 = jnp.bfloat16, jnp.float32
    gain_attn, gain_ffn, gain_final, gain_cross = (g.reshape(1, D) for g in gains)
    scratch = [
        ((SLOTS, TOK_DEV, 2 * HD), b16),
        ((SLOTS, 2 * HD, TOK_DEV), b16),
        ((256, 2 * TOK_DEV), b16),
        ((2, HD + 16, TOK_DEV), f32),
        ((TOK_DEV, 2 * TOK_DEV), f32),
        ((TOK_DEV, 2 * TOK_DEV), f32),
        (wo.shape, b16),
        (wi.shape, b16),
        (wf.shape, b16),
        (targets.shape, b16),
        (wcq.shape, b16),
        (wckv.shape, b16),
        ((3, *wo.shape), b16),
        ((3, *wi.shape), b16),
        ((3, *wf.shape), b16),
        ((TOK_DEV, 2 * HD), b16),
        ((3, ROWS, 2 * HD), b16),
        ((ROWS, D), f32),
        ((ROWS, D), f32),
        ((ROWS, D), b16),
        ((ROWS, D), b16),
        ((ROWS // 2, D), b16),
        ((ROWS // 2, D), b16),
        ((8, ROWS // 2, D), b16),
        ((256, 2 * TOK_DEV), b16),
        ((2 * HD, TOK_DEV), b16),
        ((4, *wco.shape), b16),
        ((2 * HD, TOK_DEV), f32),
        ((8, TOK_DEV), f32),
        ((2 * HD, TOK_DEV // 2), f32),
        ((8, TOK_DEV // 2), f32),
        ((2 * HD, TOK_DEV // 2), b16),
        ((8, TOK_DEV // 2), f32),
        ((2 * HD, TOK_DEV // 4), b16),
        ((8, TOK_DEV // 4), f32),
        ((TOK_DEV // 4, 2 * HD), b16),
        ((TOK_DEV // 4, 2 * HD), f32),
        ((NZ, 16, 2 * HD), b16),
        ((NZ, 16, 2 * HD), f32),
        ((4, 16, 2 * HD), b16),
        ((16, D), b16),
        ((16, D), b16),
        ((SLOTS, 16, D), b16),
    ]
    sems = [(8,), (200,), (2, SLOTS), (4, 8), (4,), (2,), (8, 2), (4,), (2, NZ), (4,), (SLOTS,)]
    return pl.pallas_call(
        layer_kernel,
        out_shape=(
            jax.ShapeDtypeStruct((TOK_DEV, D), b16),
            jax.ShapeDtypeStruct(targets.shape, b16),
        ),
        in_specs=[smem] + [vmem] * 6 + [hbm] * 7 + [smem],
        out_specs=(vmem, vmem),
        scratch_shapes=[pltpu.VMEM(*s) for s in scratch] + [pltpu.SemaphoreType.DMA(s) for s in sems],
        compiler_params=pltpu.CompilerParams(
            collective_id=0, has_side_effects=True, vmem_limit_bytes=60 << 20
        ),
        name="layer",
    )(lens, tokens, gain_attn, wqkv, gain_ffn, gain_final, gain_cross, wo, wi, wf, targets, wcq, wckv, wco, target_lens)


def local(
    tokens,
    norm_attn,
    self_qkv,
    self_out,
    norm_ffn,
    ffn_in,
    ffn_out,
    norm_final,
    pad_lengths,
    targets,
    target_lengths,
    norm_cross,
    cross_query,
    cross_kv,
    cross_out,
):
    return layer(
        pad_lengths,
        tokens,
        (norm_attn, norm_ffn, norm_final, norm_cross),
        self_qkv,
        self_out,
        jnp.swapaxes(ffn_in, 1, 2),
        ffn_out,
        targets,
        cross_query,
        cross_kv,
        cross_out,
        target_lengths,
    )


def solution(mesh):
    in_specs = (
        P("seq", None),
        P(),
        P(None, None, "head"),
        P("head", None),
        P(),
        P(None, None, "head"),
        P("head", None),
        P(),
        P(),
        P(),
        P(),
        P(),
        P(None, "head"),
        P(None, None, "head"),
        P("head", None),
    )
    out_specs = (P("seq", None), P())
    return jax.shard_map(local, mesh=mesh, in_specs=in_specs, out_specs=out_specs, check_vma=False)
```

```python
import functools
import math

import jax
import jax.numpy as jnp
from jax import lax
from jax.experimental import pallas as pl
from jax.experimental.pallas import tpu as pltpu
from jax.sharding import Mesh
from jax.sharding import PartitionSpec as P

D = 1024
HD = 64
TOK_DEV = 512


epsilon = 1e-06
masked_score = -1e30


NZ = 8
SLOTS = 32
UP = (("O", 0, 0), ("O", 0, 1), ("O", 1, 0), ("O", 1, 1), ("O", 2, 0), ("O", 2, 1), ("P", 2, 0), ("O", 3, 0), ("P", 2, 1), ("P", 3, 0))
DOWN = (("O", 0, 1), ("O", 0, 0), ("O", -1, 1), ("O", -1, 0), ("O", -2, 1), ("O", -2, 0), ("P", -2, 1), ("O", -3, 1), ("P", -3, 1), ("P", -2, 0))
SIDE = (("O", 0, 0), ("O", 0, 1), ("O", 1, 0), ("O", -1, 1), ("O", 2, 0), ("O", -2, 1), ("O", 2, 1), ("O", -2, 0), ("O", 1, 1), ("O", -1, 0))
STEPS = 10
FF_DEV = 352
ROWS = 128
UNIT = 256


def link_plan():
    arrive = {("O", 0, 0): -1, ("O", 0, 1): -1}
    arrivals = []
    for s in range(STEPS):
        new = [(UP[s][0], UP[s][1] + 1, UP[s][2]), (DOWN[s][0], DOWN[s][1] - 1, DOWN[s][2])]
        new.append(("P", SIDE[s][1], SIDE[s][2]))
        arrive.update({item: s for item in new})
        arrivals.append(new)
    waiting = {"up": list(UP), "down": list(DOWN), "side": list(SIDE)}
    sent = {name: 0 for name in waiting}
    sends = []
    for s in range(-1, STEPS):
        now = []
        for name, queue in waiting.items():
            while queue and sent[name] <= s + 2 and arrive[queue[0]] <= s:
                now.append((name, queue.pop(0)))
                sent[name] += 1
        sends.append(now)
    return arrivals, sends


ARRIVALS, SENDS = link_plan()
UNITS = (("O", 0, 0), ("O", 0, 1), *(item for step in ARRIVALS for item in step))
STEP_AT = {2: (0,), **{3 * s: (s,) for s in range(1, STEPS)}}
WEIGHT_STEP_AT = {9: (("pass", 0),), 21: (("pass", 2),), 28: (("pass", 1), ("end", 0))}
UNIT_CODES = tuple((4 - d) * 4 + (line == "P") * 2 + half for line, d, half in UNITS)
CODE_WORDS = tuple(
    sum(code << (8 * k) for k, code in enumerate(UNIT_CODES[first : first + 3]))
    for first in range(0, len(UNITS), 3)
)


def key_bias(length, first, rows):
    row = first + lax.broadcasted_iota(jnp.int32, (rows, 128), 0)
    lane = lax.broadcasted_iota(jnp.int32, (rows, 128), 1)
    return jnp.where((lane == 0) & (row >= length), masked_score, 0.0).astype(jnp.bfloat16)


def spread_queries(q_t):
    rows = lax.broadcasted_iota(jnp.int32, (256, 2 * q_t.shape[1]), 0)
    cols = lax.broadcasted_iota(jnp.int32, (256, 2 * q_t.shape[1]), 1)
    half = q_t.shape[1]
    two = jnp.concatenate([q_t, q_t], axis=1)
    full = jnp.concatenate([two, jnp.zeros_like(two)], axis=0)
    keep = ((rows < HD) & (cols < half)) | ((rows >= HD) & (rows < 2 * HD) & (cols >= half))
    return jnp.where(keep, full, jnp.where(rows == 2 * HD, 1.0, 0.0)).astype(jnp.bfloat16)


def normalised(x, gain):
    return x * lax.rsqrt(jnp.mean(x * x, axis=1, keepdims=True) + epsilon) * gain


def dot32(a, b):
    return jnp.dot(a, b, preferred_element_type=jnp.float32)


def layer_kernel(
    lens,
    tokens_hbm,
    gain_attn_hbm,
    wqkv_hbm,
    gain_ffn_hbm,
    gain_final_hbm,
    gain_cross_hbm,
    wo_hbm,
    wi_hbm,
    wf_hbm,
    targets_hbm,
    wcq_hbm,
    wckv_hbm,
    wco_hbm,
    target_lens,
    enc,
    dec,
    tokens,
    gain_attn,
    wqkv,
    gain_ffn,
    gain_final,
    gain_cross,
    kv,
    spread,
    acc,
    scores_0,
    scores_1,
    wo,
    wi,
    wf,
    targets,
    wcq,
    wckv,
    wo_all,
    wi_all,
    wf_all,
    ctx,
    ctx_in,
    hidden,
    part,
    out_1,
    in_1,
    out_2,
    in_2,
    cross_spread,
    cross_values,
    wco_all,
    o_all,
    s_all,
    o_mate,
    s_mate,
    o_half,
    s_half,
    o_side,
    s_side,
    o_rows,
    s_rows,
    o_line,
    s_line,
    c_all,
    sum_out,
    sum_in,
    local_sem,
    send,
    recv,
    recv_w,
    recv_c,
    recv_y,
    recv_e,
    recv_m,
    recv_l,
    recv_h,
    recv_d,
):
    me = lax.axis_index("seq")
    core = lax.rem(me, 2)
    y = lax.rem(me // 2, 2)
    z = me // 4
    head = lax.axis_index("head")
    x = lax.rem(head, 4)
    yh = head // 4

    def index(dz, dy, dc):
        z_at = lax.rem(z + dz + NZ, NZ)
        y_at = y if dy == 0 else 1 - y
        c_at = core if dc == 0 else 1 - core
        return z_at * 4 + y_at * 2 + c_at

    places = {
        "up": {"seq": index(1, 0, 0)},
        "down": {"seq": index(-1, 0, 0)},
        "side": {"seq": index(0, 1, 0)},
        "mate": {"seq": index(0, 0, 1)},
        "right": {"head": yh * 4 + lax.rem(x + 1, 4)},
        "left": {"head": yh * 4 + lax.rem(x + 3, 4)},
        "across": {"head": yh * 4 + lax.rem(x + 2, 4)},
        "partner": {"head": (1 - yh) * 4 + x},
    }
    for dz in range(2, NZ - 1):
        places[dz] = {"seq": index(dz, 0, 0)}
    line_place = {1: "up", NZ - 1: "down", **{dz: dz for dz in range(2, NZ - 1)}}
    barrier = pltpu.get_barrier_semaphore()
    for place in places.values():
        pl.semaphore_signal(barrier, inc=1, device_id=place, device_id_type=pl.DeviceIdType.MESH)

    pairs = {
        "tokens": (tokens_hbm, tokens),
        "wqkv": (wqkv_hbm, wqkv),
        "gain_attn": (gain_attn_hbm, gain_attn),
        "wo": (wo_hbm, wo),
        "wi": (wi_hbm, wi),
        "wf": (wf_hbm, wf),
        "wco": (wco_hbm, wco_all.at[3]),
        "targets": (targets_hbm, targets),
        "wcq": (wcq_hbm, wcq),
        "gain_cross": (gain_cross_hbm, gain_cross),
        "gain_ffn": (gain_ffn_hbm, gain_ffn),
        "gain_final": (gain_final_hbm, gain_final),
        "wckv": (wckv_hbm, wckv),
    }
    loads = {
        name: pltpu.make_async_copy(source, target, local_sem.at[k])
        for k, (name, (source, target)) in enumerate(pairs.items())
    }
    for load in loads.values():
        load.start()

    for name in ("tokens", "gain_attn", "wqkv"):
        loads[name].wait()
    normed = normalised(tokens[...].astype(jnp.float32), gain_attn[...]).astype(jnp.bfloat16)
    own_keys = dot32(normed, wqkv[1]).astype(jnp.bfloat16)
    own_values = dot32(normed, wqkv[2]).T.astype(jnp.bfloat16)
    for half in range(2):
        kv[me, half, 0:UNIT, :] = own_keys[half * UNIT : (half + 1) * UNIT, :]
        for k in range(2):
            first = half * UNIT + k * 128
            kv[me, half, pl.ds(UNIT + k * 128, 128), :] = own_values[:, first : first + 128]
    q_t = dot32(normed, wqkv[0]).T
    pl.semaphore_wait(barrier, len(places))

    def remote(source, target, number, arrival, place):
        return pltpu.make_async_remote_copy(
            src_ref=source,
            dst_ref=target,
            send_sem=send.at[number],
            recv_sem=arrival,
            device_id=places[place],
            device_id_type=pl.DeviceIdType.MESH,
        )

    def go(source, target, arrival, place, group):
        remote(source, target, group, arrival, place).start()

    def wait_block(half, slot):
        ref = kv.at[slot, half]
        remote(ref, ref, 0, recv.at[half, slot], "mate").wait_recv()

    def push(half, slot, place):
        ref = kv.at[slot, half]
        go(ref, ref, recv.at[half, slot], place, 4)

    def slot_of(line, d):
        return index(-d, 0 if line == "O" else 1, 0)

    for name, (line, d, half) in SENDS[0]:
        push(half, me, name)
    for half in range(2):
        push(half, me, "mate")

    def piece(item, slot, which, c):
        own, gathered = ((wo, wo_all), (wi, wi_all), (wf, wf_all), (wco_all.at[3], wco_all))[item]
        ref = own if slot is None else gathered.at[slot]
        if item in (0, 3):
            first, size = ((0, 64), (0, 32), (32, 32))[which]
            return ref.at[pl.ds(pl.multiple_of(c * 64 + first, 32), size), :]
        if item == 1:
            first, size = ((0, 352), (0, 176), (176, 176))[which]
            return ref.at[c, pl.ds(first, size), :]
        first, size = ((0, 176), (0, 96), (96, 80))[which]
        return ref.at[pl.ds(pl.multiple_of(c * 176 + first, 16), size), :]

    def wait_piece(item, slot, which, k, c):
        ref = piece(item, slot, which, c)
        remote(ref, ref, 0, recv_w.at[item, k], "mate").wait_recv()

    def send_piece(item, slot, slot_there, which, k, to):
        source, target = piece(item, slot, which, core), piece(item, slot_there, which, core)
        go(source, target, recv_w.at[item, k], to, item)

    def weights_start(item):
        loads[("wo", "wi", "wf", "wco")[item]].wait()
        for slot, to in ((0, "right"), (1, "left")):
            send_piece(item, None, slot, 0, slot, to)

    def weights_pass(item):
        for slot, half, onward in ((0, 1, "right"), (1, 2, "left")):
            wait_piece(item, slot, 0, slot, core)
            send_piece(item, slot, 2, half, 1 + half, onward)
            send_piece(item, slot, slot, 0, 4 + slot, "mate")

    def weights_end(item):
        for half in (1, 2):
            wait_piece(item, 2, half, 1 + half, core)
            send_piece(item, 2, 2, half, 5 + half, "mate")

    def weights_here(item):
        for slot in (0, 1):
            wait_piece(item, slot, 0, 4 + slot, 1 - core)
        for half in (1, 2):
            wait_piece(item, 2, half, 5 + half, 1 - core)

    for item in range(3):
        weights_start(item)

    spread[...] = spread_queries(q_t * (HD ** (-0.5) * math.log2(math.e)))
    acc[...] = jnp.zeros_like(acc)
    for name in ("targets", "wcq", "gain_cross", "gain_ffn", "gain_final", "wckv"):
        loads[name].wait()
    cross_normed = normalised(targets[...].astype(jnp.float32), gain_cross[...]).astype(jnp.bfloat16)
    cross_spread[...] = spread_queries(
        dot32(cross_normed, wcq[...]).T * (HD ** (-0.5) * math.log2(math.e))
    )

    def step(s):
        for line, d, half in ARRIVALS[s]:
            slot = slot_of(line, d)
            wait_block(half, slot)
            push(half, slot, "mate")
        for name, (line, d, half) in SENDS[s + 1]:
            push(half, slot_of(line, d), name)

    def unit_of(u):
        third = u // 3
        word = jnp.int32(CODE_WORDS[0])
        for k in range(1, len(CODE_WORDS)):
            word = jnp.where(third == k, CODE_WORDS[k], word)
        code = lax.rem(lax.shift_right_logical(word, 8 * (u - 3 * third)), 256)
        half = lax.rem(code, 2)
        chip = lax.rem(z + code // 4 + 4, NZ) * 4 + lax.rem(y + code // 2, 2) * 2
        return chip + core, chip + 1 - core, half

    def score(block, bias, queries, into):
        s = dot32(jnp.concatenate([block, bias], axis=1), queries[...])
        into[...] = s
        return jnp.max(s, axis=0, keepdims=True)

    def unit_score(unit, into):
        here, there, half = unit
        wait_block(half, there)
        block = jnp.concatenate([kv[here, half, 0:UNIT, :], kv[there, half, 0:UNIT, :]], axis=0)
        bias = jnp.concatenate(
            [key_bias(lens[slot], half * UNIT, UNIT) for slot in (here, there)], axis=0
        )
        return score(block, bias, spread, into)

    def rest(rows_of_head, held, old, top):
        p = jnp.exp2(held[...] - top).astype(jnp.bfloat16)
        shrink = jnp.exp2(old - top)
        ones = jnp.ones((16, TOK_DEV), jnp.bfloat16)
        for h in range(2):
            cols = slice(h * TOK_DEV, (h + 1) * TOK_DEV)
            lhs = jnp.concatenate([rows_of_head(h), ones], axis=0)
            acc[h] = acc[h] * shrink[:, cols] + dot32(lhs, p[:, cols])

    def unit_rest(unit, held, old, top):
        here, there, half = unit

        def rows_of_head(h):
            return jnp.concatenate(
                [
                    kv[slot, half, pl.ds(UNIT + k * 128 + h * HD, HD), :]
                    for slot in (here, there)
                    for k in range(2)
                ],
                axis=1,
            )

        rest(rows_of_head, held, old, top)

    def handle(u, odd):
        for at in sorted({*STEP_AT, *WEIGHT_STEP_AT}):
            if at % 2 != odd:
                continue

            @pl.when(u == at)
            def _():
                for s in STEP_AT.get(at, ()):
                    step(s)
                for what, item in WEIGHT_STEP_AT.get(at, ()):
                    (weights_pass if what == "pass" else weights_end)(item)

    start = jnp.full((1, 2 * TOK_DEV), masked_score, jnp.float32)
    zero = jnp.int32(0)
    first, second = unit_of(zero), unit_of(zero + 1)
    top = unit_score(first, scores_0)
    following = jnp.maximum(top, unit_score(second, scores_1))
    unit_rest(first, scores_0, start, top)

    def body(j, carry):
        old, top, before = carry
        u = 2 * j
        here, after = unit_of(u), unit_of(u + 1)
        handle(u, 0)
        later = jnp.maximum(top, unit_score(here, scores_0))
        unit_rest(before, scores_1, old, top)
        old, top = top, later
        handle(u + 1, 1)
        later = jnp.maximum(top, unit_score(after, scores_1))
        unit_rest(here, scores_0, old, top)
        return top, later, after

    old, top, last = lax.fori_loop(1, len(UNITS) // 2, body, (top, following, second))
    unit_rest(last, scores_1, old, top)
    both = jnp.concatenate([acc[h, 0:HD, :] / acc[h, HD : HD + 1, :] for h in range(2)], axis=0)
    ctx[...] = both.T.astype(jnp.bfloat16)

    def ctx_rows(at):
        return ctx.at[pl.ds(pl.multiple_of(lax.rem(at, 4) * ROWS, ROWS), ROWS), :]

    for g, (to, at) in enumerate((("right", x + 1), ("left", x + 3), ("across", x + 2))):
        go(ctx_rows(at), ctx_in.at[g], recv_c.at[g], to, 5)
    weights_start(3)
    weights_here(0)
    weights_end(1)
    total = dot32(ctx_rows(x)[...], wo[...])
    for g in range(3):
        remote(ctx_in.at[g], ctx_in.at[g], 0, recv_c.at[g], "mate").wait_recv()
        total += dot32(ctx_in[g], wo_all[g])
    out_1[...] = total.astype(jnp.bfloat16)
    go(out_1, in_1, recv_y.at[0], "partner", 6)
    total += tokens[pl.ds(pl.multiple_of(x * ROWS, ROWS), ROWS), :].astype(jnp.float32)
    weights_end(2)
    weights_here(1)
    weights_here(2)
    remote(out_1, in_1, 0, recv_y.at[0], "partner").wait_recv()
    total += in_1[...].astype(jnp.float32)
    hidden[...] = total
    ffn_normed = normalised(total, gain_ffn[...]).T.astype(jnp.bfloat16)
    ffn = jnp.zeros((ROWS, D), jnp.float32)
    for g in range(4):
        gate_w, up_w, down_w = (
            (wi[0], wi[1], wf[...]) if g == 3 else (wi_all[g, 0], wi_all[g, 1], wf_all[g])
        )
        gate = dot32(gate_w, ffn_normed)
        up = dot32(up_w, ffn_normed)
        activated = (jax.nn.gelu(gate, approximate=True) * up).T.astype(jnp.bfloat16)
        ffn += dot32(activated, down_w)
    part[...] = ffn
    share_rows = ROWS // 2
    mine = pl.ds(pl.multiple_of(yh * share_rows, share_rows), share_rows)
    other = pl.ds(pl.multiple_of((1 - yh) * share_rows, share_rows), share_rows)
    out_2[...] = part[other, :].astype(jnp.bfloat16)
    go(out_2, in_2, recv_y.at[1], "partner", 7)
    weights_pass(3)
    final = hidden[mine, :] + part[mine, :]
    remote(out_2, in_2, 0, recv_y.at[1], "partner").wait_recv()
    final += in_2[...].astype(jnp.float32)

    def share(dx, dy):
        return lax.rem(x + dx + 4, 4) * 2 + (yh if dy == 0 else 1 - yh)

    enc[share(0, 0)] = normalised(final, gain_final[...]).astype(jnp.bfloat16)

    def rows_of(at, half):
        if half is None:
            return enc.at[at]
        return enc.at[at, pl.ds(half * 32, 32), :]

    def send_share(at, half, to):
        go(rows_of(at, half), rows_of(at, half), recv_e.at[at, half or 0], to, 8)

    def wait_share(at, half):
        ref = rows_of(at, half)
        remote(ref, ref, 0, recv_e.at[at, half or 0], "mate").wait_recv()

    for to in ("partner", "right", "left"):
        send_share(share(0, 0), None, to)
    for dy in (0, 1):
        if dy:
            wait_share(share(0, 1), None)
            for to in ("right", "left"):
                send_share(share(0, 1), None, to)
        for dx, half, to in ((-1, 0, "right"), (1, 1, "left")):
            wait_share(share(dx, dy), None)
            send_share(share(dx, dy), half, to)
    for dy in (0, 1):
        for half in (0, 1):
            wait_share(share(2, dy), half)

    whole = enc[...].reshape(TOK_DEV, D)
    cross_keys = dot32(whole, wckv[0]).astype(jnp.bfloat16)
    cross_values[...] = dot32(whole, wckv[1]).T.astype(jnp.bfloat16)
    acc[...] = jnp.zeros_like(acc)
    cross_top = score(cross_keys, key_bias(lens[me], 0, TOK_DEV), cross_spread, scores_0)
    rest(lambda h: cross_values[pl.ds(h * HD, HD), :], scores_0, start, cross_top)
    o_all[...] = jnp.concatenate([acc[h, 0:HD, :] / acc[h, HD : HD + 1, :] for h in range(2)], axis=0)
    s_all[...] = jnp.concatenate(
        [
            cross_top[:, h * TOK_DEV : (h + 1) * TOK_DEV] + jnp.log2(acc[h, HD : HD + 1, :])
            for h in range(2)
        ]
        + [jnp.zeros((6, TOK_DEV), jnp.float32)],
        axis=0,
    )

    def joined(first, first_lse, second, second_lse):
        outs, lses = [], []
        for h in range(2):
            one, two = first_lse[h : h + 1], second_lse[h : h + 1]
            top = jnp.maximum(one, two)
            one, two = jnp.exp2(one - top), jnp.exp2(two - top)
            both = one + two
            dims = slice(h * HD, (h + 1) * HD)
            outs.append(first[dims] * (one / both) + second[dims] * (two / both))
            lses.append(top + jnp.log2(both))
        return jnp.concatenate(outs, axis=0), lses

    def lanes(at, size):
        return pl.ds(pl.multiple_of(at * size, size), size)

    def wait_for(ref, arrival):
        remote(ref, ref, 0, arrival, "mate").wait_recv()

    half, quarter = TOK_DEV // 2, TOK_DEV // 4
    go(o_all.at[:, lanes(1 - core, half)], o_mate, recv_m.at[0], "mate", 9)
    go(s_all.at[:, lanes(1 - core, half)], s_mate, recv_m.at[1], "mate", 10)
    weights_end(3)
    wait_for(o_mate, recv_m.at[0])
    wait_for(s_mate, recv_m.at[1])
    o, lse = joined(
        o_all[:, lanes(core, half)], s_all[:, lanes(core, half)], o_mate[...], s_mate[...]
    )
    o_half[...] = o.astype(jnp.bfloat16)
    s_half[...] = jnp.concatenate(lse + [jnp.zeros((6, half), jnp.float32)], axis=0)
    go(o_half.at[:, lanes(1 - y, quarter)], o_side, recv_m.at[2], "side", 11)
    go(s_half.at[:, lanes(1 - y, quarter)], s_side, recv_m.at[3], "side", 12)
    wait_for(o_side, recv_m.at[2])
    wait_for(s_side, recv_m.at[3])
    o, lse = joined(
        o_half[:, lanes(y, quarter)].astype(jnp.float32),
        s_half[:, lanes(y, quarter)],
        o_side[...].astype(jnp.float32),
        s_side[...],
    )
    o_rows[...] = o.T.astype(jnp.bfloat16)
    s_rows[...] = jnp.concatenate([jnp.broadcast_to(part, (HD, quarter)) for part in lse], axis=0).T
    few = quarter // NZ

    def few_rows(ref, at):
        return ref.at[pl.ds(pl.multiple_of(at * few, few), few), :]

    for dz in (4, 3, 5, 2, 6, 1, 7):
        at = lax.rem(z + dz, NZ)
        go(few_rows(o_rows, at), o_line.at[z], recv_l.at[0, z], line_place[dz], 13)
        go(few_rows(s_rows, at), s_line.at[z], recv_l.at[1, z], line_place[dz], 14)
    o_line[z] = few_rows(o_rows, z)[...]
    s_line[z] = few_rows(s_rows, z)[...]
    for dz in range(1, NZ):
        at = lax.rem(z + dz, NZ)
        wait_for(o_line.at[at], recv_l.at[0, at])
        wait_for(s_line.at[at], recv_l.at[1, at])
    lines = s_line[...]
    factors = jnp.exp2(lines - jnp.max(lines, axis=0, keepdims=True))
    c_all[3] = (
        jnp.sum(o_line[...].astype(jnp.float32) * factors, axis=0) / jnp.sum(factors, axis=0)
    ).astype(jnp.bfloat16)
    for g, to in enumerate(("right", "left", "across")):
        go(c_all.at[3], c_all.at[g], recv_h.at[g], to, 15)
    weights_here(3)
    for g in range(3):
        wait_for(c_all.at[g], recv_h.at[g])
    total = jnp.zeros((few, D), jnp.float32)
    for k in range(4):
        away = lax.rem(k - x + 4, 4)
        g = jnp.where(away == 0, 3, jnp.where(away == 3, 0, away))
        total += dot32(c_all[g], wco_all[g])
    sum_out[...] = total.astype(jnp.bfloat16)
    go(sum_out, sum_in, recv_h.at[3], "partner", 16)

    def place_of(z_at, dy, dc):
        y_at = y if dy == 0 else 1 - y
        c_at = core if dc == 0 else 1 - core
        return c_at * 16 + y_at * NZ + z_at

    mine = place_of(z, 0, 0)
    target_rows = targets[pl.ds(pl.multiple_of(mine * few, few), few), :].astype(jnp.float32)
    slots = z * few + lax.broadcasted_iota(jnp.int32, (few, D), 0)
    wait_for(sum_in, recv_h.at[3])
    total = sum_out[...].astype(jnp.float32) + sum_in[...].astype(jnp.float32)
    live = slots < target_lens[core * 2 + y]
    dec[mine] = (target_rows + jnp.where(live, total, 0.0)).astype(jnp.bfloat16)

    def hand(at, to):
        go(dec.at[at], dec.at[at], recv_d.at[at], to, 17)

    for dz in (4, 3, 5, 2, 6, 1, 7):
        hand(mine, line_place[dz])
    hand(mine, "side")
    hand(mine, "mate")
    for dz in (1, 7, 2, 6, 3, 5, 4):
        at = place_of(lax.rem(z + dz, NZ), 0, 0)
        wait_for(dec.at[at], recv_d.at[at])
        hand(at, "side")
        hand(at, "mate")
    for dz in (0, 1, 7, 2, 6, 3, 5, 4):
        at = place_of(lax.rem(z + dz, NZ), 1, 0)
        wait_for(dec.at[at], recv_d.at[at])
        hand(at, "mate")
    for dz in range(NZ):
        for dy in (0, 1):
            at = place_of(lax.rem(z + dz, NZ), dy, 1)
            wait_for(dec.at[at], recv_d.at[at])
    sent = (
        wo_all,
        wi_all,
        wf_all,
        wco_all.at[pl.ds(0, 3)],
        kv.at[pl.ds(0, SLOTS - 1)],
        ctx_in,
        out_1,
        out_2,
        enc.at[pl.ds(0, 7)],
        o_mate,
        s_mate,
        o_side,
        s_side,
        o_line.at[pl.ds(0, NZ - 1)],
        s_line.at[pl.ds(0, NZ - 1)],
        c_all.at[pl.ds(0, 3)],
        sum_out,
        dec.at[pl.ds(0, SLOTS - 1)],
    )
    for group, ref in enumerate(sent):
        remote(ref, ref, group, recv_y.at[0], "mate").wait_send()


def layer(lens, tokens, gains, wqkv, wo, wi, wf, targets, wcq, wckv, wco, target_lens):
    hbm = pl.BlockSpec(memory_space=pl.ANY)
    vmem = pl.BlockSpec(memory_space=pltpu.VMEM)
    smem = pl.BlockSpec(memory_space=pltpu.SMEM)
    b16, f32 = jnp.bfloat16, jnp.float32
    gain_attn, gain_ffn, gain_final, gain_cross = (g.reshape(1, D) for g in gains)
    scratch = [
        (tokens.shape, b16),
        ((1, D), f32),
        (wqkv.shape, b16),
        ((1, D), f32),
        ((1, D), f32),
        ((1, D), f32),
        ((SLOTS, 2, 2 * UNIT, 2 * HD), b16),
        ((256, 2 * TOK_DEV), b16),
        ((2, HD + 16, TOK_DEV), f32),
        ((TOK_DEV, 2 * TOK_DEV), f32),
        ((TOK_DEV, 2 * TOK_DEV), f32),
        (wo.shape, b16),
        (wi.shape, b16),
        (wf.shape, b16),
        (targets.shape, b16),
        (wcq.shape, b16),
        (wckv.shape, b16),
        ((3, *wo.shape), b16),
        ((3, *wi.shape), b16),
        ((3, *wf.shape), b16),
        ((TOK_DEV, 2 * HD), b16),
        ((3, ROWS, 2 * HD), b16),
        ((ROWS, D), f32),
        ((ROWS, D), f32),
        ((ROWS, D), b16),
        ((ROWS, D), b16),
        ((ROWS // 2, D), b16),
        ((ROWS // 2, D), b16),
        ((256, 2 * TOK_DEV), b16),
        ((2 * HD, TOK_DEV), b16),
        ((4, *wco.shape), b16),
        ((2 * HD, TOK_DEV), f32),
        ((8, TOK_DEV), f32),
        ((2 * HD, TOK_DEV // 2), f32),
        ((8, TOK_DEV // 2), f32),
        ((2 * HD, TOK_DEV // 2), b16),
        ((8, TOK_DEV // 2), f32),
        ((2 * HD, TOK_DEV // 4), b16),
        ((8, TOK_DEV // 4), f32),
        ((TOK_DEV // 4, 2 * HD), b16),
        ((TOK_DEV // 4, 2 * HD), f32),
        ((NZ, 16, 2 * HD), b16),
        ((NZ, 16, 2 * HD), f32),
        ((4, 16, 2 * HD), b16),
        ((16, D), b16),
        ((16, D), b16),
    ]
    sems = [(16,), (18,), (2, SLOTS), (4, 8), (4,), (2,), (8, 2), (4,), (2, NZ), (4,), (SLOTS,)]
    encoded, decoded = pl.pallas_call(
        layer_kernel,
        out_shape=(
            pltpu.VMEM((8, ROWS // 2, D), b16),
            pltpu.VMEM((SLOTS, 16, D), b16),
        ),
        in_specs=[smem] + [hbm] * 13 + [smem],
        out_specs=(vmem, vmem),
        scratch_shapes=[pltpu.VMEM(*s) for s in scratch] + [pltpu.SemaphoreType.DMA(s) for s in sems],
        compiler_params=pltpu.CompilerParams(
            collective_id=0, has_side_effects=True, vmem_limit_bytes=54 << 20
        ),
        name="layer",
    )(lens, tokens, gain_attn, wqkv, gain_ffn, gain_final, gain_cross, wo, wi, wf, targets, wcq, wckv, wco, target_lens)
    return encoded.reshape(TOK_DEV, D), decoded.reshape(targets.shape)


def local(
    tokens,
    norm_attn,
    self_qkv,
    self_out,
    norm_ffn,
    ffn_in,
    ffn_out,
    norm_final,
    pad_lengths,
    targets,
    target_lengths,
    norm_cross,
    cross_query,
    cross_kv,
    cross_out,
):
    return layer(
        pad_lengths,
        tokens,
        (norm_attn, norm_ffn, norm_final, norm_cross),
        self_qkv,
        self_out,
        jnp.swapaxes(ffn_in, 1, 2),
        ffn_out,
        targets,
        cross_query,
        cross_kv,
        cross_out,
        target_lengths,
    )


def solution(mesh):
    in_specs = (
        P("seq", None),
        P(),
        P(None, None, "head"),
        P("head", None),
        P(),
        P(None, None, "head"),
        P("head", None),
        P(),
        P(),
        P(),
        P(),
        P(),
        P(None, "head"),
        P(None, None, "head"),
        P("head", None),
    )
    out_specs = (P("seq", None), P())
    return jax.shard_map(local, mesh=mesh, in_specs=in_specs, out_specs=out_specs, check_vma=False)
```

```python
import functools
import math

import jax
import jax.numpy as jnp
from jax import lax
from jax.experimental import pallas as pl
from jax.experimental.pallas import tpu as pltpu
from jax.sharding import Mesh
from jax.sharding import PartitionSpec as P

D = 1024
HD = 64
TOK_DEV = 512


epsilon = 1e-06
masked_score = -1e30


NZ = 8
SLOTS = 32
UP = (("O", 0, 0), ("O", 0, 1), ("O", 1, 0), ("O", 1, 1), ("O", 2, 0), ("O", 2, 1), ("P", 2, 0), ("O", 3, 0), ("P", 2, 1), ("P", 3, 0))
DOWN = (("O", 0, 1), ("O", 0, 0), ("O", -1, 1), ("O", -1, 0), ("O", -2, 1), ("O", -2, 0), ("P", -2, 1), ("O", -3, 1), ("P", -3, 1), ("P", -2, 0))
SIDE = (("O", 0, 0), ("O", 0, 1), ("O", 1, 0), ("O", -1, 1), ("O", 2, 0), ("O", -2, 1), ("O", 2, 1), ("O", -2, 0), ("O", 1, 1), ("O", -1, 0))
STEPS = 10
FF_DEV = 352
ROWS = 128
UNIT = 256


def link_plan():
    arrive = {("O", 0, 0): -1, ("O", 0, 1): -1}
    arrivals = []
    for s in range(STEPS):
        new = [(UP[s][0], UP[s][1] + 1, UP[s][2]), (DOWN[s][0], DOWN[s][1] - 1, DOWN[s][2])]
        new.append(("P", SIDE[s][1], SIDE[s][2]))
        arrive.update({item: s for item in new})
        arrivals.append(new)
    waiting = {"up": list(UP), "down": list(DOWN), "side": list(SIDE)}
    sent = {name: 0 for name in waiting}
    sends = []
    for s in range(-1, STEPS):
        now = []
        for name, queue in waiting.items():
            while queue and sent[name] <= s + 2 and arrive[queue[0]] <= s:
                now.append((name, queue.pop(0)))
                sent[name] += 1
        sends.append(now)
    return arrivals, sends


ARRIVALS, SENDS = link_plan()
UNITS = (("O", 0, 0), ("O", 0, 1), *(item for step in ARRIVALS for item in step))
STEP_AT = {2: 0, 4: 1, 6: 2, 8: 3, 12: 4, 14: 5, 18: 6, 20: 7, 24: 8, 26: 9}
WEIGHT_STEP_AT = {8: (("pass", 0),), 14: (("start", 2),), 18: (("pass", 1), ("end", 0))}
UNIT_CODES = tuple((4 - d) * 4 + (line == "P") * 2 + half for line, d, half in UNITS)
CODE_WORDS = tuple(
    sum(code << (8 * k) for k, code in enumerate(UNIT_CODES[first : first + 3]))
    for first in range(0, len(UNITS), 3)
)


def key_bias(length, first, rows):
    row = first + lax.broadcasted_iota(jnp.int32, (rows, 128), 0)
    lane = lax.broadcasted_iota(jnp.int32, (rows, 128), 1)
    return jnp.where((lane == 0) & (row >= length), masked_score, 0.0).astype(jnp.bfloat16)


def spread_queries(q_t):
    rows = lax.broadcasted_iota(jnp.int32, (256, 2 * q_t.shape[1]), 0)
    cols = lax.broadcasted_iota(jnp.int32, (256, 2 * q_t.shape[1]), 1)
    half = q_t.shape[1]
    two = jnp.concatenate([q_t, q_t], axis=1)
    full = jnp.concatenate([two, jnp.zeros_like(two)], axis=0)
    keep = ((rows < HD) & (cols < half)) | ((rows >= HD) & (rows < 2 * HD) & (cols >= half))
    return jnp.where(keep, full, jnp.where(rows == 2 * HD, 1.0, 0.0)).astype(jnp.bfloat16)


def normalised(x, gain):
    return x * lax.rsqrt(jnp.mean(x * x, axis=1, keepdims=True) + epsilon) * gain


def dot32(a, b):
    return jnp.dot(a, b, preferred_element_type=jnp.float32)


def layer_kernel(
    lens,
    tokens_hbm,
    gain_attn_hbm,
    wqkv_hbm,
    gain_ffn_hbm,
    gain_final_hbm,
    gain_cross_hbm,
    wo_hbm,
    wi_hbm,
    wf_hbm,
    targets_hbm,
    wcq_hbm,
    wckv_hbm,
    wco_hbm,
    target_lens,
    enc,
    dec,
    tokens,
    gain_attn,
    wqkv,
    gain_ffn,
    gain_final,
    gain_cross,
    kv,
    spread,
    acc,
    scores_0,
    scores_1,
    wo,
    wi,
    wf,
    targets,
    wcq,
    wckv,
    wo_all,
    wi_all,
    wf_all,
    ctx,
    ctx_in,
    hidden,
    part,
    out_1,
    in_1,
    out_2,
    in_2,
    cross_spread,
    cross_values,
    wco_all,
    o_all,
    s_all,
    o_mate,
    s_mate,
    o_half,
    s_half,
    o_side,
    s_side,
    o_rows,
    s_rows,
    o_line,
    s_line,
    c_all,
    sum_out,
    sum_in,
    local_sem,
    send,
    recv,
    recv_w,
    recv_c,
    recv_y,
    recv_e,
    recv_m,
    recv_l,
    recv_h,
    recv_d,
):
    me = lax.axis_index("seq")
    core = lax.rem(me, 2)
    y = lax.rem(me // 2, 2)
    z = me // 4
    head = lax.axis_index("head")
    x = lax.rem(head, 4)
    yh = head // 4

    def index(dz, dy, dc):
        z_at = lax.rem(z + dz + NZ, NZ)
        y_at = y if dy == 0 else 1 - y
        c_at = core if dc == 0 else 1 - core
        return z_at * 4 + y_at * 2 + c_at

    places = {
        "up": {"seq": index(1, 0, 0)},
        "down": {"seq": index(-1, 0, 0)},
        "side": {"seq": index(0, 1, 0)},
        "mate": {"seq": index(0, 0, 1)},
        "right": {"head": yh * 4 + lax.rem(x + 1, 4)},
        "left": {"head": yh * 4 + lax.rem(x + 3, 4)},
        "across": {"head": yh * 4 + lax.rem(x + 2, 4)},
        "partner": {"head": (1 - yh) * 4 + x},
    }
    for dz in range(2, NZ - 1):
        places[dz] = {"seq": index(dz, 0, 0)}
    line_place = {1: "up", NZ - 1: "down", **{dz: dz for dz in range(2, NZ - 1)}}
    barrier = pltpu.get_barrier_semaphore()
    for place in places.values():
        pl.semaphore_signal(barrier, inc=1, device_id=place, device_id_type=pl.DeviceIdType.MESH)

    pairs = {
        "tokens": (tokens_hbm, tokens),
        "wqkv": (wqkv_hbm, wqkv),
        "gain_attn": (gain_attn_hbm, gain_attn),
        "wo": (wo_hbm, wo),
        "wi": (wi_hbm, wi),
        "wf": (wf_hbm, wf),
        "wco": (wco_hbm, wco_all.at[3]),
        "targets": (targets_hbm, targets),
        "wcq": (wcq_hbm, wcq),
        "gain_cross": (gain_cross_hbm, gain_cross),
        "gain_ffn": (gain_ffn_hbm, gain_ffn),
        "gain_final": (gain_final_hbm, gain_final),
        "wckv": (wckv_hbm, wckv),
    }
    loads = {
        name: pltpu.make_async_copy(source, target, local_sem.at[k])
        for k, (name, (source, target)) in enumerate(pairs.items())
    }
    first_loads = ("tokens", "gain_attn", "wqkv")
    for name in first_loads:
        loads[name].start()
    for name in first_loads:
        loads[name].wait()
    for name, load in loads.items():
        if name not in first_loads:
            load.start()
    normed = normalised(tokens[...].astype(jnp.float32), gain_attn[...]).astype(jnp.bfloat16)
    own_keys = dot32(normed, wqkv[1]).astype(jnp.bfloat16)
    own_values = dot32(normed, wqkv[2]).T.astype(jnp.bfloat16)
    for half in range(2):
        kv[me, half, 0:UNIT, :] = own_keys[half * UNIT : (half + 1) * UNIT, :]
        for k in range(2):
            first = half * UNIT + k * 128
            kv[me, half, pl.ds(UNIT + k * 128, 128), :] = own_values[:, first : first + 128]
    pl.semaphore_wait(barrier, len(places))

    def remote(source, target, number, arrival, place):
        return pltpu.make_async_remote_copy(
            src_ref=source,
            dst_ref=target,
            send_sem=send.at[number],
            recv_sem=arrival,
            device_id=places[place],
            device_id_type=pl.DeviceIdType.MESH,
        )

    def go(source, target, arrival, place, group):
        remote(source, target, group, arrival, place).start()

    def wait_block(half, slot):
        ref = kv.at[slot, half]
        remote(ref, ref, 0, recv.at[half, slot], "mate").wait_recv()

    def push(half, slot, place):
        ref = kv.at[slot, half]
        go(ref, ref, recv.at[half, slot], place, 4)

    def slot_of(line, d):
        return index(-d, 0 if line == "O" else 1, 0)

    for name, (line, d, half) in SENDS[0]:
        push(half, me, name)
    for half in range(2):
        push(half, me, "mate")

    def piece(item, slot, which, c):
        own, gathered = ((wo, wo_all), (wi, wi_all), (wf, wf_all), (wco_all.at[3], wco_all))[item]
        ref = own if slot is None else gathered.at[slot]
        if item in (0, 3):
            first, size = ((0, 64), (0, 32), (32, 32))[which]
            return ref.at[pl.ds(pl.multiple_of(c * 64 + first, 32), size), :]
        if item == 1:
            first, size = ((0, 352), (0, 176), (176, 176))[which]
            return ref.at[c, pl.ds(first, size), :]
        first, size = ((0, 176), (0, 96), (96, 80))[which]
        return ref.at[pl.ds(pl.multiple_of(c * 176 + first, 16), size), :]

    def wait_piece(item, slot, which, k, c):
        ref = piece(item, slot, which, c)
        remote(ref, ref, 0, recv_w.at[item, k], "mate").wait_recv()

    def send_piece(item, slot, slot_there, which, k, to):
        source, target = piece(item, slot, which, core), piece(item, slot_there, which, core)
        go(source, target, recv_w.at[item, k], to, item)

    def weights_start(item):
        loads[("wo", "wi", "wf", "wco")[item]].wait()
        for slot, to in ((0, "right"), (1, "left")):
            send_piece(item, None, slot, 0, slot, to)

    def weights_pass(item):
        for slot, half, onward in ((0, 1, "right"), (1, 2, "left")):
            wait_piece(item, slot, 0, slot, core)
            send_piece(item, slot, 2, half, 1 + half, onward)
            send_piece(item, slot, slot, 0, 4, "mate")

    def weights_end(item):
        for half in (1, 2):
            wait_piece(item, 2, half, 1 + half, core)
            send_piece(item, 2, 2, half, 4, "mate")

    def weights_here(item):
        c = 1 - core
        ref = (
            lambda: wo_all.at[:, pl.ds(pl.multiple_of(c * 64, 64), 64), :],
            lambda: wi_all.at[:, c],
            lambda: wf_all.at[:, pl.ds(pl.multiple_of(c * 176, 16), 176), :],
            lambda: wco_all.at[pl.ds(0, 3), pl.ds(pl.multiple_of(c * 64, 64), 64), :],
        )[item]()
        remote(ref, ref, 0, recv_w.at[item, 4], "mate").wait_recv()

    for item in range(2):
        weights_start(item)
    q_t = dot32(normed, wqkv[0]).T

    spread[...] = spread_queries(q_t * (HD ** (-0.5) * math.log2(math.e)))
    acc[...] = jnp.zeros_like(acc)
    for name in ("targets", "wcq", "gain_cross", "gain_ffn", "gain_final", "wckv"):
        loads[name].wait()
    cross_normed = normalised(targets[...].astype(jnp.float32), gain_cross[...]).astype(jnp.bfloat16)
    cross_spread[...] = spread_queries(
        dot32(cross_normed, wcq[...]).T * (HD ** (-0.5) * math.log2(math.e))
    )

    def step(s):
        for line, d, half in ARRIVALS[s]:
            slot = slot_of(line, d)
            wait_block(half, slot)
            push(half, slot, "mate")
        for name, (line, d, half) in SENDS[s + 1]:
            push(half, slot_of(line, d), name)

    def unit_of(u):
        third = u // 3
        word = jnp.int32(CODE_WORDS[0])
        for k in range(1, len(CODE_WORDS)):
            word = jnp.where(third == k, CODE_WORDS[k], word)
        code = lax.rem(lax.shift_right_logical(word, 8 * (u - 3 * third)), 256)
        half = lax.rem(code, 2)
        chip = lax.rem(z + code // 4 + 4, NZ) * 4 + lax.rem(y + code // 2, 2) * 2
        return chip + core, chip + 1 - core, half

    def score(block, bias, queries, into):
        s = dot32(jnp.concatenate([block, bias], axis=1), queries[...])
        into[...] = s
        return jnp.max(s, axis=0, keepdims=True)

    def unit_score(unit, into):
        here, there, half = unit
        block = jnp.concatenate([kv[here, half, 0:UNIT, :], kv[there, half, 0:UNIT, :]], axis=0)
        bias = jnp.concatenate(
            [key_bias(lens[slot], half * UNIT, UNIT) for slot in (here, there)], axis=0
        )
        return score(block, bias, spread, into)

    def rest(rows_of_head, held, old, top):
        p = jnp.exp2(held[...] - top).astype(jnp.bfloat16)
        shrink = jnp.exp2(old - top)
        ones = jnp.ones((16, TOK_DEV), jnp.bfloat16)
        for h in range(2):
            cols = slice(h * TOK_DEV, (h + 1) * TOK_DEV)
            lhs = jnp.concatenate([rows_of_head(h), ones], axis=0)
            acc[h] = acc[h] * shrink[:, cols] + dot32(lhs, p[:, cols])

    def unit_rest(unit, held, old, top):
        here, there, half = unit

        def rows_of_head(h):
            return jnp.concatenate(
                [
                    kv[slot, half, pl.ds(UNIT + k * 128 + h * HD, HD), :]
                    for slot in (here, there)
                    for k in range(2)
                ],
                axis=1,
            )

        rest(rows_of_head, held, old, top)

    acts = {"start": weights_start, "pass": weights_pass, "end": weights_end}

    def handle(u):
        for at in sorted({*STEP_AT, *WEIGHT_STEP_AT}):

            @pl.when(u == at)
            def _():
                if at in STEP_AT:
                    step(STEP_AT[at])
                for what, item in WEIGHT_STEP_AT.get(at, ()):
                    acts[what](item)

    def wait_mate(unit):
        here, there, half = unit
        wait_block(half, there)

    start = jnp.full((1, 2 * TOK_DEV), masked_score, jnp.float32)
    zero = jnp.int32(0)
    first, second = unit_of(zero), unit_of(zero + 1)
    wait_mate(first)
    wait_mate(second)
    top = unit_score(first, scores_0)
    following = jnp.maximum(top, unit_score(second, scores_1))
    unit_rest(first, scores_0, start, top)

    def body(j, carry):
        old, top, before = carry
        u = 2 * j
        here, after = unit_of(u), unit_of(u + 1)
        handle(u)
        wait_mate(here)
        wait_mate(after)
        later = jnp.maximum(top, unit_score(here, scores_0))
        unit_rest(before, scores_1, old, top)
        old, top = top, later
        later = jnp.maximum(top, unit_score(after, scores_1))
        unit_rest(here, scores_0, old, top)
        return top, later, after

    old, top, last = lax.fori_loop(1, len(UNITS) // 2, body, (top, following, second))
    unit_rest(last, scores_1, old, top)
    both = jnp.concatenate([acc[h, 0:HD, :] / acc[h, HD : HD + 1, :] for h in range(2)], axis=0)
    ctx[...] = both.T.astype(jnp.bfloat16)

    def ctx_rows(at):
        return ctx.at[pl.ds(pl.multiple_of(lax.rem(at, 4) * ROWS, ROWS), ROWS), :]

    for g, (to, at) in enumerate((("right", x + 1), ("left", x + 3), ("across", x + 2))):
        go(ctx_rows(at), ctx_in.at[g], recv_c.at[g], to, 5)
    weights_pass(2)
    weights_start(3)
    weights_here(0)
    weights_end(1)
    total = dot32(ctx_rows(x)[...], wo[...])
    for g in range(3):
        remote(ctx_in.at[g], ctx_in.at[g], 0, recv_c.at[g], "mate").wait_recv()
        total += dot32(ctx_in[g], wo_all[g])
    out_1[...] = total.astype(jnp.bfloat16)
    go(out_1, in_1, recv_y.at[0], "partner", 6)
    total += tokens[pl.ds(pl.multiple_of(x * ROWS, ROWS), ROWS), :].astype(jnp.float32)
    weights_end(2)
    weights_here(1)
    weights_here(2)
    remote(out_1, in_1, 0, recv_y.at[0], "partner").wait_recv()
    total += in_1[...].astype(jnp.float32)
    hidden[...] = total
    ffn_normed = normalised(total, gain_ffn[...]).T.astype(jnp.bfloat16)
    ffn = jnp.zeros((ROWS, D), jnp.float32)
    for g in range(4):
        gate_w, up_w, down_w = (
            (wi[0], wi[1], wf[...]) if g == 3 else (wi_all[g, 0], wi_all[g, 1], wf_all[g])
        )
        gate = dot32(gate_w, ffn_normed)
        up = dot32(up_w, ffn_normed)
        activated = (jax.nn.gelu(gate, approximate=True) * up).T.astype(jnp.bfloat16)
        ffn += dot32(activated, down_w)
    part[...] = ffn
    share_rows = ROWS // 2
    mine = pl.ds(pl.multiple_of(yh * share_rows, share_rows), share_rows)
    other = pl.ds(pl.multiple_of((1 - yh) * share_rows, share_rows), share_rows)
    out_2[...] = part[other, :].astype(jnp.bfloat16)
    go(out_2, in_2, recv_y.at[1], "partner", 7)
    weights_pass(3)
    final = hidden[mine, :] + part[mine, :]
    remote(out_2, in_2, 0, recv_y.at[1], "partner").wait_recv()
    final += in_2[...].astype(jnp.float32)

    def share(dx, dy):
        return lax.rem(x + dx + 4, 4) * 2 + (yh if dy == 0 else 1 - yh)

    enc[share(0, 0)] = normalised(final, gain_final[...]).astype(jnp.bfloat16)

    def rows_of(at, half):
        if half is None:
            return enc.at[at]
        return enc.at[at, pl.ds(half * 32, 32), :]

    def send_share(at, half, to):
        go(rows_of(at, half), rows_of(at, half), recv_e.at[at, half or 0], to, 8)

    def wait_share(at, half):
        ref = rows_of(at, half)
        remote(ref, ref, 0, recv_e.at[at, half or 0], "mate").wait_recv()

    for to in ("partner", "right", "left"):
        send_share(share(0, 0), None, to)
    for dy in (0, 1):
        if dy:
            wait_share(share(0, 1), None)
            for to in ("right", "left"):
                send_share(share(0, 1), None, to)
        for dx, half, to in ((-1, 0, "right"), (1, 1, "left")):
            wait_share(share(dx, dy), None)
            send_share(share(dx, dy), half, to)
    for dy in (0, 1):
        for half in (0, 1):
            wait_share(share(2, dy), half)

    whole = enc[...].reshape(TOK_DEV, D)
    cross_keys = dot32(whole, wckv[0]).astype(jnp.bfloat16)
    cross_values[...] = dot32(whole, wckv[1]).T.astype(jnp.bfloat16)
    acc[...] = jnp.zeros_like(acc)
    cross_top = score(cross_keys, key_bias(lens[me], 0, TOK_DEV), cross_spread, scores_0)
    rest(lambda h: cross_values[pl.ds(h * HD, HD), :], scores_0, start, cross_top)
    o_all[...] = jnp.concatenate([acc[h, 0:HD, :] / acc[h, HD : HD + 1, :] for h in range(2)], axis=0)
    s_all[...] = jnp.concatenate(
        [
            cross_top[:, h * TOK_DEV : (h + 1) * TOK_DEV] + jnp.log2(acc[h, HD : HD + 1, :])
            for h in range(2)
        ]
        + [jnp.zeros((6, TOK_DEV), jnp.float32)],
        axis=0,
    )

    def joined(first, first_lse, second, second_lse):
        outs, lses = [], []
        for h in range(2):
            one, two = first_lse[h : h + 1], second_lse[h : h + 1]
            top = jnp.maximum(one, two)
            one, two = jnp.exp2(one - top), jnp.exp2(two - top)
            both = one + two
            dims = slice(h * HD, (h + 1) * HD)
            outs.append(first[dims] * (one / both) + second[dims] * (two / both))
            lses.append(top + jnp.log2(both))
        return jnp.concatenate(outs, axis=0), lses

    def lanes(at, size):
        return pl.ds(pl.multiple_of(at * size, size), size)

    def wait_for(ref, arrival):
        remote(ref, ref, 0, arrival, "mate").wait_recv()

    half, quarter = TOK_DEV // 2, TOK_DEV // 4
    go(o_all.at[:, lanes(1 - core, half)], o_mate, recv_m.at[0], "mate", 9)
    go(s_all.at[:, lanes(1 - core, half)], s_mate, recv_m.at[1], "mate", 10)
    weights_end(3)
    wait_for(o_mate, recv_m.at[0])
    wait_for(s_mate, recv_m.at[1])
    o, lse = joined(
        o_all[:, lanes(core, half)], s_all[:, lanes(core, half)], o_mate[...], s_mate[...]
    )
    o_half[...] = o.astype(jnp.bfloat16)
    s_half[...] = jnp.concatenate(lse + [jnp.zeros((6, half), jnp.float32)], axis=0)
    go(o_half.at[:, lanes(1 - y, quarter)], o_side, recv_m.at[2], "side", 11)
    go(s_half.at[:, lanes(1 - y, quarter)], s_side, recv_m.at[3], "side", 12)
    wait_for(o_side, recv_m.at[2])
    wait_for(s_side, recv_m.at[3])
    o, lse = joined(
        o_half[:, lanes(y, quarter)].astype(jnp.float32),
        s_half[:, lanes(y, quarter)],
        o_side[...].astype(jnp.float32),
        s_side[...],
    )
    o_rows[...] = o.T.astype(jnp.bfloat16)
    s_rows[...] = jnp.concatenate([jnp.broadcast_to(part, (HD, quarter)) for part in lse], axis=0).T
    few = quarter // NZ

    def few_rows(ref, at):
        return ref.at[pl.ds(pl.multiple_of(at * few, few), few), :]

    for dz in (4, 3, 5, 2, 6, 1, 7):
        at = lax.rem(z + dz, NZ)
        go(few_rows(o_rows, at), o_line.at[z], recv_l.at[0], line_place[dz], 13)
        go(few_rows(s_rows, at), s_line.at[z], recv_l.at[1], line_place[dz], 14)
    o_line[z] = few_rows(o_rows, z)[...]
    s_line[z] = few_rows(s_rows, z)[...]
    wait_for(o_line.at[pl.ds(0, NZ - 1)], recv_l.at[0])
    wait_for(s_line.at[pl.ds(0, NZ - 1)], recv_l.at[1])
    lines = s_line[...]
    factors = jnp.exp2(lines - jnp.max(lines, axis=0, keepdims=True))
    c_all[3] = (
        jnp.sum(o_line[...].astype(jnp.float32) * factors, axis=0) / jnp.sum(factors, axis=0)
    ).astype(jnp.bfloat16)
    for g, to in enumerate(("right", "left", "across")):
        go(c_all.at[3], c_all.at[g], recv_h.at[g], to, 15)
    weights_here(3)
    for g in range(3):
        wait_for(c_all.at[g], recv_h.at[g])
    total = jnp.zeros((few, D), jnp.float32)
    for k in range(4):
        away = lax.rem(k - x + 4, 4)
        g = jnp.where(away == 0, 3, jnp.where(away == 3, 0, away))
        total += dot32(c_all[g], wco_all[g])
    sum_out[...] = total.astype(jnp.bfloat16)
    go(sum_out, sum_in, recv_h.at[3], "partner", 16)

    def place_of(z_at, dy, dc):
        y_at = y if dy == 0 else 1 - y
        c_at = core if dc == 0 else 1 - core
        return c_at * 16 + y_at * NZ + z_at

    mine = place_of(z, 0, 0)
    target_rows = targets[pl.ds(pl.multiple_of(mine * few, few), few), :].astype(jnp.float32)
    slots = z * few + lax.broadcasted_iota(jnp.int32, (few, D), 0)
    wait_for(sum_in, recv_h.at[3])
    total = sum_out[...].astype(jnp.float32) + sum_in[...].astype(jnp.float32)
    live = slots < target_lens[core * 2 + y]
    dec[mine] = (target_rows + jnp.where(live, total, 0.0)).astype(jnp.bfloat16)

    def hand(at, to):
        go(dec.at[at], dec.at[at], recv_d.at[16 if to == "mate" else at - core * 16], to, 17)

    for dz in (4, 3, 5, 2, 6, 1, 7):
        hand(mine, line_place[dz])
    hand(mine, "side")
    hand(mine, "mate")
    for dz in (1, 7, 2, 6, 3, 5, 4):
        at = place_of(lax.rem(z + dz, NZ), 0, 0)
        wait_for(dec.at[at], recv_d.at[at - core * 16])
        hand(at, "side")
        hand(at, "mate")
    for dz in (0, 1, 7, 2, 6, 3, 5, 4):
        at = place_of(lax.rem(z + dz, NZ), 1, 0)
        wait_for(dec.at[at], recv_d.at[at - core * 16])
        hand(at, "mate")
    wait_for(dec.at[pl.ds(pl.multiple_of((1 - core) * 16, 16), 16)], recv_d.at[16])
    sent = (
        wo_all,
        wi_all,
        wf_all,
        wco_all.at[pl.ds(0, 3)],
        kv.at[pl.ds(0, SLOTS - 1)],
        ctx_in,
        out_1,
        out_2,
        enc.at[pl.ds(0, 7)],
        o_mate,
        s_mate,
        o_side,
        s_side,
        o_line.at[pl.ds(0, NZ - 1)],
        s_line.at[pl.ds(0, NZ - 1)],
        c_all.at[pl.ds(0, 3)],
        sum_out,
        dec.at[pl.ds(0, SLOTS - 1)],
    )
    for group, ref in enumerate(sent):
        remote(ref, ref, group, recv_y.at[0], "mate").wait_send()


def layer(lens, tokens, gains, wqkv, wo, wi, wf, targets, wcq, wckv, wco, target_lens):
    hbm = pl.BlockSpec(memory_space=pl.ANY)
    vmem = pl.BlockSpec(memory_space=pltpu.VMEM)
    smem = pl.BlockSpec(memory_space=pltpu.SMEM)
    b16, f32 = jnp.bfloat16, jnp.float32
    gain_attn, gain_ffn, gain_final, gain_cross = (g.reshape(1, D) for g in gains)
    scratch = [
        (tokens.shape, b16),
        ((1, D), f32),
        (wqkv.shape, b16),
        ((1, D), f32),
        ((1, D), f32),
        ((1, D), f32),
        ((SLOTS, 2, 2 * UNIT, 2 * HD), b16),
        ((256, 2 * TOK_DEV), b16),
        ((2, HD + 16, TOK_DEV), f32),
        ((TOK_DEV, 2 * TOK_DEV), f32),
        ((TOK_DEV, 2 * TOK_DEV), f32),
        (wo.shape, b16),
        (wi.shape, b16),
        (wf.shape, b16),
        (targets.shape, b16),
        (wcq.shape, b16),
        (wckv.shape, b16),
        ((3, *wo.shape), b16),
        ((3, *wi.shape), b16),
        ((3, *wf.shape), b16),
        ((TOK_DEV, 2 * HD), b16),
        ((3, ROWS, 2 * HD), b16),
        ((ROWS, D), f32),
        ((ROWS, D), f32),
        ((ROWS, D), b16),
        ((ROWS, D), b16),
        ((ROWS // 2, D), b16),
        ((ROWS // 2, D), b16),
        ((256, 2 * TOK_DEV), b16),
        ((2 * HD, TOK_DEV), b16),
        ((4, *wco.shape), b16),
        ((2 * HD, TOK_DEV), f32),
        ((8, TOK_DEV), f32),
        ((2 * HD, TOK_DEV // 2), f32),
        ((8, TOK_DEV // 2), f32),
        ((2 * HD, TOK_DEV // 2), b16),
        ((8, TOK_DEV // 2), f32),
        ((2 * HD, TOK_DEV // 4), b16),
        ((8, TOK_DEV // 4), f32),
        ((TOK_DEV // 4, 2 * HD), b16),
        ((TOK_DEV // 4, 2 * HD), f32),
        ((NZ, 16, 2 * HD), b16),
        ((NZ, 16, 2 * HD), f32),
        ((4, 16, 2 * HD), b16),
        ((16, D), b16),
        ((16, D), b16),
    ]
    sems = [(16,), (18,), (2, SLOTS), (4, 5), (4,), (2,), (8, 2), (4,), (2,), (4,), (17,)]
    encoded, decoded = pl.pallas_call(
        layer_kernel,
        out_shape=(
            pltpu.VMEM((8, ROWS // 2, D), b16),
            pltpu.VMEM((SLOTS, 16, D), b16),
        ),
        in_specs=[smem] + [hbm] * 13 + [smem],
        out_specs=(vmem, vmem),
        scratch_shapes=[pltpu.VMEM(*s) for s in scratch] + [pltpu.SemaphoreType.DMA(s) for s in sems],
        compiler_params=pltpu.CompilerParams(
            collective_id=0, has_side_effects=True, vmem_limit_bytes=54 << 20
        ),
        name="layer",
    )(lens, tokens, gain_attn, wqkv, gain_ffn, gain_final, gain_cross, wo, wi, wf, targets, wcq, wckv, wco, target_lens)
    return encoded.reshape(TOK_DEV, D), decoded.reshape(targets.shape)


def local(
    tokens,
    norm_attn,
    self_qkv,
    self_out,
    norm_ffn,
    ffn_in,
    ffn_out,
    norm_final,
    pad_lengths,
    targets,
    target_lengths,
    norm_cross,
    cross_query,
    cross_kv,
    cross_out,
):
    return layer(
        pad_lengths,
        tokens,
        (norm_attn, norm_ffn, norm_final, norm_cross),
        self_qkv,
        self_out,
        jnp.swapaxes(ffn_in, 1, 2),
        ffn_out,
        targets,
        cross_query,
        cross_kv,
        cross_out,
        target_lengths,
    )


def solution(mesh):
    in_specs = (
        P("seq", None),
        P(),
        P(None, None, "head"),
        P("head", None),
        P(),
        P(None, None, "head"),
        P("head", None),
        P(),
        P(),
        P(),
        P(),
        P(),
        P(None, "head"),
        P(None, None, "head"),
        P("head", None),
    )
    out_specs = (P("seq", None), P())
    return jax.shard_map(local, mesh=mesh, in_specs=in_specs, out_specs=out_specs, check_vma=False)
```

```python
import functools
import math

import jax
import jax.numpy as jnp
from jax import lax
from jax.experimental import pallas as pl
from jax.experimental.pallas import tpu as pltpu
from jax.sharding import Mesh
from jax.sharding import PartitionSpec as P

D = 1024
HD = 64
TOK_DEV = 512


epsilon = 1e-06
masked_score = -1e30


NZ = 8
SLOTS = 32
UP = (("O", 0, 0), ("O", 0, 1), ("O", 1, 0), ("O", 1, 1), ("O", 2, 0), ("O", 2, 1), ("P", 2, 0), ("O", 3, 0), ("P", 2, 1), ("P", 3, 0))
DOWN = (("O", 0, 1), ("O", 0, 0), ("O", -1, 1), ("O", -1, 0), ("O", -2, 1), ("O", -2, 0), ("P", -2, 1), ("O", -3, 1), ("P", -3, 1), ("P", -2, 0))
SIDE = (("O", 0, 0), ("O", 0, 1), ("O", 1, 0), ("O", -1, 1), ("O", 2, 0), ("O", -2, 1), ("O", 2, 1), ("O", -2, 0), ("O", 1, 1), ("O", -1, 0))
STEPS = 10
FF_DEV = 352
ROWS = 128
UNIT = 256


def link_plan():
    arrive = {("O", 0, 0): -1, ("O", 0, 1): -1}
    arrivals = []
    for s in range(STEPS):
        new = [(UP[s][0], UP[s][1] + 1, UP[s][2]), (DOWN[s][0], DOWN[s][1] - 1, DOWN[s][2])]
        new.append(("P", SIDE[s][1], SIDE[s][2]))
        arrive.update({item: s for item in new})
        arrivals.append(new)
    waiting = {"up": list(UP), "down": list(DOWN), "side": list(SIDE)}
    sent = {name: 0 for name in waiting}
    sends = []
    for s in range(-1, STEPS):
        now = []
        for name, queue in waiting.items():
            while queue and sent[name] <= s + 2 and arrive[queue[0]] <= s:
                now.append((name, queue.pop(0)))
                sent[name] += 1
        sends.append(now)
    return arrivals, sends


ARRIVALS, SENDS = link_plan()
UNITS = (("O", 0, 0), ("O", 0, 1), *(item for step in ARRIVALS for item in step))
STEP_AT = {2: 0, 4: 1, 6: 2, 8: 3, 12: 4, 14: 5, 18: 6, 20: 7, 24: 8, 26: 9}
WEIGHT_STEP_AT = {8: (("pass", 0),), 14: (("start", 2),), 18: (("pass", 1), ("end", 0))}
UNIT_CODES = tuple((4 - d) * 4 + (line == "P") * 2 + half for line, d, half in UNITS)
CODE_WORDS = tuple(
    sum(code << (8 * k) for k, code in enumerate(UNIT_CODES[first : first + 3]))
    for first in range(0, len(UNITS), 3)
)


def key_bias(length, first, rows):
    row = first + lax.broadcasted_iota(jnp.int32, (rows, 128), 0)
    lane = lax.broadcasted_iota(jnp.int32, (rows, 128), 1)
    return jnp.where((lane == 0) & (row >= length), masked_score, 0.0).astype(jnp.bfloat16)


def spread_queries(q_t):
    rows = lax.broadcasted_iota(jnp.int32, (256, 2 * q_t.shape[1]), 0)
    cols = lax.broadcasted_iota(jnp.int32, (256, 2 * q_t.shape[1]), 1)
    half = q_t.shape[1]
    two = jnp.concatenate([q_t, q_t], axis=1)
    full = jnp.concatenate([two, jnp.zeros_like(two)], axis=0)
    keep = ((rows < HD) & (cols < half)) | ((rows >= HD) & (rows < 2 * HD) & (cols >= half))
    return jnp.where(keep, full, jnp.where(rows == 2 * HD, 1.0, 0.0)).astype(jnp.bfloat16)


def normalised(x, gain):
    return x * lax.rsqrt(jnp.mean(x * x, axis=1, keepdims=True) + epsilon) * gain


def dot32(a, b):
    return jnp.dot(a, b, preferred_element_type=jnp.float32)


def layer_kernel(
    lens,
    tokens_hbm,
    gain_attn_hbm,
    wqkv_hbm,
    gain_ffn_hbm,
    gain_final_hbm,
    gain_cross_hbm,
    wo_hbm,
    wi_hbm,
    wf_hbm,
    targets_hbm,
    wcq_hbm,
    wckv_hbm,
    wco_hbm,
    target_lens,
    enc,
    dec,
    tokens,
    gain_attn,
    wqkv,
    gain_ffn,
    gain_final,
    gain_cross,
    kv,
    spread,
    acc,
    scores_0,
    scores_1,
    wo,
    wi,
    wf,
    targets,
    wcq,
    wckv_all,
    wo_all,
    wi_all,
    wf_all,
    ctx,
    ctx_in,
    hidden,
    out_1,
    in_1,
    out_2,
    in_2,
    kvc_out,
    kvc_in,
    cross_spread,
    cross_values,
    wco_all,
    o_all,
    s_all,
    o_mate,
    s_mate,
    o_half,
    s_half,
    o_side,
    s_side,
    o_rows,
    s_rows,
    o_line,
    s_line,
    c_all,
    sum_out,
    sum_in,
    local_sem,
    send,
    recv,
    recv_w,
    recv_c,
    recv_y,
    recv_e,
    recv_m,
    recv_l,
    recv_h,
    recv_d,
    recv_k,
):
    me = lax.axis_index("seq")
    core = lax.rem(me, 2)
    y = lax.rem(me // 2, 2)
    z = me // 4
    head = lax.axis_index("head")
    x = lax.rem(head, 4)
    yh = head // 4

    def index(dz, dy, dc):
        z_at = lax.rem(z + dz + NZ, NZ)
        y_at = y if dy == 0 else 1 - y
        c_at = core if dc == 0 else 1 - core
        return z_at * 4 + y_at * 2 + c_at

    places = {
        "up": {"seq": index(1, 0, 0)},
        "down": {"seq": index(-1, 0, 0)},
        "side": {"seq": index(0, 1, 0)},
        "mate": {"seq": index(0, 0, 1)},
        "right": {"head": yh * 4 + lax.rem(x + 1, 4)},
        "left": {"head": yh * 4 + lax.rem(x + 3, 4)},
        "across": {"head": yh * 4 + lax.rem(x + 2, 4)},
        "partner": {"head": (1 - yh) * 4 + x},
    }
    for dz in range(2, NZ - 1):
        places[dz] = {"seq": index(dz, 0, 0)}
    line_place = {1: "up", NZ - 1: "down", **{dz: dz for dz in range(2, NZ - 1)}}
    barrier = pltpu.get_barrier_semaphore()
    for place in places.values():
        pl.semaphore_signal(barrier, inc=1, device_id=place, device_id_type=pl.DeviceIdType.MESH)

    pairs = {
        "tokens": (tokens_hbm, tokens),
        "wqkv": (wqkv_hbm, wqkv),
        "gain_attn": (gain_attn_hbm, gain_attn),
        "wo": (wo_hbm, wo),
        "wi": (wi_hbm, wi),
        "wf": (wf_hbm, wf),
        "wco": (wco_hbm, wco_all.at[3]),
        "targets": (targets_hbm, targets),
        "wcq": (wcq_hbm, wcq),
        "gain_cross": (gain_cross_hbm, gain_cross),
        "gain_ffn": (gain_ffn_hbm, gain_ffn),
        "gain_final": (gain_final_hbm, gain_final),
        "wckv": (wckv_hbm, wckv_all.at[3]),
    }
    loads = {
        name: pltpu.make_async_copy(source, target, local_sem.at[k])
        for k, (name, (source, target)) in enumerate(pairs.items())
    }
    first_loads = ("tokens", "gain_attn", "wqkv")
    for name in first_loads:
        loads[name].start()
    for name in first_loads:
        loads[name].wait()
    for name, load in loads.items():
        if name not in first_loads:
            load.start()
    normed = normalised(tokens[...].astype(jnp.float32), gain_attn[...]).astype(jnp.bfloat16)
    own_keys = dot32(normed, wqkv[1]).astype(jnp.bfloat16)
    own_values = dot32(normed, wqkv[2]).T.astype(jnp.bfloat16)
    for half in range(2):
        kv[me, half, 0:UNIT, :] = own_keys[half * UNIT : (half + 1) * UNIT, :]
        for k in range(2):
            first = half * UNIT + k * 128
            kv[me, half, pl.ds(UNIT + k * 128, 128), :] = own_values[:, first : first + 128]
    pl.semaphore_wait(barrier, len(places))

    def remote(source, target, number, arrival, place):
        return pltpu.make_async_remote_copy(
            src_ref=source,
            dst_ref=target,
            send_sem=send.at[number],
            recv_sem=arrival,
            device_id=places[place],
            device_id_type=pl.DeviceIdType.MESH,
        )

    def go(source, target, arrival, place, group):
        remote(source, target, group, arrival, place).start()

    def wait_block(half, slot):
        ref = kv.at[slot, half]
        remote(ref, ref, 0, recv.at[half, slot], "mate").wait_recv()

    def push(half, slot, place):
        ref = kv.at[slot, half]
        go(ref, ref, recv.at[half, slot], place, 4)

    def slot_of(line, d):
        return index(-d, 0 if line == "O" else 1, 0)

    for name, (line, d, half) in SENDS[0]:
        push(half, me, name)
    for half in range(2):
        push(half, me, "mate")

    def piece(item, slot, which, c):
        own, gathered = ((wo, wo_all), (wi, wi_all), (wf, wf_all), (wco_all.at[3], wco_all), (wckv_all.at[3], wckv_all))[item]
        ref = own if slot is None else gathered.at[slot]
        if item in (0, 3):
            first, size = ((0, 64), (0, 32), (32, 32))[which]
            return ref.at[pl.ds(pl.multiple_of(c * 64 + first, 32), size), :]
        if item in (1, 4):
            rows = ref.shape[1] // 2
            first, size = ((0, 2 * rows), (0, rows), (rows, rows))[which]
            return ref.at[c, pl.ds(first, size), :]
        first, size = ((0, 176), (0, 96), (96, 80))[which]
        return ref.at[pl.ds(pl.multiple_of(c * 176 + first, 16), size), :]

    def wait_piece(item, slot, which, k, c):
        ref = piece(item, slot, which, c)
        remote(ref, ref, 0, recv_w.at[item, k], "mate").wait_recv()

    def send_piece(item, slot, slot_there, which, k, to):
        source, target = piece(item, slot, which, core), piece(item, slot_there, which, core)
        go(source, target, recv_w.at[item, k], to, 18 if item == 4 else item)

    def weights_start(item):
        loads[("wo", "wi", "wf", "wco", "wckv")[item]].wait()
        for slot, to in ((0, "right"), (1, "left")):
            send_piece(item, None, slot, 0, slot, to)

    def weights_pass(item):
        for slot, half, onward in ((0, 1, "right"), (1, 2, "left")):
            wait_piece(item, slot, 0, slot, core)
            send_piece(item, slot, 2, half, 1 + half, onward)
            send_piece(item, slot, slot, 0, 4, "mate")

    def weights_end(item):
        for half in (1, 2):
            wait_piece(item, 2, half, 1 + half, core)
            send_piece(item, 2, 2, half, 4, "mate")

    def weights_here(item):
        c = 1 - core
        ref = (
            lambda: wo_all.at[:, pl.ds(pl.multiple_of(c * 64, 64), 64), :],
            lambda: wi_all.at[:, c],
            lambda: wf_all.at[:, pl.ds(pl.multiple_of(c * 176, 16), 176), :],
            lambda: wco_all.at[pl.ds(0, 3), pl.ds(pl.multiple_of(c * 64, 64), 64), :],
            lambda: wckv_all.at[pl.ds(0, 3), c],
        )[item]()
        remote(ref, ref, 0, recv_w.at[item, 4], "mate").wait_recv()

    for item in range(2):
        weights_start(item)
    q_t = dot32(normed, wqkv[0]).T

    spread[...] = spread_queries(q_t * (HD ** (-0.5) * math.log2(math.e)))
    acc[...] = jnp.zeros_like(acc)
    for name in ("targets", "wcq", "gain_cross", "gain_ffn", "gain_final"):
        loads[name].wait()
    cross_normed = normalised(targets[...].astype(jnp.float32), gain_cross[...]).astype(jnp.bfloat16)
    cross_spread[...] = spread_queries(
        dot32(cross_normed, wcq[...]).T * (HD ** (-0.5) * math.log2(math.e))
    )

    def step(s):
        for line, d, half in ARRIVALS[s]:
            slot = slot_of(line, d)
            wait_block(half, slot)
            push(half, slot, "mate")
        for name, (line, d, half) in SENDS[s + 1]:
            push(half, slot_of(line, d), name)

    def unit_of(u):
        third = u // 3
        word = jnp.int32(CODE_WORDS[0])
        for k in range(1, len(CODE_WORDS)):
            word = jnp.where(third == k, CODE_WORDS[k], word)
        code = lax.rem(lax.shift_right_logical(word, 8 * (u - 3 * third)), 256)
        half = lax.rem(code, 2)
        chip = lax.rem(z + code // 4 + 4, NZ) * 4 + lax.rem(y + code // 2, 2) * 2
        return chip + core, chip + 1 - core, half

    def score(block, bias, queries, into):
        s = dot32(jnp.concatenate([block, bias], axis=1), queries[...])
        into[...] = s
        return jnp.max(s, axis=0, keepdims=True)

    def unit_score(unit, into):
        here, there, half = unit
        block = jnp.concatenate([kv[here, half, 0:UNIT, :], kv[there, half, 0:UNIT, :]], axis=0)
        bias = jnp.concatenate(
            [key_bias(lens[slot], half * UNIT, UNIT) for slot in (here, there)], axis=0
        )
        return score(block, bias, spread, into)

    def rest(rows_of_head, held, old, top):
        p = jnp.exp2(held[...] - top).astype(jnp.bfloat16)
        shrink = jnp.exp2(old - top)
        ones = jnp.ones((16, TOK_DEV), jnp.bfloat16)
        for h in range(2):
            cols = slice(h * TOK_DEV, (h + 1) * TOK_DEV)
            lhs = jnp.concatenate([rows_of_head(h), ones], axis=0)
            acc[h] = acc[h] * shrink[:, cols] + dot32(lhs, p[:, cols])

    def unit_rest(unit, held, old, top):
        here, there, half = unit

        def rows_of_head(h):
            return jnp.concatenate(
                [
                    kv[slot, half, pl.ds(UNIT + k * 128 + h * HD, HD), :]
                    for slot in (here, there)
                    for k in range(2)
                ],
                axis=1,
            )

        rest(rows_of_head, held, old, top)

    acts = {"start": weights_start, "pass": weights_pass, "end": weights_end}

    def handle(u):
        for at in sorted({*STEP_AT, *WEIGHT_STEP_AT}):

            @pl.when(u == at)
            def _():
                if at in STEP_AT:
                    step(STEP_AT[at])
                for what, item in WEIGHT_STEP_AT.get(at, ()):
                    acts[what](item)

    def wait_mate(unit):
        here, there, half = unit
        wait_block(half, there)

    start = jnp.full((1, 2 * TOK_DEV), masked_score, jnp.float32)
    zero = jnp.int32(0)
    first, second = unit_of(zero), unit_of(zero + 1)
    wait_mate(first)
    wait_mate(second)
    top = unit_score(first, scores_0)
    following = jnp.maximum(top, unit_score(second, scores_1))
    unit_rest(first, scores_0, start, top)

    def body(j, carry):
        old, top, before = carry
        u = 2 * j
        here, after = unit_of(u), unit_of(u + 1)
        handle(u)
        wait_mate(here)
        wait_mate(after)
        later = jnp.maximum(top, unit_score(here, scores_0))
        unit_rest(before, scores_1, old, top)
        old, top = top, later
        later = jnp.maximum(top, unit_score(after, scores_1))
        unit_rest(here, scores_0, old, top)
        return top, later, after

    old, top, last = lax.fori_loop(1, len(UNITS) // 2, body, (top, following, second))
    unit_rest(last, scores_1, old, top)
    both = jnp.concatenate([acc[h, 0:HD, :] / acc[h, HD : HD + 1, :] for h in range(2)], axis=0)
    ctx[...] = both.T.astype(jnp.bfloat16)

    def ctx_rows(at):
        return ctx.at[pl.ds(pl.multiple_of(lax.rem(at, 4) * ROWS, ROWS), ROWS), :]

    for g, (to, at) in enumerate((("right", x + 1), ("left", x + 3), ("across", x + 2))):
        go(ctx_rows(at), ctx_in.at[g], recv_c.at[g], to, 5)
    weights_pass(2)
    weights_here(0)
    weights_end(1)
    total = dot32(ctx_rows(x)[...], wo[...])
    for g in range(3):
        remote(ctx_in.at[g], ctx_in.at[g], 0, recv_c.at[g], "mate").wait_recv()
        total += dot32(ctx_in[g], wo_all[g])
    out_1[...] = total.astype(jnp.bfloat16)
    go(out_1, in_1, recv_y.at[0], "partner", 6)
    weights_start(4)
    weights_end(2)
    weights_here(1)
    weights_here(2)
    remote(out_1, in_1, 0, recv_y.at[0], "partner").wait_recv()
    total = out_1[...].astype(jnp.float32) + in_1[...].astype(jnp.float32)
    total += tokens[pl.ds(pl.multiple_of(x * ROWS, ROWS), ROWS), :].astype(jnp.float32)
    hidden[...] = total
    ffn_normed = normalised(total, gain_ffn[...]).T.astype(jnp.bfloat16)
    ffn = jnp.zeros((ROWS, D), jnp.float32)
    for g in range(4):
        gate_w, up_w, down_w = (
            (wi[0], wi[1], wf[...]) if g == 3 else (wi_all[g, 0], wi_all[g, 1], wf_all[g])
        )
        gate = dot32(gate_w, ffn_normed)
        up = dot32(up_w, ffn_normed)
        activated = (jax.nn.gelu(gate, approximate=True) * up).T.astype(jnp.bfloat16)
        ffn += dot32(activated, down_w)
        if g == 1:
            weights_pass(4)
    out_2[...] = ffn.astype(jnp.bfloat16)
    go(out_2, in_2, recv_y.at[1], "partner", 7)
    weights_end(4)
    weights_start(3)
    weights_here(4)
    remote(out_2, in_2, 0, recv_y.at[1], "partner").wait_recv()
    final = out_2[...].astype(jnp.float32) + in_2[...].astype(jnp.float32)
    final += hidden[...]
    rows_here = normalised(final, gain_final[...]).astype(jnp.bfloat16)
    enc[x] = rows_here

    def cross_pair(slot):
        weights = jnp.concatenate([wckv_all[slot, 0], wckv_all[slot, 1]], axis=1)
        return dot32(rows_here, weights).astype(jnp.bfloat16)

    for slot, to in ((2, "across"), (0, "left"), (1, "right")):
        both = cross_pair(slot)
        kvc_out[slot, 0] = both[:, : 2 * HD]
        kvc_out[slot, 1] = both[:, 2 * HD :]
        go(kvc_out.at[slot], kvc_in.at[x], recv_k.at[x], to, 19)
    both = cross_pair(3)
    kvc_in[x, 0] = both[:, : 2 * HD]
    kvc_in[x, 1] = both[:, 2 * HD :]

    def beside(dx):
        return lax.rem(x + dx + 4, 4)

    for dx in (-1, 1, 2):
        ref = kvc_in.at[beside(dx)]
        remote(ref, ref, 0, recv_k.at[beside(dx)], "mate").wait_recv()

    def rows_of(at, half):
        if half is None:
            return enc.at[at]
        return enc.at[at, pl.ds(half * 64, 64), :]

    def send_share(at, half, to):
        go(rows_of(at, half), rows_of(at, half), recv_e.at[at, half or 0], to, 8)

    def wait_share(at, half):
        ref = rows_of(at, half)
        remote(ref, ref, 0, recv_e.at[at, half or 0], "mate").wait_recv()

    weights_pass(3)
    cross_keys = jnp.concatenate([kvc_in[k, 0] for k in range(4)], axis=0)
    cross_rows = jnp.concatenate([kvc_in[k, 1] for k in range(4)], axis=0)
    cross_values[...] = cross_rows.astype(jnp.float32).T.astype(jnp.bfloat16)
    acc[...] = jnp.zeros_like(acc)
    cross_top = score(cross_keys, key_bias(lens[me], 0, TOK_DEV), cross_spread, scores_0)
    rest(lambda h: cross_values[pl.ds(h * HD, HD), :], scores_0, start, cross_top)
    o_all[...] = jnp.concatenate([acc[h, 0:HD, :] / acc[h, HD : HD + 1, :] for h in range(2)], axis=0)
    s_all[...] = jnp.concatenate(
        [
            cross_top[:, h * TOK_DEV : (h + 1) * TOK_DEV] + jnp.log2(acc[h, HD : HD + 1, :])
            for h in range(2)
        ]
        + [jnp.zeros((6, TOK_DEV), jnp.float32)],
        axis=0,
    )

    def joined(first, first_lse, second, second_lse):
        outs, lses = [], []
        for h in range(2):
            one, two = first_lse[h : h + 1], second_lse[h : h + 1]
            top = jnp.maximum(one, two)
            one, two = jnp.exp2(one - top), jnp.exp2(two - top)
            both = one + two
            dims = slice(h * HD, (h + 1) * HD)
            outs.append(first[dims] * (one / both) + second[dims] * (two / both))
            lses.append(top + jnp.log2(both))
        return jnp.concatenate(outs, axis=0), lses

    def lanes(at, size):
        return pl.ds(pl.multiple_of(at * size, size), size)

    def wait_for(ref, arrival):
        remote(ref, ref, 0, arrival, "mate").wait_recv()

    half, quarter = TOK_DEV // 2, TOK_DEV // 4
    go(o_all.at[:, lanes(1 - core, half)], o_mate, recv_m.at[0], "mate", 9)
    go(s_all.at[:, lanes(1 - core, half)], s_mate, recv_m.at[1], "mate", 10)
    for to in ("right", "left"):
        send_share(x, None, to)
    wait_for(o_mate, recv_m.at[0])
    wait_for(s_mate, recv_m.at[1])
    o, lse = joined(
        o_all[:, lanes(core, half)], s_all[:, lanes(core, half)], o_mate[...], s_mate[...]
    )
    o_half[...] = o.astype(jnp.bfloat16)
    s_half[...] = jnp.concatenate(lse + [jnp.zeros((6, half), jnp.float32)], axis=0)
    go(o_half.at[:, lanes(1 - y, quarter)], o_side, recv_m.at[2], "side", 11)
    go(s_half.at[:, lanes(1 - y, quarter)], s_side, recv_m.at[3], "side", 12)
    wait_for(o_side, recv_m.at[2])
    wait_for(s_side, recv_m.at[3])
    o, lse = joined(
        o_half[:, lanes(y, quarter)].astype(jnp.float32),
        s_half[:, lanes(y, quarter)],
        o_side[...].astype(jnp.float32),
        s_side[...],
    )
    o_rows[...] = o.T.astype(jnp.bfloat16)
    s_rows[...] = jnp.concatenate([jnp.broadcast_to(part, (HD, quarter)) for part in lse], axis=0).T
    few = quarter // NZ

    def few_rows(ref, at):
        return ref.at[pl.ds(pl.multiple_of(at * few, few), few), :]

    for dz in (4, 3, 5, 2, 6, 1, 7):
        at = lax.rem(z + dz, NZ)
        go(few_rows(o_rows, at), o_line.at[z], recv_l.at[0], line_place[dz], 13)
        go(few_rows(s_rows, at), s_line.at[z], recv_l.at[1], line_place[dz], 14)
    for dx, half, to in ((-1, 0, "right"), (1, 1, "left")):
        wait_share(beside(dx), None)
        send_share(beside(dx), half, to)
    weights_end(3)
    o_line[z] = few_rows(o_rows, z)[...]
    s_line[z] = few_rows(s_rows, z)[...]
    wait_for(o_line.at[pl.ds(0, NZ - 1)], recv_l.at[0])
    wait_for(s_line.at[pl.ds(0, NZ - 1)], recv_l.at[1])
    lines = s_line[...]
    factors = jnp.exp2(lines - jnp.max(lines, axis=0, keepdims=True))
    c_all[3] = (
        jnp.sum(o_line[...].astype(jnp.float32) * factors, axis=0) / jnp.sum(factors, axis=0)
    ).astype(jnp.bfloat16)
    for g, to in enumerate(("right", "left", "across")):
        go(c_all.at[3], c_all.at[g], recv_h.at[g], to, 15)
    weights_here(3)
    for g in range(3):
        wait_for(c_all.at[g], recv_h.at[g])
    total = jnp.zeros((few, D), jnp.float32)
    for k in range(4):
        away = lax.rem(k - x + 4, 4)
        g = jnp.where(away == 0, 3, jnp.where(away == 3, 0, away))
        total += dot32(c_all[g], wco_all[g])
    sum_out[...] = total.astype(jnp.bfloat16)
    go(sum_out, sum_in, recv_h.at[3], "partner", 16)

    def place_of(z_at, dy, dc):
        y_at = y if dy == 0 else 1 - y
        c_at = core if dc == 0 else 1 - core
        return c_at * 16 + y_at * NZ + z_at

    mine = place_of(z, 0, 0)
    target_rows = targets[pl.ds(pl.multiple_of(mine * few, few), few), :].astype(jnp.float32)
    slots = z * few + lax.broadcasted_iota(jnp.int32, (few, D), 0)
    wait_for(sum_in, recv_h.at[3])
    total = sum_out[...].astype(jnp.float32) + sum_in[...].astype(jnp.float32)
    live = slots < target_lens[core * 2 + y]
    dec[mine] = (target_rows + jnp.where(live, total, 0.0)).astype(jnp.bfloat16)

    def hand(at, to):
        go(dec.at[at], dec.at[at], recv_d.at[16 if to == "mate" else at - core * 16], to, 17)

    for dz in (4, 3, 5, 2, 6, 1, 7):
        hand(mine, line_place[dz])
    hand(mine, "side")
    hand(mine, "mate")
    for dz in (1, 7, 2, 6, 3, 5, 4):
        at = place_of(lax.rem(z + dz, NZ), 0, 0)
        wait_for(dec.at[at], recv_d.at[at - core * 16])
        hand(at, "side")
        hand(at, "mate")
    for dz in (0, 1, 7, 2, 6, 3, 5, 4):
        at = place_of(lax.rem(z + dz, NZ), 1, 0)
        wait_for(dec.at[at], recv_d.at[at - core * 16])
        hand(at, "mate")
    wait_for(dec.at[pl.ds(pl.multiple_of((1 - core) * 16, 16), 16)], recv_d.at[16])
    for half in (0, 1):
        wait_share(beside(2), half)
    sent = (
        wo_all,
        wi_all,
        wf_all,
        wco_all.at[pl.ds(0, 3)],
        kv.at[pl.ds(0, SLOTS - 1)],
        ctx_in,
        out_1,
        out_2,
        enc.at[pl.ds(0, 3)],
        o_mate,
        s_mate,
        o_side,
        s_side,
        o_line.at[pl.ds(0, NZ - 1)],
        s_line.at[pl.ds(0, NZ - 1)],
        c_all.at[pl.ds(0, 3)],
        sum_out,
        dec.at[pl.ds(0, SLOTS - 1)],
        wckv_all.at[pl.ds(0, 3)],
        kvc_out,
    )
    for group, ref in enumerate(sent):
        remote(ref, ref, group, recv_y.at[0], "mate").wait_send()


def layer(lens, tokens, gains, wqkv, wo, wi, wf, targets, wcq, wckv, wco, target_lens):
    hbm = pl.BlockSpec(memory_space=pl.ANY)
    vmem = pl.BlockSpec(memory_space=pltpu.VMEM)
    smem = pl.BlockSpec(memory_space=pltpu.SMEM)
    b16, f32 = jnp.bfloat16, jnp.float32
    gain_attn, gain_ffn, gain_final, gain_cross = (g.reshape(1, D) for g in gains)
    scratch = [
        (tokens.shape, b16),
        ((1, D), f32),
        (wqkv.shape, b16),
        ((1, D), f32),
        ((1, D), f32),
        ((1, D), f32),
        ((SLOTS, 2, 2 * UNIT, 2 * HD), b16),
        ((256, 2 * TOK_DEV), b16),
        ((2, HD + 16, TOK_DEV), f32),
        ((TOK_DEV, 2 * TOK_DEV), f32),
        ((TOK_DEV, 2 * TOK_DEV), f32),
        (wo.shape, b16),
        (wi.shape, b16),
        (wf.shape, b16),
        (targets.shape, b16),
        (wcq.shape, b16),
        ((4, *wckv.shape), b16),
        ((3, *wo.shape), b16),
        ((3, *wi.shape), b16),
        ((3, *wf.shape), b16),
        ((TOK_DEV, 2 * HD), b16),
        ((3, ROWS, 2 * HD), b16),
        ((ROWS, D), f32),
        ((ROWS, D), b16),
        ((ROWS, D), b16),
        ((ROWS, D), b16),
        ((ROWS, D), b16),
        ((3, 2, ROWS, 2 * HD), b16),
        ((4, 2, ROWS, 2 * HD), b16),
        ((256, 2 * TOK_DEV), b16),
        ((2 * HD, TOK_DEV), b16),
        ((4, *wco.shape), b16),
        ((2 * HD, TOK_DEV), f32),
        ((8, TOK_DEV), f32),
        ((2 * HD, TOK_DEV // 2), f32),
        ((8, TOK_DEV // 2), f32),
        ((2 * HD, TOK_DEV // 2), b16),
        ((8, TOK_DEV // 2), f32),
        ((2 * HD, TOK_DEV // 4), b16),
        ((8, TOK_DEV // 4), f32),
        ((TOK_DEV // 4, 2 * HD), b16),
        ((TOK_DEV // 4, 2 * HD), f32),
        ((NZ, 16, 2 * HD), b16),
        ((NZ, 16, 2 * HD), f32),
        ((4, 16, 2 * HD), b16),
        ((16, D), b16),
        ((16, D), b16),
    ]
    sems = [(16,), (20,), (2, SLOTS), (5, 5), (3,), (2,), (4, 2), (4,), (2,), (4,), (17,), (4,)]
    encoded, decoded = pl.pallas_call(
        layer_kernel,
        out_shape=(
            pltpu.VMEM((4, ROWS, D), b16),
            pltpu.VMEM((SLOTS, 16, D), b16),
        ),
        in_specs=[smem] + [hbm] * 13 + [smem],
        out_specs=(vmem, vmem),
        scratch_shapes=[pltpu.VMEM(*s) for s in scratch] + [pltpu.SemaphoreType.DMA(s) for s in sems],
        compiler_params=pltpu.CompilerParams(
            collective_id=0, has_side_effects=True, vmem_limit_bytes=54 << 20
        ),
        name="layer",
    )(lens, tokens, gain_attn, wqkv, gain_ffn, gain_final, gain_cross, wo, wi, wf, targets, wcq, wckv, wco, target_lens)
    return encoded.reshape(TOK_DEV, D), decoded.reshape(targets.shape)


def local(
    tokens,
    norm_attn,
    self_qkv,
    self_out,
    norm_ffn,
    ffn_in,
    ffn_out,
    norm_final,
    pad_lengths,
    targets,
    target_lengths,
    norm_cross,
    cross_query,
    cross_kv,
    cross_out,
):
    return layer(
        pad_lengths,
        tokens,
        (norm_attn, norm_ffn, norm_final, norm_cross),
        self_qkv,
        self_out,
        jnp.swapaxes(ffn_in, 1, 2),
        ffn_out,
        targets,
        cross_query,
        cross_kv,
        cross_out,
        target_lengths,
    )


def solution(mesh):
    in_specs = (
        P("seq", None),
        P(),
        P(None, None, "head"),
        P("head", None),
        P(),
        P(None, None, "head"),
        P("head", None),
        P(),
        P(),
        P(),
        P(),
        P(),
        P(None, "head"),
        P(None, None, "head"),
        P("head", None),
    )
    out_specs = (P("seq", None), P())
    return jax.shard_map(local, mesh=mesh, in_specs=in_specs, out_specs=out_specs, check_vma=False)
```

```python
import functools
import math

import jax
import jax.numpy as jnp
from jax import lax
from jax.experimental import pallas as pl
from jax.experimental.pallas import tpu as pltpu
from jax.sharding import Mesh
from jax.sharding import PartitionSpec as P

D = 1024
HD = 64
TOK_DEV = 512


epsilon = 1e-06
masked_score = -1e30


NZ = 8
SLOTS = 32
UP = (("O", 0, 0), ("O", 0, 1), ("O", 1, 0), ("O", 1, 1), ("O", 2, 0), ("O", 2, 1), ("P", 2, 0), ("O", 3, 0), ("P", 2, 1), ("P", 3, 0))
DOWN = (("O", 0, 1), ("O", 0, 0), ("O", -1, 1), ("O", -1, 0), ("O", -2, 1), ("O", -2, 0), ("P", -2, 1), ("O", -3, 1), ("P", -3, 1), ("P", -2, 0))
SIDE = (("O", 0, 0), ("O", 0, 1), ("O", 1, 0), ("O", -1, 1), ("O", 2, 0), ("O", -2, 1), ("O", 2, 1), ("O", -2, 0), ("O", 1, 1), ("O", -1, 0))
STEPS = 10
FF_DEV = 352
ROWS = 128
UNIT = 256


def link_plan():
    arrive = {("O", 0, 0): -1, ("O", 0, 1): -1}
    arrivals = []
    for s in range(STEPS):
        new = [(UP[s][0], UP[s][1] + 1, UP[s][2]), (DOWN[s][0], DOWN[s][1] - 1, DOWN[s][2])]
        new.append(("P", SIDE[s][1], SIDE[s][2]))
        arrive.update({item: s for item in new})
        arrivals.append(new)
    waiting = {"up": list(UP), "down": list(DOWN), "side": list(SIDE)}
    sent = {name: 0 for name in waiting}
    sends = []
    for s in range(-1, STEPS):
        now = []
        for name, queue in waiting.items():
            while queue and sent[name] <= s + 2 and arrive[queue[0]] <= s:
                now.append((name, queue.pop(0)))
                sent[name] += 1
        sends.append(now)
    return arrivals, sends


ARRIVALS, SENDS = link_plan()
UNITS = (("O", 0, 0), ("O", 0, 1), *(item for step in ARRIVALS for item in step))
MATE_AT = {(2 + 3 * s) // 2 * 2: s for s in range(STEPS)}
STEP_AT = {2: 0, 4: 1, 6: 2, 8: 3, 12: 4, 14: 5, 18: 6, 20: 7, 24: 8, 26: 9}
WEIGHT_STEP_AT = {8: (("pass", 0),), 14: (("start", 2),), 18: (("pass", 1), ("end", 0))}
UNIT_CODES = tuple((4 - d) * 4 + (line == "P") * 2 + half for line, d, half in UNITS)
CODE_WORDS = tuple(
    sum(code << (8 * k) for k, code in enumerate(UNIT_CODES[first : first + 3]))
    for first in range(0, len(UNITS), 3)
)


def key_bias(length, first, rows):
    row = first + lax.broadcasted_iota(jnp.int32, (rows, 128), 0)
    lane = lax.broadcasted_iota(jnp.int32, (rows, 128), 1)
    return jnp.where((lane == 0) & (row >= length), masked_score, 0.0).astype(jnp.bfloat16)


def spread_queries(q_t):
    rows = lax.broadcasted_iota(jnp.int32, (256, 2 * q_t.shape[1]), 0)
    cols = lax.broadcasted_iota(jnp.int32, (256, 2 * q_t.shape[1]), 1)
    half = q_t.shape[1]
    two = jnp.concatenate([q_t, q_t], axis=1)
    full = jnp.concatenate([two, jnp.zeros_like(two)], axis=0)
    keep = ((rows < HD) & (cols < half)) | ((rows >= HD) & (rows < 2 * HD) & (cols >= half))
    return jnp.where(keep, full, jnp.where(rows == 2 * HD, 1.0, 0.0)).astype(jnp.bfloat16)


def normalised(x, gain):
    return x * lax.rsqrt(jnp.mean(x * x, axis=1, keepdims=True) + epsilon) * gain


def dot32(a, b):
    return jnp.dot(a, b, preferred_element_type=jnp.float32)


def layer_kernel(
    lens,
    tokens_hbm,
    gain_attn_hbm,
    wqkv_hbm,
    gain_ffn_hbm,
    gain_final_hbm,
    gain_cross_hbm,
    wo_hbm,
    wi_hbm,
    wf_hbm,
    targets_hbm,
    wcq_hbm,
    wckv_hbm,
    wco_hbm,
    target_lens,
    enc,
    dec,
    tokens,
    gain_attn,
    wqkv,
    gain_ffn,
    gain_final,
    gain_cross,
    kv,
    spread,
    acc,
    scores_0,
    scores_1,
    wo,
    wi,
    wf,
    targets,
    wcq,
    wckv_all,
    wo_all,
    wi_all,
    wf_all,
    ctx,
    ctx_in,
    hidden,
    out_1,
    in_1,
    out_2,
    in_2,
    kvc_out,
    kvc_in,
    cross_spread,
    cross_values,
    wco_all,
    o_all,
    s_all,
    o_mate,
    s_mate,
    o_half,
    s_half,
    o_side,
    s_side,
    o_rows,
    s_rows,
    o_line,
    s_line,
    c_all,
    sum_out,
    sum_in,
    local_sem,
    send,
    recv,
    recv_w,
    recv_c,
    recv_y,
    recv_e,
    recv_m,
    recv_l,
    recv_h,
    recv_d,
    recv_k,
):
    me = lax.axis_index("seq")
    core = lax.rem(me, 2)
    y = lax.rem(me // 2, 2)
    z = me // 4
    head = lax.axis_index("head")
    x = lax.rem(head, 4)
    yh = head // 4

    def index(dz, dy, dc):
        z_at = lax.rem(z + dz + NZ, NZ)
        y_at = y if dy == 0 else 1 - y
        c_at = core if dc == 0 else 1 - core
        return z_at * 4 + y_at * 2 + c_at

    places = {
        "up": {"seq": index(1, 0, 0)},
        "down": {"seq": index(-1, 0, 0)},
        "side": {"seq": index(0, 1, 0)},
        "mate": {"seq": index(0, 0, 1)},
        "right": {"head": yh * 4 + lax.rem(x + 1, 4)},
        "left": {"head": yh * 4 + lax.rem(x + 3, 4)},
        "across": {"head": yh * 4 + lax.rem(x + 2, 4)},
        "partner": {"head": (1 - yh) * 4 + x},
    }
    for dz in range(2, NZ - 1):
        places[dz] = {"seq": index(dz, 0, 0)}
    line_place = {1: "up", NZ - 1: "down", **{dz: dz for dz in range(2, NZ - 1)}}
    barrier = pltpu.get_barrier_semaphore()
    for place in places.values():
        pl.semaphore_signal(barrier, inc=1, device_id=place, device_id_type=pl.DeviceIdType.MESH)

    pairs = {
        "tokens": (tokens_hbm, tokens),
        "wqkv": (wqkv_hbm, wqkv),
        "gain_attn": (gain_attn_hbm, gain_attn),
        "wo": (wo_hbm, wo),
        "wi": (wi_hbm, wi),
        "wf": (wf_hbm, wf),
        "wco": (wco_hbm, wco_all.at[3]),
        "targets": (targets_hbm, targets),
        "wcq": (wcq_hbm, wcq),
        "gain_cross": (gain_cross_hbm, gain_cross),
        "gain_ffn": (gain_ffn_hbm, gain_ffn),
        "gain_final": (gain_final_hbm, gain_final),
        "wckv": (wckv_hbm, wckv_all.at[3]),
    }
    loads = {
        name: pltpu.make_async_copy(source, target, local_sem.at[k])
        for k, (name, (source, target)) in enumerate(pairs.items())
    }
    first_loads = ("tokens", "gain_attn", "wqkv")
    for name in first_loads:
        loads[name].start()
    for name in first_loads:
        loads[name].wait()
    for name, load in loads.items():
        if name not in first_loads:
            load.start()
    normed = normalised(tokens[...].astype(jnp.float32), gain_attn[...]).astype(jnp.bfloat16)
    own_keys = dot32(normed, wqkv[1]).astype(jnp.bfloat16)
    own_values = dot32(normed, wqkv[2]).T.astype(jnp.bfloat16)
    for half in range(2):
        kv[me, half, 0:UNIT, :] = own_keys[half * UNIT : (half + 1) * UNIT, :]
        for k in range(2):
            first = half * UNIT + k * 128
            kv[me, half, pl.ds(UNIT + k * 128, 128), :] = own_values[:, first : first + 128]
    pl.semaphore_wait(barrier, len(places))

    def remote(source, target, number, arrival, place):
        return pltpu.make_async_remote_copy(
            src_ref=source,
            dst_ref=target,
            send_sem=send.at[number],
            recv_sem=arrival,
            device_id=places[place],
            device_id_type=pl.DeviceIdType.MESH,
        )

    def go(source, target, arrival, place, group):
        remote(source, target, group, arrival, place).start()

    def wait_step(mate_side, s):
        ref = kv.at[pl.ds(0, 3), 0]
        remote(ref, ref, 0, recv.at[mate_side, s], "mate").wait_recv()

    def push(half, slot, place, s):
        ref = kv.at[slot, half]
        go(ref, ref, recv.at[int(place == "mate"), s], place, 4)

    def slot_of(line, d):
        return index(-d, 0 if line == "O" else 1, 0)

    link_items = {"up": UP, "down": DOWN, "side": SIDE}
    for name, item in SENDS[0]:
        push(item[2], me, name, link_items[name].index(item))
    for half in range(2):
        push(half, me, "mate", STEPS)

    def piece(item, slot, which, c):
        own, gathered = ((wo, wo_all), (wi, wi_all), (wf, wf_all), (wco_all.at[3], wco_all), (wckv_all.at[3], wckv_all))[item]
        ref = own if slot is None else gathered.at[slot]
        if item in (0, 3):
            first, size = ((0, 64), (0, 32), (32, 32))[which]
            return ref.at[pl.ds(pl.multiple_of(c * 64 + first, 32), size), :]
        if item in (1, 4):
            rows = ref.shape[1] // 2
            first, size = ((0, 2 * rows), (0, rows), (rows, rows))[which]
            return ref.at[c, pl.ds(first, size), :]
        first, size = ((0, 176), (0, 96), (96, 80))[which]
        return ref.at[pl.ds(pl.multiple_of(c * 176 + first, 16), size), :]

    def wait_piece(item, slot, which, k, c):
        ref = piece(item, slot, which, c)
        remote(ref, ref, 0, recv_w.at[item, k], "mate").wait_recv()

    def send_piece(item, slot, slot_there, which, k, to):
        source, target = piece(item, slot, which, core), piece(item, slot_there, which, core)
        go(source, target, recv_w.at[item, k], to, 18 if item == 4 else item)

    def weights_start(item):
        loads[("wo", "wi", "wf", "wco", "wckv")[item]].wait()
        for slot, to in ((0, "right"), (1, "left")):
            send_piece(item, None, slot, 0, slot, to)

    def weights_pass(item):
        for slot, half, onward in ((0, 1, "right"), (1, 2, "left")):
            wait_piece(item, slot, 0, slot, core)
            send_piece(item, slot, 2, half, 1 + half, onward)
            send_piece(item, slot, slot, 0, 4, "mate")

    def weights_end(item):
        for half in (1, 2):
            wait_piece(item, 2, half, 1 + half, core)
            send_piece(item, 2, 2, half, 4, "mate")

    def weights_here(item):
        c = 1 - core
        ref = (
            lambda: wo_all.at[:, pl.ds(pl.multiple_of(c * 64, 64), 64), :],
            lambda: wi_all.at[:, c],
            lambda: wf_all.at[:, pl.ds(pl.multiple_of(c * 176, 16), 176), :],
            lambda: wco_all.at[pl.ds(0, 3), pl.ds(pl.multiple_of(c * 64, 64), 64), :],
            lambda: wckv_all.at[pl.ds(0, 3), c],
        )[item]()
        remote(ref, ref, 0, recv_w.at[item, 4], "mate").wait_recv()

    for item in range(2):
        weights_start(item)
    q_t = dot32(normed, wqkv[0]).T

    spread[...] = spread_queries(q_t * (HD ** (-0.5) * math.log2(math.e)))
    acc[...] = jnp.zeros_like(acc)
    for name in ("targets", "wcq", "gain_cross", "gain_ffn", "gain_final"):
        loads[name].wait()
    cross_normed = normalised(targets[...].astype(jnp.float32), gain_cross[...]).astype(jnp.bfloat16)
    cross_spread[...] = spread_queries(
        dot32(cross_normed, wcq[...]).T * (HD ** (-0.5) * math.log2(math.e))
    )

    def step(s):
        wait_step(0, s)
        for line, d, half in ARRIVALS[s]:
            push(half, slot_of(line, d), "mate", s)
        for name, item in SENDS[s + 1]:
            line, d, half = item
            push(half, slot_of(line, d), name, link_items[name].index(item))

    def unit_of(u):
        third = u // 3
        word = jnp.int32(CODE_WORDS[0])
        for k in range(1, len(CODE_WORDS)):
            word = jnp.where(third == k, CODE_WORDS[k], word)
        code = lax.rem(lax.shift_right_logical(word, 8 * (u - 3 * third)), 256)
        half = lax.rem(code, 2)
        chip = lax.rem(z + code // 4 + 4, NZ) * 4 + lax.rem(y + code // 2, 2) * 2
        return chip + core, chip + 1 - core, half

    def score(block, bias, queries, into):
        s = dot32(jnp.concatenate([block, bias], axis=1), queries[...])
        into[...] = s
        return jnp.max(s, axis=0, keepdims=True)

    def unit_score(unit, into):
        here, there, half = unit
        block = jnp.concatenate([kv[here, half, 0:UNIT, :], kv[there, half, 0:UNIT, :]], axis=0)
        bias = jnp.concatenate(
            [key_bias(lens[slot], half * UNIT, UNIT) for slot in (here, there)], axis=0
        )
        return score(block, bias, spread, into)

    def rest(rows_of_head, held, old, top):
        p = jnp.exp2(held[...] - top).astype(jnp.bfloat16)
        shrink = jnp.exp2(old - top)
        ones = jnp.ones((16, TOK_DEV), jnp.bfloat16)
        for h in range(2):
            cols = slice(h * TOK_DEV, (h + 1) * TOK_DEV)
            lhs = jnp.concatenate([rows_of_head(h), ones], axis=0)
            acc[h] = acc[h] * shrink[:, cols] + dot32(lhs, p[:, cols])

    def unit_rest(unit, held, old, top):
        here, there, half = unit

        def rows_of_head(h):
            return jnp.concatenate(
                [
                    kv[slot, half, pl.ds(UNIT + k * 128 + h * HD, HD), :]
                    for slot in (here, there)
                    for k in range(2)
                ],
                axis=1,
            )

        rest(rows_of_head, held, old, top)

    acts = {"start": weights_start, "pass": weights_pass, "end": weights_end}

    def handle(u):
        for at in sorted({*STEP_AT, *MATE_AT, *WEIGHT_STEP_AT}):

            @pl.when(u == at)
            def _():
                if at in STEP_AT:
                    step(STEP_AT[at])
                for what, item in WEIGHT_STEP_AT.get(at, ()):
                    acts[what](item)
                if at in MATE_AT:
                    wait_step(1, MATE_AT[at])

    start = jnp.full((1, 2 * TOK_DEV), masked_score, jnp.float32)
    zero = jnp.int32(0)
    first, second = unit_of(zero), unit_of(zero + 1)
    both_halves = kv.at[me]
    remote(both_halves, both_halves, 0, recv.at[1, STEPS], "mate").wait_recv()
    top = unit_score(first, scores_0)
    following = jnp.maximum(top, unit_score(second, scores_1))
    unit_rest(first, scores_0, start, top)

    def body(j, carry):
        old, top, before = carry
        u = 2 * j
        here, after = unit_of(u), unit_of(u + 1)
        handle(u)
        later = jnp.maximum(top, unit_score(here, scores_0))
        unit_rest(before, scores_1, old, top)
        old, top = top, later
        later = jnp.maximum(top, unit_score(after, scores_1))
        unit_rest(here, scores_0, old, top)
        return top, later, after

    old, top, last = lax.fori_loop(1, len(UNITS) // 2, body, (top, following, second))
    unit_rest(last, scores_1, old, top)
    both = jnp.concatenate([acc[h, 0:HD, :] / acc[h, HD : HD + 1, :] for h in range(2)], axis=0)
    ctx[...] = both.T.astype(jnp.bfloat16)

    def ctx_rows(at):
        return ctx.at[pl.ds(pl.multiple_of(lax.rem(at, 4) * ROWS, ROWS), ROWS), :]

    for g, (to, at) in enumerate((("right", x + 1), ("left", x + 3), ("across", x + 2))):
        go(ctx_rows(at), ctx_in.at[g], recv_c.at[g], to, 5)
    weights_pass(2)
    weights_here(0)
    weights_end(1)
    total = dot32(ctx_rows(x)[...], wo[...])
    for g in range(3):
        remote(ctx_in.at[g], ctx_in.at[g], 0, recv_c.at[g], "mate").wait_recv()
        total += dot32(ctx_in[g], wo_all[g])
    out_1[...] = total.astype(jnp.bfloat16)
    go(out_1, in_1, recv_y.at[0], "partner", 6)
    weights_start(4)
    weights_end(2)
    weights_here(1)
    weights_here(2)
    remote(out_1, in_1, 0, recv_y.at[0], "partner").wait_recv()
    total = out_1[...].astype(jnp.float32) + in_1[...].astype(jnp.float32)
    total += tokens[pl.ds(pl.multiple_of(x * ROWS, ROWS), ROWS), :].astype(jnp.float32)
    hidden[...] = total
    ffn_normed = normalised(total, gain_ffn[...]).T.astype(jnp.bfloat16)
    acts_here = []
    for g in range(4):
        gate_w, up_w, down_w = (
            (wi[0], wi[1], wf) if g == 3 else (wi_all[g, 0], wi_all[g, 1], wf_all.at[g])
        )
        gate = dot32(gate_w, ffn_normed)
        up = dot32(up_w, ffn_normed)
        activated = (jax.nn.gelu(gate, approximate=True) * up).T.astype(jnp.bfloat16)
        acts_here.append((activated, down_w))
        if g == 1:
            weights_pass(4)
    wide = D // 2
    for k in range(2):
        ffn = jnp.zeros((ROWS, wide), jnp.float32)
        for activated, down_w in acts_here:
            ffn += dot32(activated, down_w[:, k * wide : (k + 1) * wide])
        out_2[k] = ffn.astype(jnp.bfloat16)
        go(out_2.at[k], in_2.at[k], recv_y.at[1 + k], "partner", 7 if k == 0 else 20)
    weights_end(4)
    weights_start(3)
    weights_here(4)
    for k in range(2):
        remote(out_2.at[k], in_2.at[k], 0, recv_y.at[1 + k], "partner").wait_recv()
    final = jnp.concatenate(
        [out_2[k].astype(jnp.float32) + in_2[k].astype(jnp.float32) for k in range(2)], axis=1
    )
    final += hidden[...]
    rows_here = normalised(final, gain_final[...]).astype(jnp.bfloat16)
    enc[x] = rows_here

    def cross_pair(slot):
        weights = jnp.concatenate([wckv_all[slot, 0], wckv_all[slot, 1]], axis=1)
        return dot32(rows_here, weights).astype(jnp.bfloat16)

    for slot, to in ((2, "across"), (0, "left"), (1, "right")):
        both = cross_pair(slot)
        kvc_out[slot, 0] = both[:, : 2 * HD]
        kvc_out[slot, 1] = both[:, 2 * HD :]
        go(kvc_out.at[slot], kvc_in.at[x], recv_k.at[x], to, 19)
    both = cross_pair(3)
    kvc_in[x, 0] = both[:, : 2 * HD]
    kvc_in[x, 1] = both[:, 2 * HD :]

    def beside(dx):
        return lax.rem(x + dx + 4, 4)

    for dx in (-1, 1, 2):
        ref = kvc_in.at[beside(dx)]
        remote(ref, ref, 0, recv_k.at[beside(dx)], "mate").wait_recv()

    def rows_of(at, half):
        if half is None:
            return enc.at[at]
        return enc.at[at, pl.ds(half * 64, 64), :]

    def send_share(at, half, to):
        go(rows_of(at, half), rows_of(at, half), recv_e.at[at, half or 0], to, 8)

    def wait_share(at, half):
        ref = rows_of(at, half)
        remote(ref, ref, 0, recv_e.at[at, half or 0], "mate").wait_recv()

    weights_pass(3)
    cross_keys = jnp.concatenate([kvc_in[k, 0] for k in range(4)], axis=0)
    cross_rows = jnp.concatenate([kvc_in[k, 1] for k in range(4)], axis=0)
    cross_values[...] = cross_rows.astype(jnp.float32).T.astype(jnp.bfloat16)
    acc[...] = jnp.zeros_like(acc)
    cross_top = score(cross_keys, key_bias(lens[me], 0, TOK_DEV), cross_spread, scores_0)
    rest(lambda h: cross_values[pl.ds(h * HD, HD), :], scores_0, start, cross_top)
    o_all[...] = jnp.concatenate([acc[h, 0:HD, :] / acc[h, HD : HD + 1, :] for h in range(2)], axis=0)
    s_all[...] = jnp.concatenate(
        [
            cross_top[:, h * TOK_DEV : (h + 1) * TOK_DEV] + jnp.log2(acc[h, HD : HD + 1, :])
            for h in range(2)
        ]
        + [jnp.zeros((6, TOK_DEV), jnp.float32)],
        axis=0,
    )

    def joined(first, first_lse, second, second_lse):
        outs, lses = [], []
        for h in range(2):
            one, two = first_lse[h : h + 1], second_lse[h : h + 1]
            top = jnp.maximum(one, two)
            one, two = jnp.exp2(one - top), jnp.exp2(two - top)
            both = one + two
            dims = slice(h * HD, (h + 1) * HD)
            outs.append(first[dims] * (one / both) + second[dims] * (two / both))
            lses.append(top + jnp.log2(both))
        return jnp.concatenate(outs, axis=0), lses

    def lanes(at, size):
        return pl.ds(pl.multiple_of(at * size, size), size)

    def wait_for(ref, arrival):
        remote(ref, ref, 0, arrival, "mate").wait_recv()

    half, quarter = TOK_DEV // 2, TOK_DEV // 4
    go(o_all.at[:, lanes(1 - core, half)], o_mate, recv_m.at[0], "mate", 9)
    go(s_all.at[:, lanes(1 - core, half)], s_mate, recv_m.at[1], "mate", 10)
    for to in ("right", "left"):
        send_share(x, None, to)
    wait_for(o_mate, recv_m.at[0])
    wait_for(s_mate, recv_m.at[1])
    o, lse = joined(
        o_all[:, lanes(core, half)], s_all[:, lanes(core, half)], o_mate[...], s_mate[...]
    )
    o_half[...] = o.astype(jnp.bfloat16)
    s_half[...] = jnp.concatenate(lse + [jnp.zeros((6, half), jnp.float32)], axis=0)
    go(o_half.at[:, lanes(1 - y, quarter)], o_side, recv_m.at[2], "side", 11)
    go(s_half.at[:, lanes(1 - y, quarter)], s_side, recv_m.at[3], "side", 12)
    wait_for(o_side, recv_m.at[2])
    wait_for(s_side, recv_m.at[3])
    o, lse = joined(
        o_half[:, lanes(y, quarter)].astype(jnp.float32),
        s_half[:, lanes(y, quarter)],
        o_side[...].astype(jnp.float32),
        s_side[...],
    )
    o_rows[...] = o.T.astype(jnp.bfloat16)
    s_rows[...] = jnp.concatenate([jnp.broadcast_to(part, (HD, quarter)) for part in lse], axis=0).T
    few = quarter // NZ

    def few_rows(ref, at):
        return ref.at[pl.ds(pl.multiple_of(at * few, few), few), :]

    for dz in (4, 3, 5, 2, 6, 1, 7):
        at = lax.rem(z + dz, NZ)
        go(few_rows(o_rows, at), o_line.at[z], recv_l.at[0], line_place[dz], 13)
        go(few_rows(s_rows, at), s_line.at[z], recv_l.at[1], line_place[dz], 14)
    for dx, half, to in ((-1, 0, "right"), (1, 1, "left")):
        wait_share(beside(dx), None)
        send_share(beside(dx), half, to)
    weights_end(3)
    o_line[z] = few_rows(o_rows, z)[...]
    s_line[z] = few_rows(s_rows, z)[...]
    wait_for(o_line.at[pl.ds(0, NZ - 1)], recv_l.at[0])
    wait_for(s_line.at[pl.ds(0, NZ - 1)], recv_l.at[1])
    lines = s_line[...]
    factors = jnp.exp2(lines - jnp.max(lines, axis=0, keepdims=True))
    c_all[3] = (
        jnp.sum(o_line[...].astype(jnp.float32) * factors, axis=0) / jnp.sum(factors, axis=0)
    ).astype(jnp.bfloat16)
    for g, to in enumerate(("right", "left", "across")):
        go(c_all.at[3], c_all.at[g], recv_h.at[g], to, 15)
    weights_here(3)
    for g in range(3):
        wait_for(c_all.at[g], recv_h.at[g])
    total = jnp.zeros((few, D), jnp.float32)
    for k in range(4):
        away = lax.rem(k - x + 4, 4)
        g = jnp.where(away == 0, 3, jnp.where(away == 3, 0, away))
        total += dot32(c_all[g], wco_all[g])
    sum_out[...] = total.astype(jnp.bfloat16)
    go(sum_out, sum_in, recv_h.at[3], "partner", 16)

    def place_of(z_at, dy, dc):
        y_at = y if dy == 0 else 1 - y
        c_at = core if dc == 0 else 1 - core
        return c_at * 16 + y_at * NZ + z_at

    mine = place_of(z, 0, 0)
    target_rows = targets[pl.ds(pl.multiple_of(mine * few, few), few), :].astype(jnp.float32)
    slots = z * few + lax.broadcasted_iota(jnp.int32, (few, D), 0)
    wait_for(sum_in, recv_h.at[3])
    total = sum_out[...].astype(jnp.float32) + sum_in[...].astype(jnp.float32)
    live = slots < target_lens[core * 2 + y]
    dec[mine] = (target_rows + jnp.where(live, total, 0.0)).astype(jnp.bfloat16)

    def hand(at, to):
        go(dec.at[at], dec.at[at], recv_d.at[16 if to == "mate" else at - core * 16], to, 17)

    hand(mine, "side")
    hand(mine, "mate")
    for dz in (1, 7, 2, 6, 3, 5, 4):
        hand(mine, line_place[dz])
    for dz in (1, 7, 2, 6, 3, 5, 4):
        at = place_of(lax.rem(z + dz, NZ), 0, 0)
        wait_for(dec.at[at], recv_d.at[at - core * 16])
        hand(at, "side")
        hand(at, "mate")
    for dz in (0, 1, 7, 2, 6, 3, 5, 4):
        at = place_of(lax.rem(z + dz, NZ), 1, 0)
        wait_for(dec.at[at], recv_d.at[at - core * 16])
        hand(at, "mate")
    wait_for(dec.at[pl.ds(pl.multiple_of((1 - core) * 16, 16), 16)], recv_d.at[16])
    for half in (0, 1):
        wait_share(beside(2), half)
    sent = (
        wo_all,
        wi_all,
        wf_all,
        wco_all.at[pl.ds(0, 3)],
        kv.at[pl.ds(0, SLOTS - 1)],
        ctx_in,
        out_1,
        out_2.at[0],
        enc.at[pl.ds(0, 3)],
        o_mate,
        s_mate,
        o_side,
        s_side,
        o_line.at[pl.ds(0, NZ - 1)],
        s_line.at[pl.ds(0, NZ - 1)],
        c_all.at[pl.ds(0, 3)],
        sum_out,
        dec.at[pl.ds(0, SLOTS - 1)],
        wckv_all.at[pl.ds(0, 3)],
        kvc_out,
        out_2.at[1],
    )
    for group, ref in enumerate(sent):
        remote(ref, ref, group, recv_y.at[0], "mate").wait_send()


def leave_kernel(encoded, decoded, encoded_out, decoded_out, sems):
    moves = (
        pltpu.make_async_copy(encoded, encoded_out, sems.at[0]),
        pltpu.make_async_copy(decoded, decoded_out, sems.at[1]),
    )
    for move in moves:
        move.start()
    for move in moves:
        move.wait()


def layer(lens, tokens, gains, wqkv, wo, wi, wf, targets, wcq, wckv, wco, target_lens):
    hbm = pl.BlockSpec(memory_space=pl.ANY)
    vmem = pl.BlockSpec(memory_space=pltpu.VMEM)
    smem = pl.BlockSpec(memory_space=pltpu.SMEM)
    b16, f32 = jnp.bfloat16, jnp.float32
    gain_attn, gain_ffn, gain_final, gain_cross = (g.reshape(1, D) for g in gains)
    scratch = [
        (tokens.shape, b16),
        ((1, D), f32),
        (wqkv.shape, b16),
        ((1, D), f32),
        ((1, D), f32),
        ((1, D), f32),
        ((SLOTS, 2, 2 * UNIT, 2 * HD), b16),
        ((256, 2 * TOK_DEV), b16),
        ((2, HD + 16, TOK_DEV), f32),
        ((TOK_DEV, 2 * TOK_DEV), f32),
        ((TOK_DEV, 2 * TOK_DEV), f32),
        (wo.shape, b16),
        (wi.shape, b16),
        (wf.shape, b16),
        (targets.shape, b16),
        (wcq.shape, b16),
        ((4, *wckv.shape), b16),
        ((3, *wo.shape), b16),
        ((3, *wi.shape), b16),
        ((3, *wf.shape), b16),
        ((TOK_DEV, 2 * HD), b16),
        ((3, ROWS, 2 * HD), b16),
        ((ROWS, D), f32),
        ((ROWS, D), b16),
        ((ROWS, D), b16),
        ((2, ROWS, D // 2), b16),
        ((2, ROWS, D // 2), b16),
        ((3, 2, ROWS, 2 * HD), b16),
        ((4, 2, ROWS, 2 * HD), b16),
        ((256, 2 * TOK_DEV), b16),
        ((2 * HD, TOK_DEV), b16),
        ((4, *wco.shape), b16),
        ((2 * HD, TOK_DEV), f32),
        ((8, TOK_DEV), f32),
        ((2 * HD, TOK_DEV // 2), f32),
        ((8, TOK_DEV // 2), f32),
        ((2 * HD, TOK_DEV // 2), b16),
        ((8, TOK_DEV // 2), f32),
        ((2 * HD, TOK_DEV // 4), b16),
        ((8, TOK_DEV // 4), f32),
        ((TOK_DEV // 4, 2 * HD), b16),
        ((TOK_DEV // 4, 2 * HD), f32),
        ((NZ, 16, 2 * HD), b16),
        ((NZ, 16, 2 * HD), f32),
        ((4, 16, 2 * HD), b16),
        ((16, D), b16),
        ((16, D), b16),
    ]
    sems = [(16,), (21,), (2, STEPS + 1), (5, 5), (3,), (3,), (4, 2), (4,), (2,), (4,), (17,), (4,)]
    encoded, decoded = pl.pallas_call(
        layer_kernel,
        out_shape=(
            pltpu.VMEM((4, ROWS, D), b16),
            pltpu.VMEM((SLOTS, 16, D), b16),
        ),
        in_specs=[smem] + [hbm] * 13 + [smem],
        out_specs=(vmem, vmem),
        scratch_shapes=[pltpu.VMEM(*s) for s in scratch] + [pltpu.SemaphoreType.DMA(s) for s in sems],
        compiler_params=pltpu.CompilerParams(
            collective_id=0, has_side_effects=True, vmem_limit_bytes=54 << 20
        ),
        name="layer",
    )(lens, tokens, gain_attn, wqkv, gain_ffn, gain_final, gain_cross, wo, wi, wf, targets, wcq, wckv, wco, target_lens)
    encoded, decoded = pl.pallas_call(
        leave_kernel,
        out_shape=(
            jax.ShapeDtypeStruct(encoded.shape, b16),
            jax.ShapeDtypeStruct(decoded.shape, b16),
        ),
        in_specs=[vmem, vmem],
        out_specs=(hbm, hbm),
        scratch_shapes=[pltpu.SemaphoreType.DMA((2,))],
        name="leave",
    )(
        pltpu.with_memory_space_constraint(encoded, pltpu.VMEM),
        pltpu.with_memory_space_constraint(decoded, pltpu.VMEM),
    )
    return encoded.reshape(TOK_DEV, D), decoded.reshape(targets.shape)


def local(
    tokens,
    norm_attn,
    self_qkv,
    self_out,
    norm_ffn,
    ffn_in,
    ffn_out,
    norm_final,
    pad_lengths,
    targets,
    target_lengths,
    norm_cross,
    cross_query,
    cross_kv,
    cross_out,
):
    return layer(
        pad_lengths,
        tokens,
        (norm_attn, norm_ffn, norm_final, norm_cross),
        self_qkv,
        self_out,
        jnp.swapaxes(ffn_in, 1, 2),
        ffn_out,
        targets,
        cross_query,
        cross_kv,
        cross_out,
        target_lengths,
    )


def solution(mesh):
    in_specs = (
        P("seq", None),
        P(),
        P(None, None, "head"),
        P("head", None),
        P(),
        P(None, None, "head"),
        P("head", None),
        P(),
        P(),
        P(),
        P(),
        P(),
        P(None, "head"),
        P(None, None, "head"),
        P("head", None),
    )
    out_specs = (P("seq", None), P())
    return jax.shard_map(local, mesh=mesh, in_specs=in_specs, out_specs=out_specs, check_vma=False)
```

```python
import functools
import math

import jax
import jax.numpy as jnp
from jax import lax
from jax.experimental import pallas as pl
from jax.experimental.pallas import tpu as pltpu
from jax.sharding import Mesh
from jax.sharding import PartitionSpec as P

D = 1024
HD = 64
TOK_DEV = 512


epsilon = 1e-06
masked_score = -1e30


NZ = 8
SLOTS = 32
UP = (("O", 0, 0), ("O", 0, 1), ("O", 1, 0), ("O", 1, 1), ("O", 2, 0), ("O", 2, 1), ("P", 2, 0), ("O", 3, 0), ("P", 2, 1), ("P", 3, 0))
DOWN = (("O", 0, 1), ("O", 0, 0), ("O", -1, 1), ("O", -1, 0), ("O", -2, 1), ("O", -2, 0), ("P", -2, 1), ("O", -3, 1), ("P", -3, 1), ("P", -2, 0))
SIDE = (("O", 0, 0), ("O", 0, 1), ("O", 1, 0), ("O", -1, 1), ("O", 2, 0), ("O", -2, 1), ("O", 2, 1), ("O", -2, 0), ("O", 1, 1), ("O", -1, 0))
STEPS = 10
FF_DEV = 352
ROWS = 128
UNIT = 256


def link_plan():
    arrive = {("O", 0, 0): -1, ("O", 0, 1): -1}
    arrivals = []
    for s in range(STEPS):
        new = [(UP[s][0], UP[s][1] + 1, UP[s][2]), (DOWN[s][0], DOWN[s][1] - 1, DOWN[s][2])]
        new.append(("P", SIDE[s][1], SIDE[s][2]))
        arrive.update({item: s for item in new})
        arrivals.append(new)
    waiting = {"up": list(UP), "down": list(DOWN), "side": list(SIDE)}
    sent = {name: 0 for name in waiting}
    sends = []
    for s in range(-1, STEPS):
        now = []
        for name, queue in waiting.items():
            while queue and sent[name] <= s + 2 and arrive[queue[0]] <= s:
                now.append((name, queue.pop(0)))
                sent[name] += 1
        sends.append(now)
    return arrivals, sends


ARRIVALS, SENDS = link_plan()
UNITS = (("O", 0, 0), ("O", 0, 1), *(item for step in ARRIVALS for item in step))
MATE_AT = {(2 + 3 * s) // 2 * 2: s for s in range(STEPS)}
STEP_AT = {2: 0, 4: 1, 6: 2, 8: 3, 12: 4, 14: 5, 18: 6, 20: 7, 24: 8, 26: 9}
WEIGHT_STEP_AT = {8: (("pass", 0),), 14: (("start", 2),), 18: (("pass", 1), ("end", 0))}
UNIT_CODES = tuple((4 - d) * 4 + (line == "P") * 2 + half for line, d, half in UNITS)
CODE_WORDS = tuple(
    sum(code << (8 * k) for k, code in enumerate(UNIT_CODES[first : first + 3]))
    for first in range(0, len(UNITS), 3)
)


def key_bias(length, first, rows):
    row = first + lax.broadcasted_iota(jnp.int32, (rows, 128), 0)
    lane = lax.broadcasted_iota(jnp.int32, (rows, 128), 1)
    return jnp.where((lane == 0) & (row >= length), masked_score, 0.0).astype(jnp.bfloat16)


def spread_queries(q_t):
    rows = lax.broadcasted_iota(jnp.int32, (256, 2 * q_t.shape[1]), 0)
    cols = lax.broadcasted_iota(jnp.int32, (256, 2 * q_t.shape[1]), 1)
    half = q_t.shape[1]
    two = jnp.concatenate([q_t, q_t], axis=1)
    full = jnp.concatenate([two, jnp.zeros_like(two)], axis=0)
    keep = ((rows < HD) & (cols < half)) | ((rows >= HD) & (rows < 2 * HD) & (cols >= half))
    return jnp.where(keep, full, jnp.where(rows == 2 * HD, 1.0, 0.0)).astype(jnp.bfloat16)


def normalised(x, gain):
    return x * lax.rsqrt(jnp.mean(x * x, axis=1, keepdims=True) + epsilon) * gain


def dot32(a, b):
    return jnp.dot(a, b, preferred_element_type=jnp.float32)


def layer_kernel(
    lens,
    tokens_hbm,
    gain_attn_hbm,
    wqkv_hbm,
    gain_ffn_hbm,
    gain_final_hbm,
    gain_cross_hbm,
    wo_hbm,
    wi_hbm,
    wf_hbm,
    targets_hbm,
    wcq_hbm,
    wckv_hbm,
    wco_hbm,
    target_lens,
    enc,
    dec,
    tokens,
    gain_attn,
    wqkv,
    gain_ffn,
    gain_final,
    gain_cross,
    kv,
    spread,
    acc,
    scores_0,
    scores_1,
    wo,
    wi,
    wf,
    targets,
    wcq,
    wckv_all,
    wo_all,
    wi_all,
    wf_all,
    ctx,
    ctx_in,
    hidden,
    out_1,
    in_1,
    out_2,
    in_2,
    kvc_out,
    kvc_in,
    cross_spread,
    cross_values,
    wco_all,
    o_all,
    s_all,
    o_mate,
    s_mate,
    o_half,
    s_half,
    o_side,
    s_side,
    o_rows,
    s_rows,
    o_line,
    s_line,
    c_all,
    sum_out,
    sum_in,
    local_sem,
    send,
    recv,
    recv_w,
    recv_c,
    recv_y,
    recv_e,
    recv_m,
    recv_l,
    recv_h,
    recv_d,
    recv_k,
):
    me = lax.axis_index("seq")
    core = lax.rem(me, 2)
    y = lax.rem(me // 2, 2)
    z = me // 4
    head = lax.axis_index("head")
    x = lax.rem(head, 4)
    yh = head // 4

    def index(dz, dy, dc):
        z_at = lax.rem(z + dz + NZ, NZ)
        y_at = y if dy == 0 else 1 - y
        c_at = core if dc == 0 else 1 - core
        return z_at * 4 + y_at * 2 + c_at

    places = {
        "up": {"seq": index(1, 0, 0)},
        "down": {"seq": index(-1, 0, 0)},
        "side": {"seq": index(0, 1, 0)},
        "mate": {"seq": index(0, 0, 1)},
        "diagonal": {"seq": index(0, 1, 1)},
        "right": {"head": yh * 4 + lax.rem(x + 1, 4)},
        "left": {"head": yh * 4 + lax.rem(x + 3, 4)},
        "across": {"head": yh * 4 + lax.rem(x + 2, 4)},
        "partner": {"head": (1 - yh) * 4 + x},
    }
    for dz in range(2, NZ - 1):
        places[dz] = {"seq": index(dz, 0, 0)}
    line_place = {1: "up", NZ - 1: "down", **{dz: dz for dz in range(2, NZ - 1)}}
    barrier = pltpu.get_barrier_semaphore()
    for place in places.values():
        pl.semaphore_signal(barrier, inc=1, device_id=place, device_id_type=pl.DeviceIdType.MESH)

    pairs = {
        "tokens": (tokens_hbm, tokens),
        "wqkv": (wqkv_hbm, wqkv),
        "gain_attn": (gain_attn_hbm, gain_attn),
        "wo": (wo_hbm, wo),
        "wi": (wi_hbm, wi),
        "wf": (wf_hbm, wf),
        "wco": (wco_hbm, wco_all.at[3]),
        "targets": (targets_hbm, targets),
        "wcq": (wcq_hbm, wcq),
        "gain_cross": (gain_cross_hbm, gain_cross),
        "gain_ffn": (gain_ffn_hbm, gain_ffn),
        "gain_final": (gain_final_hbm, gain_final),
        "wckv": (wckv_hbm, wckv_all.at[3]),
    }
    loads = {
        name: pltpu.make_async_copy(source, target, local_sem.at[k])
        for k, (name, (source, target)) in enumerate(pairs.items())
    }
    first_loads = ("tokens", "gain_attn", "wqkv")
    for name in first_loads:
        loads[name].start()
    for name in first_loads:
        loads[name].wait()
    for name, load in loads.items():
        if name not in first_loads:
            load.start()
    normed = normalised(tokens[...].astype(jnp.float32), gain_attn[...]).astype(jnp.bfloat16)
    own_keys = dot32(normed, wqkv[1]).astype(jnp.bfloat16)
    own_values = dot32(normed, wqkv[2]).T.astype(jnp.bfloat16)
    for half in range(2):
        kv[me, half, 0:UNIT, :] = own_keys[half * UNIT : (half + 1) * UNIT, :]
        for k in range(2):
            first = half * UNIT + k * 128
            kv[me, half, pl.ds(UNIT + k * 128, 128), :] = own_values[:, first : first + 128]
    pl.semaphore_wait(barrier, len(places))

    def remote(source, target, number, arrival, place):
        return pltpu.make_async_remote_copy(
            src_ref=source,
            dst_ref=target,
            send_sem=send.at[number],
            recv_sem=arrival,
            device_id=places[place],
            device_id_type=pl.DeviceIdType.MESH,
        )

    def go(source, target, arrival, place, group):
        remote(source, target, group, arrival, place).start()

    def wait_step(mate_side, s):
        ref = kv.at[pl.ds(0, 3), 0]
        remote(ref, ref, 0, recv.at[mate_side, s], "mate").wait_recv()

    def push(half, slot, place, s):
        ref = kv.at[slot, half]
        go(ref, ref, recv.at[int(place == "mate"), s], place, 4)

    def slot_of(line, d):
        return index(-d, 0 if line == "O" else 1, 0)

    link_items = {"up": UP, "down": DOWN, "side": SIDE}
    for name, item in SENDS[0]:
        push(item[2], me, name, link_items[name].index(item))
    for half in range(2):
        push(half, me, "mate", STEPS)

    def piece(item, slot, which, c):
        own, gathered = ((wo, wo_all), (wi, wi_all), (wf, wf_all), (wco_all.at[3], wco_all), (wckv_all.at[3], wckv_all))[item]
        ref = own if slot is None else gathered.at[slot]
        if item in (0, 3):
            first, size = ((0, 64), (0, 32), (32, 32))[which]
            return ref.at[pl.ds(pl.multiple_of(c * 64 + first, 32), size), :]
        if item in (1, 4):
            rows = ref.shape[1] // 2
            first, size = ((0, 2 * rows), (0, rows), (rows, rows))[which]
            return ref.at[c, pl.ds(first, size), :]
        first, size = ((0, 176), (0, 96), (96, 80))[which]
        return ref.at[pl.ds(pl.multiple_of(c * 176 + first, 16), size), :]

    def wait_piece(item, slot, which, k, c):
        ref = piece(item, slot, which, c)
        remote(ref, ref, 0, recv_w.at[item, k], "mate").wait_recv()

    def send_piece(item, slot, slot_there, which, k, to):
        source, target = piece(item, slot, which, core), piece(item, slot_there, which, core)
        go(source, target, recv_w.at[item, k], to, 18 if item == 4 else item)

    def weights_start(item):
        loads[("wo", "wi", "wf", "wco", "wckv")[item]].wait()
        for slot, to in ((0, "right"), (1, "left")):
            send_piece(item, None, slot, 0, slot, to)

    def weights_pass(item):
        for slot, half, onward in ((0, 1, "right"), (1, 2, "left")):
            wait_piece(item, slot, 0, slot, core)
            send_piece(item, slot, 2, half, 1 + half, onward)
            send_piece(item, slot, slot, 0, 4, "mate")

    def weights_end(item):
        for half in (1, 2):
            wait_piece(item, 2, half, 1 + half, core)
            send_piece(item, 2, 2, half, 4, "mate")

    def weights_here(item):
        c = 1 - core
        ref = (
            lambda: wo_all.at[:, pl.ds(pl.multiple_of(c * 64, 64), 64), :],
            lambda: wi_all.at[:, c],
            lambda: wf_all.at[:, pl.ds(pl.multiple_of(c * 176, 16), 176), :],
            lambda: wco_all.at[pl.ds(0, 3), pl.ds(pl.multiple_of(c * 64, 64), 64), :],
            lambda: wckv_all.at[pl.ds(0, 3), c],
        )[item]()
        remote(ref, ref, 0, recv_w.at[item, 4], "mate").wait_recv()

    for item in range(2):
        weights_start(item)
    q_t = dot32(normed, wqkv[0]).T

    spread[...] = spread_queries(q_t * (HD ** (-0.5) * math.log2(math.e)))
    acc[...] = jnp.zeros_like(acc)
    for name in ("targets", "wcq", "gain_cross", "gain_ffn", "gain_final"):
        loads[name].wait()
    cross_normed = normalised(targets[...].astype(jnp.float32), gain_cross[...]).astype(jnp.bfloat16)
    cross_spread[...] = spread_queries(
        dot32(cross_normed, wcq[...]).T * (HD ** (-0.5) * math.log2(math.e))
    )

    def step(s):
        wait_step(0, s)
        for line, d, half in ARRIVALS[s]:
            push(half, slot_of(line, d), "mate", s)
        for name, item in SENDS[s + 1]:
            line, d, half = item
            push(half, slot_of(line, d), name, link_items[name].index(item))

    def unit_of(u):
        third = u // 3
        word = jnp.int32(CODE_WORDS[0])
        for k in range(1, len(CODE_WORDS)):
            word = jnp.where(third == k, CODE_WORDS[k], word)
        code = lax.rem(lax.shift_right_logical(word, 8 * (u - 3 * third)), 256)
        half = lax.rem(code, 2)
        chip = lax.rem(z + code // 4 + 4, NZ) * 4 + lax.rem(y + code // 2, 2) * 2
        return chip + core, chip + 1 - core, half

    def score(block, bias, queries, into):
        s = dot32(jnp.concatenate([block, bias], axis=1), queries[...])
        into[...] = s
        return jnp.max(s, axis=0, keepdims=True)

    def unit_score(unit, into):
        here, there, half = unit
        block = jnp.concatenate([kv[here, half, 0:UNIT, :], kv[there, half, 0:UNIT, :]], axis=0)
        bias = jnp.concatenate(
            [key_bias(lens[slot], half * UNIT, UNIT) for slot in (here, there)], axis=0
        )
        return score(block, bias, spread, into)

    def rest(rows_of_head, held, old, top):
        p = jnp.exp2(held[...] - top).astype(jnp.bfloat16)
        shrink = jnp.exp2(old - top)
        ones = jnp.ones((16, TOK_DEV), jnp.bfloat16)
        for h in range(2):
            cols = slice(h * TOK_DEV, (h + 1) * TOK_DEV)
            lhs = jnp.concatenate([rows_of_head(h), ones], axis=0)
            acc[h] = acc[h] * shrink[:, cols] + dot32(lhs, p[:, cols])

    def unit_rest(unit, held, old, top):
        here, there, half = unit

        def rows_of_head(h):
            return jnp.concatenate(
                [
                    kv[slot, half, pl.ds(UNIT + k * 128 + h * HD, HD), :]
                    for slot in (here, there)
                    for k in range(2)
                ],
                axis=1,
            )

        rest(rows_of_head, held, old, top)

    acts = {"start": weights_start, "pass": weights_pass, "end": weights_end}

    def handle(u):
        for at in sorted({*STEP_AT, *MATE_AT, *WEIGHT_STEP_AT}):

            @pl.when(u == at)
            def _():
                if at in STEP_AT:
                    step(STEP_AT[at])
                for what, item in WEIGHT_STEP_AT.get(at, ()):
                    acts[what](item)
                if at in MATE_AT:
                    wait_step(1, MATE_AT[at])

    start = jnp.full((1, 2 * TOK_DEV), masked_score, jnp.float32)
    zero = jnp.int32(0)
    first, second = unit_of(zero), unit_of(zero + 1)
    both_halves = kv.at[me]
    remote(both_halves, both_halves, 0, recv.at[1, STEPS], "mate").wait_recv()
    top = unit_score(first, scores_0)
    following = jnp.maximum(top, unit_score(second, scores_1))
    unit_rest(first, scores_0, start, top)

    def body(j, carry):
        old, top, before = carry
        u = 2 * j
        here, after = unit_of(u), unit_of(u + 1)
        handle(u)
        later = jnp.maximum(top, unit_score(here, scores_0))
        unit_rest(before, scores_1, old, top)
        old, top = top, later
        later = jnp.maximum(top, unit_score(after, scores_1))
        unit_rest(here, scores_0, old, top)
        return top, later, after

    old, top, last = lax.fori_loop(1, len(UNITS) // 2, body, (top, following, second))
    unit_rest(last, scores_1, old, top)
    both = jnp.concatenate([acc[h, 0:HD, :] / acc[h, HD : HD + 1, :] for h in range(2)], axis=0)
    ctx[...] = both.T.astype(jnp.bfloat16)

    def ctx_rows(at):
        return ctx.at[pl.ds(pl.multiple_of(lax.rem(at, 4) * ROWS, ROWS), ROWS), :]

    for g, (to, at) in enumerate((("right", x + 1), ("left", x + 3), ("across", x + 2))):
        go(ctx_rows(at), ctx_in.at[g], recv_c.at[g], to, 5)
    weights_pass(2)
    weights_here(0)
    weights_end(1)
    total = dot32(ctx_rows(x)[...], wo[...])
    for g in range(3):
        remote(ctx_in.at[g], ctx_in.at[g], 0, recv_c.at[g], "mate").wait_recv()
        total += dot32(ctx_in[g], wo_all[g])
    out_1[...] = total.astype(jnp.bfloat16)
    go(out_1, in_1, recv_y.at[0], "partner", 6)
    weights_start(4)
    weights_end(2)
    weights_here(1)
    weights_here(2)
    remote(out_1, in_1, 0, recv_y.at[0], "partner").wait_recv()
    total = out_1[...].astype(jnp.float32) + in_1[...].astype(jnp.float32)
    total += tokens[pl.ds(pl.multiple_of(x * ROWS, ROWS), ROWS), :].astype(jnp.float32)
    hidden[...] = total
    ffn_normed = normalised(total, gain_ffn[...]).T.astype(jnp.bfloat16)
    acts_here = []
    for g in range(4):
        gate_w, up_w, down_w = (
            (wi[0], wi[1], wf) if g == 3 else (wi_all[g, 0], wi_all[g, 1], wf_all.at[g])
        )
        gate = dot32(gate_w, ffn_normed)
        up = dot32(up_w, ffn_normed)
        activated = (jax.nn.gelu(gate, approximate=True) * up).T.astype(jnp.bfloat16)
        acts_here.append((activated, down_w))
        if g == 1:
            weights_pass(4)
    wide = D // 2
    for k in range(2):
        ffn = jnp.zeros((ROWS, wide), jnp.float32)
        for activated, down_w in acts_here:
            ffn += dot32(activated, down_w[:, k * wide : (k + 1) * wide])
        out_2[k] = ffn.astype(jnp.bfloat16)
        go(out_2.at[k], in_2.at[k], recv_y.at[1 + k], "partner", 7 if k == 0 else 20)
    weights_end(4)
    weights_start(3)
    weights_here(4)
    for k in range(2):
        remote(out_2.at[k], in_2.at[k], 0, recv_y.at[1 + k], "partner").wait_recv()
    final = jnp.concatenate(
        [out_2[k].astype(jnp.float32) + in_2[k].astype(jnp.float32) for k in range(2)], axis=1
    )
    final += hidden[...]
    rows_here = normalised(final, gain_final[...]).astype(jnp.bfloat16)
    enc[x] = rows_here

    def cross_pair(slot):
        weights = jnp.concatenate([wckv_all[slot, 0], wckv_all[slot, 1]], axis=1)
        return dot32(rows_here, weights).astype(jnp.bfloat16)

    for slot, to in ((2, "across"), (0, "left"), (1, "right")):
        both = cross_pair(slot)
        kvc_out[slot, 0] = both[:, : 2 * HD]
        kvc_out[slot, 1] = both[:, 2 * HD :]
        go(kvc_out.at[slot], kvc_in.at[x], recv_k.at[x], to, 19)
    both = cross_pair(3)
    kvc_in[x, 0] = both[:, : 2 * HD]
    kvc_in[x, 1] = both[:, 2 * HD :]

    def beside(dx):
        return lax.rem(x + dx + 4, 4)

    for dx in (-1, 1, 2):
        ref = kvc_in.at[beside(dx)]
        remote(ref, ref, 0, recv_k.at[beside(dx)], "mate").wait_recv()

    def rows_of(at, half):
        if half is None:
            return enc.at[at]
        return enc.at[at, pl.ds(half * 64, 64), :]

    def send_share(at, half, to):
        go(rows_of(at, half), rows_of(at, half), recv_e.at[at, half or 0], to, 8)

    def wait_share(at, half):
        ref = rows_of(at, half)
        remote(ref, ref, 0, recv_e.at[at, half or 0], "mate").wait_recv()

    weights_pass(3)
    cross_keys = jnp.concatenate([kvc_in[k, 0] for k in range(4)], axis=0)
    cross_rows = jnp.concatenate([kvc_in[k, 1] for k in range(4)], axis=0)
    cross_values[...] = cross_rows.astype(jnp.float32).T.astype(jnp.bfloat16)
    acc[...] = jnp.zeros_like(acc)
    cross_top = score(cross_keys, key_bias(lens[me], 0, TOK_DEV), cross_spread, scores_0)
    rest(lambda h: cross_values[pl.ds(h * HD, HD), :], scores_0, start, cross_top)
    o_all[...] = jnp.concatenate([acc[h, 0:HD, :] / acc[h, HD : HD + 1, :] for h in range(2)], axis=0)
    s_all[...] = jnp.concatenate(
        [
            cross_top[:, h * TOK_DEV : (h + 1) * TOK_DEV] + jnp.log2(acc[h, HD : HD + 1, :])
            for h in range(2)
        ]
        + [jnp.zeros((6, TOK_DEV), jnp.float32)],
        axis=0,
    )

    def joined(first, first_lse, second, second_lse):
        outs, lses = [], []
        for h in range(2):
            one, two = first_lse[h : h + 1], second_lse[h : h + 1]
            top = jnp.maximum(one, two)
            one, two = jnp.exp2(one - top), jnp.exp2(two - top)
            both = one + two
            dims = slice(h * HD, (h + 1) * HD)
            outs.append(first[dims] * (one / both) + second[dims] * (two / both))
            lses.append(top + jnp.log2(both))
        return jnp.concatenate(outs, axis=0), lses

    def lanes(at, size):
        return pl.ds(pl.multiple_of(at * size, size), size)

    def wait_for(ref, arrival):
        remote(ref, ref, 0, arrival, "mate").wait_recv()

    half, quarter = TOK_DEV // 2, TOK_DEV // 4
    go(o_all.at[:, lanes(1 - core, half)], o_mate, recv_m.at[0], "mate", 9)
    go(s_all.at[:, lanes(1 - core, half)], s_mate, recv_m.at[1], "mate", 10)
    for to in ("right", "left"):
        send_share(x, None, to)
    wait_for(o_mate, recv_m.at[0])
    wait_for(s_mate, recv_m.at[1])
    o, lse = joined(
        o_all[:, lanes(core, half)], s_all[:, lanes(core, half)], o_mate[...], s_mate[...]
    )
    o_half[...] = o.astype(jnp.bfloat16)
    s_half[...] = jnp.concatenate(lse + [jnp.zeros((6, half), jnp.float32)], axis=0)
    go(o_half.at[:, lanes(1 - y, quarter)], o_side, recv_m.at[2], "side", 11)
    go(s_half.at[:, lanes(1 - y, quarter)], s_side, recv_m.at[3], "side", 12)
    wait_for(o_side, recv_m.at[2])
    wait_for(s_side, recv_m.at[3])
    o, lse = joined(
        o_half[:, lanes(y, quarter)].astype(jnp.float32),
        s_half[:, lanes(y, quarter)],
        o_side[...].astype(jnp.float32),
        s_side[...],
    )
    o_rows[...] = o.T.astype(jnp.bfloat16)
    s_rows[...] = jnp.concatenate([jnp.broadcast_to(part, (HD, quarter)) for part in lse], axis=0).T
    few = quarter // NZ

    def few_rows(ref, at):
        return ref.at[pl.ds(pl.multiple_of(at * few, few), few), :]

    for dz in (4, 3, 5, 2, 6, 1, 7):
        at = lax.rem(z + dz, NZ)
        go(few_rows(o_rows, at), o_line.at[z], recv_l.at[0], line_place[dz], 13)
        go(few_rows(s_rows, at), s_line.at[z], recv_l.at[1], line_place[dz], 14)
    for dx, half, to in ((-1, 0, "right"), (1, 1, "left")):
        wait_share(beside(dx), None)
        send_share(beside(dx), half, to)
    weights_end(3)
    o_line[z] = few_rows(o_rows, z)[...]
    s_line[z] = few_rows(s_rows, z)[...]
    wait_for(o_line.at[pl.ds(0, NZ - 1)], recv_l.at[0])
    wait_for(s_line.at[pl.ds(0, NZ - 1)], recv_l.at[1])
    lines = s_line[...]
    factors = jnp.exp2(lines - jnp.max(lines, axis=0, keepdims=True))
    c_all[3] = (
        jnp.sum(o_line[...].astype(jnp.float32) * factors, axis=0) / jnp.sum(factors, axis=0)
    ).astype(jnp.bfloat16)
    for g, to in enumerate(("right", "left", "across")):
        go(c_all.at[3], c_all.at[g], recv_h.at[g], to, 15)
    weights_here(3)
    for g in range(3):
        wait_for(c_all.at[g], recv_h.at[g])
    total = jnp.zeros((few, D), jnp.float32)
    for k in range(4):
        away = lax.rem(k - x + 4, 4)
        g = jnp.where(away == 0, 3, jnp.where(away == 3, 0, away))
        total += dot32(c_all[g], wco_all[g])
    sum_out[...] = total.astype(jnp.bfloat16)
    go(sum_out, sum_in, recv_h.at[3], "partner", 16)

    def place_of(z_at, dy, dc):
        y_at = y if dy == 0 else 1 - y
        c_at = core if dc == 0 else 1 - core
        return c_at * 16 + y_at * NZ + z_at

    mine = place_of(z, 0, 0)
    target_rows = targets[pl.ds(pl.multiple_of(mine * few, few), few), :].astype(jnp.float32)
    slots = z * few + lax.broadcasted_iota(jnp.int32, (few, D), 0)
    wait_for(sum_in, recv_h.at[3])
    total = sum_out[...].astype(jnp.float32) + sum_in[...].astype(jnp.float32)
    live = slots < target_lens[core * 2 + y]
    dec[mine] = (target_rows + jnp.where(live, total, 0.0)).astype(jnp.bfloat16)

    same_core = ("side", *line_place.values())

    def hand(at, to):
        go(dec.at[at], dec.at[at], recv_d.at[at - core * 16 if to in same_core else 16], to, 17)

    far = (3, 4, 5)
    hand(mine, "side")
    hand(mine, "mate")
    for dz in (1, 7, 2, 6, 3, 5, 4):
        hand(mine, line_place[dz])
    for dz in (1, 7, 2, 6, 3, 5, 4):
        at = place_of(lax.rem(z + dz, NZ), 0, 0)
        wait_for(dec.at[at], recv_d.at[at - core * 16])
        hand(at, "side")
        hand(at, "mate")
        if dz in far:
            hand(at, "diagonal")
    for dz in (0, 1, 7, 2, 6, 3, 5, 4):
        at = place_of(lax.rem(z + dz, NZ), 1, 0)
        wait_for(dec.at[at], recv_d.at[at - core * 16])
        if dz not in far:
            hand(at, "mate")
    wait_for(dec.at[pl.ds(pl.multiple_of((1 - core) * 16, 16), 16)], recv_d.at[16])
    for half in (0, 1):
        wait_share(beside(2), half)
    sent = (
        wo_all,
        wi_all,
        wf_all,
        wco_all.at[pl.ds(0, 3)],
        kv.at[pl.ds(0, SLOTS - 1)],
        ctx_in,
        out_1,
        out_2.at[0],
        enc.at[pl.ds(0, 3)],
        o_mate,
        s_mate,
        o_side,
        s_side,
        o_line.at[pl.ds(0, NZ - 1)],
        s_line.at[pl.ds(0, NZ - 1)],
        c_all.at[pl.ds(0, 3)],
        sum_out,
        dec.at[pl.ds(0, SLOTS - 1)],
        wckv_all.at[pl.ds(0, 3)],
        kvc_out,
        out_2.at[1],
    )
    for group, ref in enumerate(sent):
        remote(ref, ref, group, recv_y.at[0], "mate").wait_send()


def leave_kernel(encoded, decoded, encoded_out, decoded_out, sems):
    moves = (
        pltpu.make_async_copy(encoded, encoded_out, sems.at[0]),
        pltpu.make_async_copy(decoded, decoded_out, sems.at[1]),
    )
    for move in moves:
        move.start()
    for move in moves:
        move.wait()


def layer(lens, tokens, gains, wqkv, wo, wi, wf, targets, wcq, wckv, wco, target_lens):
    hbm = pl.BlockSpec(memory_space=pl.ANY)
    vmem = pl.BlockSpec(memory_space=pltpu.VMEM)
    smem = pl.BlockSpec(memory_space=pltpu.SMEM)
    b16, f32 = jnp.bfloat16, jnp.float32
    gain_attn, gain_ffn, gain_final, gain_cross = (g.reshape(1, D) for g in gains)
    scratch = [
        (tokens.shape, b16),
        ((1, D), f32),
        (wqkv.shape, b16),
        ((1, D), f32),
        ((1, D), f32),
        ((1, D), f32),
        ((SLOTS, 2, 2 * UNIT, 2 * HD), b16),
        ((256, 2 * TOK_DEV), b16),
        ((2, HD + 16, TOK_DEV), f32),
        ((TOK_DEV, 2 * TOK_DEV), f32),
        ((TOK_DEV, 2 * TOK_DEV), f32),
        (wo.shape, b16),
        (wi.shape, b16),
        (wf.shape, b16),
        (targets.shape, b16),
        (wcq.shape, b16),
        ((4, *wckv.shape), b16),
        ((3, *wo.shape), b16),
        ((3, *wi.shape), b16),
        ((3, *wf.shape), b16),
        ((TOK_DEV, 2 * HD), b16),
        ((3, ROWS, 2 * HD), b16),
        ((ROWS, D), f32),
        ((ROWS, D), b16),
        ((ROWS, D), b16),
        ((2, ROWS, D // 2), b16),
        ((2, ROWS, D // 2), b16),
        ((3, 2, ROWS, 2 * HD), b16),
        ((4, 2, ROWS, 2 * HD), b16),
        ((256, 2 * TOK_DEV), b16),
        ((2 * HD, TOK_DEV), b16),
        ((4, *wco.shape), b16),
        ((2 * HD, TOK_DEV), f32),
        ((8, TOK_DEV), f32),
        ((2 * HD, TOK_DEV // 2), f32),
        ((8, TOK_DEV // 2), f32),
        ((2 * HD, TOK_DEV // 2), b16),
        ((8, TOK_DEV // 2), f32),
        ((2 * HD, TOK_DEV // 4), b16),
        ((8, TOK_DEV // 4), f32),
        ((TOK_DEV // 4, 2 * HD), b16),
        ((TOK_DEV // 4, 2 * HD), f32),
        ((NZ, 16, 2 * HD), b16),
        ((NZ, 16, 2 * HD), f32),
        ((4, 16, 2 * HD), b16),
        ((16, D), b16),
        ((16, D), b16),
    ]
    sems = [(16,), (21,), (2, STEPS + 1), (5, 5), (3,), (3,), (4, 2), (4,), (2,), (4,), (17,), (4,)]
    encoded, decoded = pl.pallas_call(
        layer_kernel,
        out_shape=(
            pltpu.VMEM((4, ROWS, D), b16),
            pltpu.VMEM((SLOTS, 16, D), b16),
        ),
        in_specs=[smem] + [hbm] * 13 + [smem],
        out_specs=(vmem, vmem),
        scratch_shapes=[pltpu.VMEM(*s) for s in scratch] + [pltpu.SemaphoreType.DMA(s) for s in sems],
        compiler_params=pltpu.CompilerParams(
            collective_id=0, has_side_effects=True, vmem_limit_bytes=54 << 20
        ),
        name="layer",
    )(lens, tokens, gain_attn, wqkv, gain_ffn, gain_final, gain_cross, wo, wi, wf, targets, wcq, wckv, wco, target_lens)
    encoded, decoded = pl.pallas_call(
        leave_kernel,
        out_shape=(
            jax.ShapeDtypeStruct(encoded.shape, b16),
            jax.ShapeDtypeStruct(decoded.shape, b16),
        ),
        in_specs=[vmem, vmem],
        out_specs=(hbm, hbm),
        scratch_shapes=[pltpu.SemaphoreType.DMA((2,))],
        name="leave",
    )(
        pltpu.with_memory_space_constraint(encoded, pltpu.VMEM),
        pltpu.with_memory_space_constraint(decoded, pltpu.VMEM),
    )
    return encoded.reshape(TOK_DEV, D), decoded.reshape(targets.shape)


def local(
    tokens,
    norm_attn,
    self_qkv,
    self_out,
    norm_ffn,
    ffn_in,
    ffn_out,
    norm_final,
    pad_lengths,
    targets,
    target_lengths,
    norm_cross,
    cross_query,
    cross_kv,
    cross_out,
):
    return layer(
        pad_lengths,
        tokens,
        (norm_attn, norm_ffn, norm_final, norm_cross),
        self_qkv,
        self_out,
        jnp.swapaxes(ffn_in, 1, 2),
        ffn_out,
        targets,
        cross_query,
        cross_kv,
        cross_out,
        target_lengths,
    )


def solution(mesh):
    in_specs = (
        P("seq", None),
        P(),
        P(None, None, "head"),
        P("head", None),
        P(),
        P(None, None, "head"),
        P("head", None),
        P(),
        P(),
        P(),
        P(),
        P(),
        P(None, "head"),
        P(None, None, "head"),
        P("head", None),
    )
    out_specs = (P("seq", None), P())
    return jax.shard_map(local, mesh=mesh, in_specs=in_specs, out_specs=out_specs, check_vma=False)
```

```python
import functools
import math

import jax
import jax.numpy as jnp
from jax import lax
from jax.experimental import pallas as pl
from jax.experimental.pallas import tpu as pltpu
from jax.sharding import Mesh
from jax.sharding import PartitionSpec as P

D = 1024
HD = 64
TOK_DEV = 512


epsilon = 1e-06
masked_score = -1e30


NZ = 8
SLOTS = 32
UP = (("O", 0, 0), ("O", 0, 1), ("O", 1, 0), ("O", 1, 1), ("O", 2, 0), ("O", 2, 1), ("P", 2, 0), ("O", 3, 0), ("P", 2, 1), ("P", 3, 0))
DOWN = (("O", 0, 1), ("O", 0, 0), ("O", -1, 1), ("O", -1, 0), ("O", -2, 1), ("O", -2, 0), ("P", -2, 1), ("O", -3, 1), ("P", -3, 1), ("P", -2, 0))
SIDE = (("O", 0, 0), ("O", 0, 1), ("O", 1, 0), ("O", -1, 1), ("O", 2, 0), ("O", -2, 1), ("O", 2, 1), ("O", -2, 0), ("O", 1, 1), ("O", -1, 0))
STEPS = 10
FF_DEV = 352
ROWS = 128
UNIT = 256


def link_plan():
    arrive = {("O", 0, 0): -1, ("O", 0, 1): -1}
    arrivals = []
    for s in range(STEPS):
        new = [(UP[s][0], UP[s][1] + 1, UP[s][2]), (DOWN[s][0], DOWN[s][1] - 1, DOWN[s][2])]
        new.append(("P", SIDE[s][1], SIDE[s][2]))
        arrive.update({item: s for item in new})
        arrivals.append(new)
    waiting = {"up": list(UP), "down": list(DOWN), "side": list(SIDE)}
    sent = {name: 0 for name in waiting}
    sends = []
    for s in range(-1, STEPS):
        now = []
        for name, queue in waiting.items():
            while queue and sent[name] <= s + 2 and arrive[queue[0]] <= s:
                now.append((name, queue.pop(0)))
                sent[name] += 1
        sends.append(now)
    return arrivals, sends


ARRIVALS, SENDS = link_plan()
UNITS = (("O", 0, 0), ("O", 0, 1), *(item for step in ARRIVALS for item in step))
MATE_AT = {(2 + 3 * s) // 2 * 2: s for s in range(STEPS)}
STEP_AT = {2: 0, 4: 1, 6: 2, 8: 3, 12: 4, 14: 5, 18: 6, 20: 7, 24: 8, 26: 9}
WEIGHT_STEP_AT = {8: (("pass", 0),), 14: (("start", 2),), 18: (("pass", 1), ("end", 0))}
UNIT_CODES = tuple((4 - d) * 4 + (line == "P") * 2 + half for line, d, half in UNITS)
CODE_WORDS = tuple(
    sum(code << (8 * k) for k, code in enumerate(UNIT_CODES[first : first + 3]))
    for first in range(0, len(UNITS), 3)
)


def key_bias(length, first, rows):
    row = first + lax.broadcasted_iota(jnp.int32, (rows, 128), 0)
    lane = lax.broadcasted_iota(jnp.int32, (rows, 128), 1)
    return jnp.where((lane == 0) & (row >= length), masked_score, 0.0).astype(jnp.bfloat16)


def spread_queries(q_t):
    rows = lax.broadcasted_iota(jnp.int32, (256, 2 * q_t.shape[1]), 0)
    cols = lax.broadcasted_iota(jnp.int32, (256, 2 * q_t.shape[1]), 1)
    half = q_t.shape[1]
    two = jnp.concatenate([q_t, q_t], axis=1)
    full = jnp.concatenate([two, jnp.zeros_like(two)], axis=0)
    keep = ((rows < HD) & (cols < half)) | ((rows >= HD) & (rows < 2 * HD) & (cols >= half))
    return jnp.where(keep, full, jnp.where(rows == 2 * HD, 1.0, 0.0)).astype(jnp.bfloat16)


def normalised(x, gain):
    return x * lax.rsqrt(jnp.mean(x * x, axis=1, keepdims=True) + epsilon) * gain


def dot32(a, b):
    return jnp.dot(a, b, preferred_element_type=jnp.float32)


def layer_kernel(
    lens,
    tokens_hbm,
    gain_attn_hbm,
    wqkv_hbm,
    gain_ffn_hbm,
    gain_final_hbm,
    gain_cross_hbm,
    wo_hbm,
    wi_hbm,
    wf_hbm,
    targets_hbm,
    wcq_hbm,
    wckv_hbm,
    wco_hbm,
    target_lens,
    enc,
    dec,
    tokens,
    gain_attn,
    wqkv,
    gain_ffn,
    gain_final,
    gain_cross,
    kv,
    spread,
    acc,
    scores_0,
    scores_1,
    wo,
    wi,
    wf,
    targets,
    wcq,
    wckv_all,
    wo_all,
    wi_all,
    wf_all,
    ctx,
    ctx_in,
    hidden,
    out_1,
    in_1,
    out_2,
    in_2,
    kvc_out,
    kvc_in,
    cross_spread,
    cross_values,
    wco_all,
    o_all,
    s_all,
    o_mate,
    s_mate,
    o_half,
    s_half,
    o_side,
    s_side,
    o_rows,
    s_rows,
    o_line,
    s_line,
    c_all,
    sum_out,
    sum_in,
    local_sem,
    send,
    recv,
    recv_w,
    recv_c,
    recv_y,
    recv_e,
    recv_m,
    recv_l,
    recv_h,
    recv_d,
    recv_k,
):
    me = lax.axis_index("seq")
    core = lax.rem(me, 2)
    y = lax.rem(me // 2, 2)
    z = me // 4
    head = lax.axis_index("head")
    x = lax.rem(head, 4)
    yh = head // 4

    def index(dz, dy, dc):
        z_at = lax.rem(z + dz + NZ, NZ)
        y_at = y if dy == 0 else 1 - y
        c_at = core if dc == 0 else 1 - core
        return z_at * 4 + y_at * 2 + c_at

    places = {
        "up": {"seq": index(1, 0, 0)},
        "down": {"seq": index(-1, 0, 0)},
        "side": {"seq": index(0, 1, 0)},
        "mate": {"seq": index(0, 0, 1)},
        "diagonal": {"seq": index(0, 1, 1)},
        "right": {"head": yh * 4 + lax.rem(x + 1, 4)},
        "left": {"head": yh * 4 + lax.rem(x + 3, 4)},
        "across": {"head": yh * 4 + lax.rem(x + 2, 4)},
        "partner": {"head": (1 - yh) * 4 + x},
    }
    for dz in range(2, NZ - 1):
        places[dz] = {"seq": index(dz, 0, 0)}
    line_place = {1: "up", NZ - 1: "down", **{dz: dz for dz in range(2, NZ - 1)}}
    barrier = pltpu.get_barrier_semaphore()
    for place in places.values():
        pl.semaphore_signal(barrier, inc=1, device_id=place, device_id_type=pl.DeviceIdType.MESH)

    pairs = {
        "tokens": (tokens_hbm, tokens),
        "wqkv": (wqkv_hbm, wqkv),
        "gain_attn": (gain_attn_hbm, gain_attn),
        "wo": (wo_hbm, wo),
        "wi": (wi_hbm, wi),
        "wf": (wf_hbm, wf),
        "wco": (wco_hbm, wco_all.at[3]),
        "targets": (targets_hbm, targets),
        "wcq": (wcq_hbm, wcq),
        "gain_cross": (gain_cross_hbm, gain_cross),
        "gain_ffn": (gain_ffn_hbm, gain_ffn),
        "gain_final": (gain_final_hbm, gain_final),
        "wckv": (wckv_hbm, wckv_all.at[3]),
    }
    loads = {
        name: pltpu.make_async_copy(source, target, local_sem.at[k])
        for k, (name, (source, target)) in enumerate(pairs.items())
    }
    first_loads = ("tokens", "gain_attn", "wqkv")
    for name in first_loads:
        loads[name].start()
    for name in first_loads:
        loads[name].wait()
    for name, load in loads.items():
        if name not in first_loads:
            load.start()
    normed = normalised(tokens[...].astype(jnp.float32), gain_attn[...]).astype(jnp.bfloat16)
    own_keys = dot32(normed, wqkv[1]).astype(jnp.bfloat16)
    own_values = dot32(normed, wqkv[2]).T.astype(jnp.bfloat16)
    for half in range(2):
        kv[me, half, 0:UNIT, :] = own_keys[half * UNIT : (half + 1) * UNIT, :]
        for k in range(2):
            first = half * UNIT + k * 128
            kv[me, half, pl.ds(UNIT + k * 128, 128), :] = own_values[:, first : first + 128]
    pl.semaphore_wait(barrier, len(places))

    def remote(source, target, number, arrival, place):
        return pltpu.make_async_remote_copy(
            src_ref=source,
            dst_ref=target,
            send_sem=send.at[number],
            recv_sem=arrival,
            device_id=places[place],
            device_id_type=pl.DeviceIdType.MESH,
        )

    def go(source, target, arrival, place, group):
        remote(source, target, group, arrival, place).start()

    def wait_step(mate_side, s):
        ref = kv.at[pl.ds(0, 3), 0]
        remote(ref, ref, 0, recv.at[mate_side, s], "mate").wait_recv()

    def push(half, slot, place, s):
        ref = kv.at[slot, half]
        go(ref, ref, recv.at[int(place == "mate"), s], place, 4)

    def slot_of(line, d):
        return index(-d, 0 if line == "O" else 1, 0)

    link_items = {"up": UP, "down": DOWN, "side": SIDE}
    for name, item in SENDS[0]:
        push(item[2], me, name, link_items[name].index(item))
    for half in range(2):
        push(half, me, "mate", STEPS)

    def piece(item, slot, which, c):
        own, gathered = ((wo, wo_all), (wi, wi_all), (wf, wf_all), (wco_all.at[3], wco_all), (wckv_all.at[3], wckv_all))[item]
        ref = own if slot is None else gathered.at[slot]
        if item in (0, 3):
            first, size = ((0, 64), (0, 32), (32, 32))[which]
            return ref.at[pl.ds(pl.multiple_of(c * 64 + first, 32), size), :]
        if item in (1, 4):
            rows = ref.shape[1] // 2
            first, size = ((0, 2 * rows), (0, rows), (rows, rows))[which]
            return ref.at[c, pl.ds(first, size), :]
        first, size = ((0, 176), (0, 96), (96, 80))[which]
        return ref.at[pl.ds(pl.multiple_of(c * 176 + first, 16), size), :]

    def wait_piece(item, slot, which, k, c):
        ref = piece(item, slot, which, c)
        remote(ref, ref, 0, recv_w.at[item, k], "mate").wait_recv()

    def send_piece(item, slot, slot_there, which, k, to):
        source, target = piece(item, slot, which, core), piece(item, slot_there, which, core)
        go(source, target, recv_w.at[item, k], to, 18 if item == 4 else item)

    def weights_start(item):
        loads[("wo", "wi", "wf", "wco", "wckv")[item]].wait()
        for slot, to in ((0, "right"), (1, "left")):
            send_piece(item, None, slot, 0, slot, to)

    def weights_pass(item):
        for slot, half, onward in ((0, 1, "right"), (1, 2, "left")):
            wait_piece(item, slot, 0, slot, core)
            send_piece(item, slot, 2, half, 1 + half, onward)
            send_piece(item, slot, slot, 0, 4, "mate")

    def weights_end(item):
        for half in (1, 2):
            wait_piece(item, 2, half, 1 + half, core)
            send_piece(item, 2, 2, half, 4, "mate")

    def weights_here(item):
        c = 1 - core
        ref = (
            lambda: wo_all.at[:, pl.ds(pl.multiple_of(c * 64, 64), 64), :],
            lambda: wi_all.at[:, c],
            lambda: wf_all.at[:, pl.ds(pl.multiple_of(c * 176, 16), 176), :],
            lambda: wco_all.at[pl.ds(0, 3), pl.ds(pl.multiple_of(c * 64, 64), 64), :],
            lambda: wckv_all.at[pl.ds(0, 3), c],
        )[item]()
        remote(ref, ref, 0, recv_w.at[item, 4], "mate").wait_recv()

    for item in range(2):
        weights_start(item)
    q_t = dot32(normed, wqkv[0]).T

    spread[...] = spread_queries(q_t * (HD ** (-0.5) * math.log2(math.e)))
    acc[...] = jnp.zeros_like(acc)
    for name in ("targets", "wcq", "gain_cross", "gain_ffn", "gain_final"):
        loads[name].wait()
    cross_normed = normalised(targets[...].astype(jnp.float32), gain_cross[...]).astype(jnp.bfloat16)
    cross_spread[...] = spread_queries(
        dot32(cross_normed, wcq[...]).T * (HD ** (-0.5) * math.log2(math.e))
    )

    def step(s):
        wait_step(0, s)
        for line, d, half in ARRIVALS[s]:
            push(half, slot_of(line, d), "mate", s)
        for name, item in SENDS[s + 1]:
            line, d, half = item
            push(half, slot_of(line, d), name, link_items[name].index(item))

    def unit_of(u):
        third = u // 3
        word = jnp.int32(CODE_WORDS[0])
        for k in range(1, len(CODE_WORDS)):
            word = jnp.where(third == k, CODE_WORDS[k], word)
        code = lax.rem(lax.shift_right_logical(word, 8 * (u - 3 * third)), 256)
        half = lax.rem(code, 2)
        chip = lax.rem(z + code // 4 + 4, NZ) * 4 + lax.rem(y + code // 2, 2) * 2
        return chip + core, chip + 1 - core, half

    def score(block, bias, queries, into):
        s = dot32(jnp.concatenate([block, bias], axis=1), queries[...])
        into[...] = s
        return jnp.max(s, axis=0, keepdims=True)

    def unit_score(unit, into):
        here, there, half = unit
        block = jnp.concatenate([kv[here, half, 0:UNIT, :], kv[there, half, 0:UNIT, :]], axis=0)
        bias = jnp.concatenate(
            [key_bias(lens[slot], half * UNIT, UNIT) for slot in (here, there)], axis=0
        )
        return score(block, bias, spread, into)

    def rest(rows_of_head, held, old, top):
        p = jnp.exp2(held[...] - top).astype(jnp.bfloat16)
        shrink = jnp.exp2(old - top)
        ones = jnp.ones((16, TOK_DEV), jnp.bfloat16)
        for h in range(2):
            cols = slice(h * TOK_DEV, (h + 1) * TOK_DEV)
            lhs = jnp.concatenate([rows_of_head(h), ones], axis=0)
            acc[h] = acc[h] * shrink[:, cols] + dot32(lhs, p[:, cols])

    def unit_rest(unit, held, old, top):
        here, there, half = unit

        def rows_of_head(h):
            return jnp.concatenate(
                [
                    kv[slot, half, pl.ds(UNIT + k * 128 + h * HD, HD), :]
                    for slot in (here, there)
                    for k in range(2)
                ],
                axis=1,
            )

        rest(rows_of_head, held, old, top)

    acts = {"start": weights_start, "pass": weights_pass, "end": weights_end}

    def handle(u):
        for at in sorted({*STEP_AT, *MATE_AT, *WEIGHT_STEP_AT}):

            @pl.when(u == at)
            def _():
                if at in STEP_AT:
                    step(STEP_AT[at])
                for what, item in WEIGHT_STEP_AT.get(at, ()):
                    acts[what](item)
                if at in MATE_AT:
                    wait_step(1, MATE_AT[at])

    start = jnp.full((1, 2 * TOK_DEV), masked_score, jnp.float32)
    zero = jnp.int32(0)
    first, second = unit_of(zero), unit_of(zero + 1)
    both_halves = kv.at[me]
    remote(both_halves, both_halves, 0, recv.at[1, STEPS], "mate").wait_recv()
    top = unit_score(first, scores_0)
    following = jnp.maximum(top, unit_score(second, scores_1))
    unit_rest(first, scores_0, start, top)

    def body(j, carry):
        old, top, before = carry
        u = 2 * j
        here, after = unit_of(u), unit_of(u + 1)
        handle(u)
        later = jnp.maximum(top, unit_score(here, scores_0))
        unit_rest(before, scores_1, old, top)
        old, top = top, later
        later = jnp.maximum(top, unit_score(after, scores_1))
        unit_rest(here, scores_0, old, top)
        return top, later, after

    old, top, last = lax.fori_loop(1, len(UNITS) // 2, body, (top, following, second))
    unit_rest(last, scores_1, old, top)
    both = jnp.concatenate([acc[h, 0:HD, :] / acc[h, HD : HD + 1, :] for h in range(2)], axis=0)
    ctx[...] = both.T.astype(jnp.bfloat16)

    def ctx_rows(at):
        return ctx.at[pl.ds(pl.multiple_of(lax.rem(at, 4) * ROWS, ROWS), ROWS), :]

    for g, (to, at) in enumerate((("right", x + 1), ("left", x + 3), ("across", x + 2))):
        go(ctx_rows(at), ctx_in.at[g], recv_c.at[g], to, 5)
    weights_pass(2)
    weights_here(0)
    weights_end(1)
    total = dot32(ctx_rows(x)[...], wo[...])
    for g in range(3):
        remote(ctx_in.at[g], ctx_in.at[g], 0, recv_c.at[g], "mate").wait_recv()
    wide = D // 2
    for k in range(2):
        cols = slice(k * wide, (k + 1) * wide)
        summed = total[:, cols]
        for g in range(3):
            summed += dot32(ctx_in[g], wo_all[g, :, cols])
        out_1[k] = summed.astype(jnp.bfloat16)
        go(out_1.at[k], in_1.at[k], recv_y.at[3 * k], "partner", 6 if k == 0 else 21)
    weights_start(4)
    weights_end(2)
    weights_here(1)
    weights_here(2)
    for k in range(2):
        remote(out_1.at[k], in_1.at[k], 0, recv_y.at[3 * k], "partner").wait_recv()
    total = jnp.concatenate(
        [out_1[k].astype(jnp.float32) + in_1[k].astype(jnp.float32) for k in range(2)], axis=1
    )
    total += tokens[pl.ds(pl.multiple_of(x * ROWS, ROWS), ROWS), :].astype(jnp.float32)
    hidden[...] = total
    ffn_normed = normalised(total, gain_ffn[...]).T.astype(jnp.bfloat16)
    acts_here = []
    for g in range(4):
        gate_w, up_w, down_w = (
            (wi[0], wi[1], wf) if g == 3 else (wi_all[g, 0], wi_all[g, 1], wf_all.at[g])
        )
        gate = dot32(gate_w, ffn_normed)
        up = dot32(up_w, ffn_normed)
        activated = (jax.nn.gelu(gate, approximate=True) * up).T.astype(jnp.bfloat16)
        acts_here.append((activated, down_w))
        if g == 1:
            weights_pass(4)
    for k in range(2):
        ffn = jnp.zeros((ROWS, wide), jnp.float32)
        for activated, down_w in acts_here:
            ffn += dot32(activated, down_w[:, k * wide : (k + 1) * wide])
        out_2[k] = ffn.astype(jnp.bfloat16)
        go(out_2.at[k], in_2.at[k], recv_y.at[1 + k], "partner", 7 if k == 0 else 20)
    weights_end(4)
    weights_start(3)
    weights_here(4)
    for k in range(2):
        remote(out_2.at[k], in_2.at[k], 0, recv_y.at[1 + k], "partner").wait_recv()
    final = jnp.concatenate(
        [out_2[k].astype(jnp.float32) + in_2[k].astype(jnp.float32) for k in range(2)], axis=1
    )
    final += hidden[...]
    rows_here = normalised(final, gain_final[...]).astype(jnp.bfloat16)
    enc[x] = rows_here

    def cross_pair(slot):
        weights = jnp.concatenate([wckv_all[slot, 0], wckv_all[slot, 1]], axis=1)
        return dot32(rows_here, weights).astype(jnp.bfloat16)

    for slot, to in ((2, "across"), (0, "left"), (1, "right")):
        both = cross_pair(slot)
        kvc_out[slot, 0] = both[:, : 2 * HD]
        kvc_out[slot, 1] = both[:, 2 * HD :]
        go(kvc_out.at[slot], kvc_in.at[x], recv_k.at[x], to, 19)
    both = cross_pair(3)
    kvc_in[x, 0] = both[:, : 2 * HD]
    kvc_in[x, 1] = both[:, 2 * HD :]

    def beside(dx):
        return lax.rem(x + dx + 4, 4)

    for dx in (-1, 1, 2):
        ref = kvc_in.at[beside(dx)]
        remote(ref, ref, 0, recv_k.at[beside(dx)], "mate").wait_recv()

    def rows_of(at, half):
        if half is None:
            return enc.at[at]
        return enc.at[at, pl.ds(half * 64, 64), :]

    def send_share(at, half, to):
        go(rows_of(at, half), rows_of(at, half), recv_e.at[at, half or 0], to, 8)

    def wait_share(at, half):
        ref = rows_of(at, half)
        remote(ref, ref, 0, recv_e.at[at, half or 0], "mate").wait_recv()

    weights_pass(3)
    cross_keys = jnp.concatenate([kvc_in[k, 0] for k in range(4)], axis=0)
    cross_rows = jnp.concatenate([kvc_in[k, 1] for k in range(4)], axis=0)
    cross_values[...] = cross_rows.astype(jnp.float32).T.astype(jnp.bfloat16)
    acc[...] = jnp.zeros_like(acc)
    cross_top = score(cross_keys, key_bias(lens[me], 0, TOK_DEV), cross_spread, scores_0)
    rest(lambda h: cross_values[pl.ds(h * HD, HD), :], scores_0, start, cross_top)
    o_all[...] = jnp.concatenate([acc[h, 0:HD, :] / acc[h, HD : HD + 1, :] for h in range(2)], axis=0)
    s_all[...] = jnp.concatenate(
        [
            cross_top[:, h * TOK_DEV : (h + 1) * TOK_DEV] + jnp.log2(acc[h, HD : HD + 1, :])
            for h in range(2)
        ]
        + [jnp.zeros((6, TOK_DEV), jnp.float32)],
        axis=0,
    )

    def joined(first, first_lse, second, second_lse):
        outs, lses = [], []
        for h in range(2):
            one, two = first_lse[h : h + 1], second_lse[h : h + 1]
            top = jnp.maximum(one, two)
            one, two = jnp.exp2(one - top), jnp.exp2(two - top)
            both = one + two
            dims = slice(h * HD, (h + 1) * HD)
            outs.append(first[dims] * (one / both) + second[dims] * (two / both))
            lses.append(top + jnp.log2(both))
        return jnp.concatenate(outs, axis=0), lses

    def lanes(at, size):
        return pl.ds(pl.multiple_of(at * size, size), size)

    def wait_for(ref, arrival):
        remote(ref, ref, 0, arrival, "mate").wait_recv()

    half, quarter = TOK_DEV // 2, TOK_DEV // 4
    go(o_all.at[:, lanes(1 - core, half)], o_mate, recv_m.at[0], "mate", 9)
    go(s_all.at[:, lanes(1 - core, half)], s_mate, recv_m.at[1], "mate", 10)
    for to in ("right", "left"):
        send_share(x, None, to)
    wait_for(o_mate, recv_m.at[0])
    wait_for(s_mate, recv_m.at[1])
    o, lse = joined(
        o_all[:, lanes(core, half)], s_all[:, lanes(core, half)], o_mate[...], s_mate[...]
    )
    o_half[...] = o.astype(jnp.bfloat16)
    s_half[...] = jnp.concatenate(lse + [jnp.zeros((6, half), jnp.float32)], axis=0)
    go(o_half.at[:, lanes(1 - y, quarter)], o_side, recv_m.at[2], "side", 11)
    go(s_half.at[:, lanes(1 - y, quarter)], s_side, recv_m.at[3], "side", 12)
    wait_for(o_side, recv_m.at[2])
    wait_for(s_side, recv_m.at[3])
    o, lse = joined(
        o_half[:, lanes(y, quarter)].astype(jnp.float32),
        s_half[:, lanes(y, quarter)],
        o_side[...].astype(jnp.float32),
        s_side[...],
    )
    o_rows[...] = o.T.astype(jnp.bfloat16)
    s_rows[...] = jnp.concatenate([jnp.broadcast_to(part, (HD, quarter)) for part in lse], axis=0).T
    few = quarter // NZ

    def few_rows(ref, at):
        return ref.at[pl.ds(pl.multiple_of(at * few, few), few), :]

    for dz in (4, 3, 5, 2, 6, 1, 7):
        at = lax.rem(z + dz, NZ)
        go(few_rows(o_rows, at), o_line.at[z], recv_l.at[0], line_place[dz], 13)
        go(few_rows(s_rows, at), s_line.at[z], recv_l.at[1], line_place[dz], 14)
    for dx, half, to in ((-1, 0, "right"), (1, 1, "left")):
        wait_share(beside(dx), None)
        send_share(beside(dx), half, to)
    weights_end(3)
    o_line[z] = few_rows(o_rows, z)[...]
    s_line[z] = few_rows(s_rows, z)[...]
    wait_for(o_line.at[pl.ds(0, NZ - 1)], recv_l.at[0])
    wait_for(s_line.at[pl.ds(0, NZ - 1)], recv_l.at[1])
    lines = s_line[...]
    factors = jnp.exp2(lines - jnp.max(lines, axis=0, keepdims=True))
    c_all[3] = (
        jnp.sum(o_line[...].astype(jnp.float32) * factors, axis=0) / jnp.sum(factors, axis=0)
    ).astype(jnp.bfloat16)
    for g, to in enumerate(("right", "left", "across")):
        go(c_all.at[3], c_all.at[g], recv_h.at[g], to, 15)
    weights_here(3)
    for g in range(3):
        wait_for(c_all.at[g], recv_h.at[g])
    total = jnp.zeros((few, D), jnp.float32)
    for k in range(4):
        away = lax.rem(k - x + 4, 4)
        g = jnp.where(away == 0, 3, jnp.where(away == 3, 0, away))
        total += dot32(c_all[g], wco_all[g])
    sum_out[...] = total.astype(jnp.bfloat16)
    go(sum_out, sum_in, recv_h.at[3], "partner", 16)

    def place_of(z_at, dy, dc):
        y_at = y if dy == 0 else 1 - y
        c_at = core if dc == 0 else 1 - core
        return c_at * 16 + y_at * NZ + z_at

    mine = place_of(z, 0, 0)
    target_rows = targets[pl.ds(pl.multiple_of(mine * few, few), few), :].astype(jnp.float32)
    slots = z * few + lax.broadcasted_iota(jnp.int32, (few, D), 0)
    wait_for(sum_in, recv_h.at[3])
    total = sum_out[...].astype(jnp.float32) + sum_in[...].astype(jnp.float32)
    live = slots < target_lens[core * 2 + y]
    dec[mine] = (target_rows + jnp.where(live, total, 0.0)).astype(jnp.bfloat16)

    same_core = ("side", *line_place.values())

    def hand(at, to):
        go(dec.at[at], dec.at[at], recv_d.at[at - core * 16 if to in same_core else 16], to, 17)

    far = (3, 4, 5)
    hand(mine, "side")
    hand(mine, "mate")
    for dz in (1, 7, 2, 6, 3, 5, 4):
        hand(mine, line_place[dz])
    for dz in (1, 7, 2, 6, 3, 5, 4):
        at = place_of(lax.rem(z + dz, NZ), 0, 0)
        wait_for(dec.at[at], recv_d.at[at - core * 16])
        hand(at, "side")
        hand(at, "mate")
        if dz in far:
            hand(at, "diagonal")
    for dz in (0, 1, 7, 2, 6, 3, 5, 4):
        at = place_of(lax.rem(z + dz, NZ), 1, 0)
        wait_for(dec.at[at], recv_d.at[at - core * 16])
        if dz not in far:
            hand(at, "mate")
    wait_for(dec.at[pl.ds(pl.multiple_of((1 - core) * 16, 16), 16)], recv_d.at[16])
    for half in (0, 1):
        wait_share(beside(2), half)
    sent = (
        wo_all,
        wi_all,
        wf_all,
        wco_all.at[pl.ds(0, 3)],
        kv.at[pl.ds(0, SLOTS - 1)],
        ctx_in,
        out_1.at[0],
        out_2.at[0],
        enc.at[pl.ds(0, 3)],
        o_mate,
        s_mate,
        o_side,
        s_side,
        o_line.at[pl.ds(0, NZ - 1)],
        s_line.at[pl.ds(0, NZ - 1)],
        c_all.at[pl.ds(0, 3)],
        sum_out,
        dec.at[pl.ds(0, SLOTS - 1)],
        wckv_all.at[pl.ds(0, 3)],
        kvc_out,
        out_2.at[1],
        out_1.at[1],
    )
    for group, ref in enumerate(sent):
        remote(ref, ref, group, recv_y.at[0], "mate").wait_send()


def leave_kernel(encoded, decoded, encoded_out, decoded_out, sems):
    moves = (
        pltpu.make_async_copy(encoded, encoded_out, sems.at[0]),
        pltpu.make_async_copy(decoded, decoded_out, sems.at[1]),
    )
    for move in moves:
        move.start()
    for move in moves:
        move.wait()


def layer(lens, tokens, gains, wqkv, wo, wi, wf, targets, wcq, wckv, wco, target_lens):
    hbm = pl.BlockSpec(memory_space=pl.ANY)
    vmem = pl.BlockSpec(memory_space=pltpu.VMEM)
    smem = pl.BlockSpec(memory_space=pltpu.SMEM)
    b16, f32 = jnp.bfloat16, jnp.float32
    gain_attn, gain_ffn, gain_final, gain_cross = (g.reshape(1, D) for g in gains)
    scratch = [
        (tokens.shape, b16),
        ((1, D), f32),
        (wqkv.shape, b16),
        ((1, D), f32),
        ((1, D), f32),
        ((1, D), f32),
        ((SLOTS, 2, 2 * UNIT, 2 * HD), b16),
        ((256, 2 * TOK_DEV), b16),
        ((2, HD + 16, TOK_DEV), f32),
        ((TOK_DEV, 2 * TOK_DEV), f32),
        ((TOK_DEV, 2 * TOK_DEV), f32),
        (wo.shape, b16),
        (wi.shape, b16),
        (wf.shape, b16),
        (targets.shape, b16),
        (wcq.shape, b16),
        ((4, *wckv.shape), b16),
        ((3, *wo.shape), b16),
        ((3, *wi.shape), b16),
        ((3, *wf.shape), b16),
        ((TOK_DEV, 2 * HD), b16),
        ((3, ROWS, 2 * HD), b16),
        ((ROWS, D), f32),
        ((2, ROWS, D // 2), b16),
        ((2, ROWS, D // 2), b16),
        ((2, ROWS, D // 2), b16),
        ((2, ROWS, D // 2), b16),
        ((3, 2, ROWS, 2 * HD), b16),
        ((4, 2, ROWS, 2 * HD), b16),
        ((256, 2 * TOK_DEV), b16),
        ((2 * HD, TOK_DEV), b16),
        ((4, *wco.shape), b16),
        ((2 * HD, TOK_DEV), f32),
        ((8, TOK_DEV), f32),
        ((2 * HD, TOK_DEV // 2), f32),
        ((8, TOK_DEV // 2), f32),
        ((2 * HD, TOK_DEV // 2), b16),
        ((8, TOK_DEV // 2), f32),
        ((2 * HD, TOK_DEV // 4), b16),
        ((8, TOK_DEV // 4), f32),
        ((TOK_DEV // 4, 2 * HD), b16),
        ((TOK_DEV // 4, 2 * HD), f32),
        ((NZ, 16, 2 * HD), b16),
        ((NZ, 16, 2 * HD), f32),
        ((4, 16, 2 * HD), b16),
        ((16, D), b16),
        ((16, D), b16),
    ]
    sems = [(16,), (22,), (2, STEPS + 1), (5, 5), (3,), (4,), (4, 2), (4,), (2,), (4,), (17,), (4,)]
    encoded, decoded = pl.pallas_call(
        layer_kernel,
        out_shape=(
            pltpu.VMEM((4, ROWS, D), b16),
            pltpu.VMEM((SLOTS, 16, D), b16),
        ),
        in_specs=[smem] + [hbm] * 13 + [smem],
        out_specs=(vmem, vmem),
        scratch_shapes=[pltpu.VMEM(*s) for s in scratch] + [pltpu.SemaphoreType.DMA(s) for s in sems],
        compiler_params=pltpu.CompilerParams(
            collective_id=0, has_side_effects=True, vmem_limit_bytes=54 << 20
        ),
        name="layer",
    )(lens, tokens, gain_attn, wqkv, gain_ffn, gain_final, gain_cross, wo, wi, wf, targets, wcq, wckv, wco, target_lens)
    encoded, decoded = pl.pallas_call(
        leave_kernel,
        out_shape=(
            jax.ShapeDtypeStruct(encoded.shape, b16),
            jax.ShapeDtypeStruct(decoded.shape, b16),
        ),
        in_specs=[vmem, vmem],
        out_specs=(hbm, hbm),
        scratch_shapes=[pltpu.SemaphoreType.DMA((2,))],
        name="leave",
    )(
        pltpu.with_memory_space_constraint(encoded, pltpu.VMEM),
        pltpu.with_memory_space_constraint(decoded, pltpu.VMEM),
    )
    return encoded.reshape(TOK_DEV, D), decoded.reshape(targets.shape)


def local(
    tokens,
    norm_attn,
    self_qkv,
    self_out,
    norm_ffn,
    ffn_in,
    ffn_out,
    norm_final,
    pad_lengths,
    targets,
    target_lengths,
    norm_cross,
    cross_query,
    cross_kv,
    cross_out,
):
    return layer(
        pad_lengths,
        tokens,
        (norm_attn, norm_ffn, norm_final, norm_cross),
        self_qkv,
        self_out,
        jnp.swapaxes(ffn_in, 1, 2),
        ffn_out,
        targets,
        cross_query,
        cross_kv,
        cross_out,
        target_lengths,
    )


def solution(mesh):
    in_specs = (
        P("seq", None),
        P(),
        P(None, None, "head"),
        P("head", None),
        P(),
        P(None, None, "head"),
        P("head", None),
        P(),
        P(),
        P(),
        P(),
        P(),
        P(None, "head"),
        P(None, None, "head"),
        P("head", None),
    )
    out_specs = (P("seq", None), P())
    return jax.shard_map(local, mesh=mesh, in_specs=in_specs, out_specs=out_specs, check_vma=False)
```
